32 devices in a mesh: gx: 4 (over x, core), gy: 2 (over y), gz: 4 (over z).
Axes of the slice: x: 2, y: 2, z: 4, core: 2. Of those that a mesh axis runs over, the one named last changes fastest.
Arguments:
- warped_image: float32 [256, 128, 512], P('gx', 'gy', 'gz'), may hold values from -6 to 6
- fixed_image: float32 [256, 128, 512], P('gx', 'gy', 'gz'), may hold values from -6 to 6
- fine_control: float32 [3, 32, 16, 64], P(None, 'gx', 'gy', 'gz'), may hold values from -6 to 6
- coarse_control: float32 [3, 8, 4, 16], replicated, may hold values from -6 to 6
Outputs:
- fine_gradient: float32 [3, 32, 16, 64], P(None, 'gx', 'gy', 'gz')
- coarse_gradient: float32 [3, 8, 4, 16], replicated
The draws below stay inside these ranges and needn't reach their ends.
All inputs are finite; a program needn't handle non-finite values.
Results may differ from the reference program's by a relative error of at most 0.0003.
Values sent between devices are 32-bit elements; how exact they have to be, the bound alone decides.
A program may use at most 64 MiB of HBM per device.

```python
import jax
import jax.numpy as jnp
from jax import lax

SPF = 8
SPC = 32
NX = 256
NY = 128
NZ = 512
FX = 32
FY = 16
FZ = 64
KX = 8
KY = 4
KZ = 16


def levels(key, shape, shards, low, largest):
    def one(position, shards_of):
        draws = jax.random.uniform(jax.random.fold_in(jax.random.fold_in(key, 6), position), (shards_of,), jnp.float32, low / len(shards), largest / len(shards))
        return jnp.repeat(jnp.exp(draws), shape[position] // shards_of).reshape((-1,) + (1,) * (len(shape) - position - 1))

    gain = one(*shards[0])
    for cut in shards[1:]:
        gain = gain * one(*cut)
    return gain


def scatter_about(rng, extent, deviation, most, cuts=(), kind=jnp.bfloat16):
    entries = deviation * jax.random.normal(rng, extent, jnp.float32)
    if cuts:
        entries = entries * levels(rng, extent, cuts, -0.22, 0.18)
    return jnp.clip(entries, -most, most).astype(kind)


def setup_inputs(seed: int = 0) -> dict:
    arg_keys = jax.random.split(jax.random.key(seed), 5)
    return {
        "warped_image": scatter_about(arg_keys[0], (NX, NY, NZ), 1.0, 6.0, ((0, 4), (1, 2), (2, 4)), jnp.float32),
        "fixed_image": scatter_about(arg_keys[1], (NX, NY, NZ), 1.0, 6.0, ((0, 4), (1, 2), (2, 4)), jnp.float32),
        "fine_control": scatter_about(arg_keys[2], (3, FX, FY, FZ), 1.0, 6.0, ((1, 4), (2, 2), (3, 4)), jnp.float32),
        "coarse_control": scatter_about(arg_keys[3], (3, KX, KY, KZ), 1.0, 6.0, (), jnp.float32),
    }


bend_factor = 0.01
highest = lax.Precision.HIGHEST


def spline(values):
    magnitude = jnp.abs(values)
    inner = 2.0 / 3.0 - magnitude * magnitude + 0.5 * magnitude * magnitude * magnitude
    remain = 2.0 - magnitude
    outer = remain * remain * remain / 6.0
    return jnp.where(magnitude < 1.0, inner, jnp.where(magnitude < 2.0, outer, 0.0 * magnitude))


def basis_matrix(voxels, points, spacing, voxel_start, point_start):
    voxel = (jnp.arange(voxels, dtype=jnp.int32) + voxel_start).astype(jnp.float32) + 0.5
    centre = (jnp.arange(points, dtype=jnp.int32) + point_start).astype(jnp.float32) * spacing + 0.5 * spacing
    return spline((voxel[:, None] - centre[None, :]) / spacing)


def slope(padded, axis):
    rank = padded.ndim
    count = padded.shape[axis] - 4

    def shifted(offset):
        piece = lax.slice_in_dim(padded, offset, offset + count, axis=axis)
        for other in range(rank - 3, rank):
            if other != axis:
                piece = lax.slice_in_dim(piece, 2, piece.shape[other] - 2, axis=other)
        return piece

    return (shifted(0) - 8.0 * shifted(1) + 8.0 * shifted(3) - shifted(4)) / 12.0


def stencil(padded):
    centre = padded[:, 1:-1, 1:-1, 1:-1]
    total = padded[:, 2:, 1:-1, 1:-1] + padded[:, :-2, 1:-1, 1:-1]
    total = total + padded[:, 1:-1, 2:, 1:-1] + padded[:, 1:-1, :-2, 1:-1]
    total = total + padded[:, 1:-1, 1:-1, 2:] + padded[:, 1:-1, 1:-1, :-2]
    return total - 6.0 * centre


def laplace(field):
    return stencil(jnp.pad(field, ((0, 0), (1, 1), (1, 1), (1, 1))))


def project_blocks(force, along_x, along_y, along_z):
    section = jnp.einsum("axyz,zr->axyr", force, along_z, precision=highest)
    section = jnp.einsum("axyr,yq->axqr", section, along_y, precision=highest)
    return jnp.einsum("axqr,xp->apqr", section, along_x, precision=highest)


def reference(warped_image, fixed_image, fine_control, coarse_control):
    summed = jnp.pad(warped_image + fixed_image, 2)
    difference = warped_image - fixed_image
    fine_x = basis_matrix(NX, FX, SPF, 0, 0)
    fine_y = basis_matrix(NY, FY, SPF, 0, 0)
    fine_z = basis_matrix(NZ, FZ, SPF, 0, 0)
    coarse_x = basis_matrix(NX, KX, SPC, 0, 0)
    coarse_y = basis_matrix(NY, KY, SPC, 0, 0)
    coarse_z = basis_matrix(NZ, KZ, SPC, 0, 0)
    block_rows = 16

    def block(carry, start):
        fine_sum, coarse_sum = carry
        slab = lax.dynamic_slice_in_dim(summed, start, block_rows + 4, 0)
        slopes = jnp.stack([slope(slab, 0), slope(slab, 1), slope(slab, 2)]) * 0.5
        local = lax.dynamic_slice_in_dim(difference, start, block_rows, 0)
        force = slopes * local[None]
        fine_rows = lax.dynamic_slice_in_dim(fine_x, start, block_rows, 0)
        coarse_rows = lax.dynamic_slice_in_dim(coarse_x, start, block_rows, 0)
        fine_sum = fine_sum + project_blocks(force, fine_rows, fine_y, fine_z)
        coarse_sum = coarse_sum + project_blocks(force, coarse_rows, coarse_y, coarse_z)
        return (fine_sum, coarse_sum), None

    starts = jnp.arange(NX // block_rows, dtype=jnp.int32) * block_rows
    initial = (jnp.zeros((3, FX, FY, FZ), jnp.float32), jnp.zeros((3, KX, KY, KZ), jnp.float32))
    (fine_sum, coarse_sum), _ = lax.scan(block, initial, starts)
    fine_gradient = fine_sum * (SPF ** -1.5) + bend_factor * laplace(laplace(fine_control))
    coarse_gradient = coarse_sum * (SPC ** -1.5) + bend_factor * laplace(laplace(coarse_control))
    return fine_gradient, coarse_gradient
```

```python
import functools

import jax
import jax.numpy as jnp
from jax import lax
from jax.experimental import pallas as pl
from jax.experimental.pallas import tpu as pltpu
from jax.sharding import PartitionSpec as P

SPF = 8
SPC = 32
BEND = 0.01
HI = lax.Precision.HIGHEST
MESH = pl.DeviceIdType.MESH
f32 = jnp.float32
bf16 = jnp.bfloat16


def nn(a, b):
    return lax.dot_general(
        a, b, (((1,), (0,)), ((), ())), precision=HI, preferred_element_type=f32
    )


def nt(a, b):
    return lax.dot_general(
        a, b, (((1,), (1,)), ((), ())), precision=HI, preferred_element_type=f32
    )


def spline(t):
    m = jnp.abs(t)
    inner = 2.0 / 3.0 - m * m + 0.5 * m * m * m
    r = 2.0 - m
    outer = r * r * r * (1.0 / 6.0)
    return jnp.where(m < 1.0, inner, jnp.where(m < 2.0, outer, 0.0))


def weight(voxel, point, spacing):
    scaled = (2 * voxel + 1 - spacing * (2 * point + 1)).astype(f32)
    return spline(scaled * (0.5 / spacing))


def iota(shape, axis):
    return lax.broadcasted_iota(jnp.int32, shape, axis)


def diff1(out, inp):
    d = jnp.abs(out - inp)
    return jnp.where(d == 0, -2.0, jnp.where(d == 1, 1.0, 0.0)).astype(f32)


def diff2(out, inp, count):
    d = jnp.abs(out - inp)
    edge = (inp == 0) | (inp == count - 1)
    centre = jnp.where(edge, 5.0, 6.0)
    return jnp.where(
        d == 0, centre, jnp.where(d == 1, -4.0, jnp.where(d == 2, 1.0, 0.0))
    ).astype(f32)


def same(out, inp):
    return jnp.where(out == inp, 1.0, 0.0).astype(f32)


def bend_planes(px, py, qx, qy, cx, cy):
    jx, jy = same(px, qx), same(py, qy)
    tx, ty = diff1(px, qx), diff1(py, qy)
    m0 = diff2(px, qx, cx) * jy + jx * diff2(py, qy, cy) + 2.0 * tx * ty
    m1 = 2.0 * (tx * jy + jx * ty)
    return m0 * BEND, m1 * BEND, jx * jy * BEND


def kernel(sizes, w_hbm, f_hbm, fc_hbm, cc_hbm, fo_ref, co_ref,
           w_v, f_v, fc_ref, cc_ref, s_v, ysend, yrecv, zsend, zrecv, zcorr,
           wf_v, wc_v, fh_v, fl_v,
           accf, accc, tz_v, bend_v, ccp, bendc, zmsg, zgot, a_v, agot, b_v, bgot,
           cslots, load_sem, small_sem, hs_sem, hr_sem, ys_sem, yr_sem,
           ms_sem, mr_sem, cs_sem, cr_sem):
    nx, ny, nz = sizes
    axes = ("gx", "gy", "gz")
    counts = sizes
    me = [lax.axis_index(a) for a in axes]
    SX, SY, SZ = w_v.shape
    PX, PY, PZ = SX // SPF, SY // SPF, SZ // SPF
    KX, KY, KZ = cc_ref.shape[1:]
    EX, QE, QC = PX + 4, 2 * PY, accc.shape[1]
    cells = SX // SPF
    lanes = 3 * SZ

    loads = []
    for c in range(cells):
        part = pl.ds(c * SPF, SPF)
        loads.append((
            pltpu.make_async_copy(w_hbm.at[part], w_v.at[part], load_sem.at[0, c]),
            pltpu.make_async_copy(f_hbm.at[part], f_v.at[part], load_sem.at[1, c]),
        ))
    small = (pltpu.make_async_copy(fc_hbm, fc_ref, small_sem.at[0]),
             pltpu.make_async_copy(cc_hbm, cc_ref, small_sem.at[1]))
    order = [0, cells - 1] + list(range(1, cells - 1))
    for c in order:
        loads[c][0].start()
        loads[c][1].start()
    for copy in small:
        copy.start()

    zero_plane = jnp.zeros((2, SY, SZ), f32)
    s_v[0:2, 8:8 + SY, :] = zero_plane
    s_v[SX + 2:SX + 4, 8:8 + SY, :] = zero_plane
    yrecv[...] = jnp.zeros(yrecv.shape, f32)
    zrecv[...] = jnp.zeros(zrecv.shape, f32)
    zgot[...] = jnp.zeros(zgot.shape, f32)
    agot[...] = jnp.zeros(agot.shape, f32)
    bgot[...] = jnp.zeros(bgot.shape, f32)

    barrier = pltpu.get_barrier_semaphore()
    total = 0
    for k, a in enumerate(axes):
        for d in range(1, counts[k]):
            pl.semaphore_signal(
                barrier, inc=1, device_id={a: lax.rem(me[k] + d, counts[k])}, device_id_type=MESH
            )
            total += 1

    def split_store(ref, index, value):
        high = value.astype(bf16)
        ref[index + (0,)] = high
        ref[index + (1,)] = (value - high.astype(f32)).astype(bf16)

    KC = SPF * SY
    def ext_q(q):
        return jnp.where(q < PY, q, jnp.where(q < PY + 2, q - PY - 2, q - 2))

    rows, cols = iota((5 * QE, KC), 0), iota((5 * QE, KC), 1)
    split_store(wf_v, (), weight(cols // SY, rows // QE - 2, SPF)
                * weight(cols % SY, ext_q(rows % QE), SPF))
    rows, cols = iota((4 * QC, KC), 0), iota((4 * QC, KC), 1)
    along_y = weight(cols % SY + me[1] * SY, rows % QC, SPC)
    for ph in range(SPC // SPF):
        first = -2 if ph < SPC // SPF // 2 else -1
        split_store(wc_v, (ph,),
                    weight(cols // SY + ph * SPF, rows // QC + first, SPC) * along_y)

    pl.semaphore_wait(barrier, total)

    has = [(me[k] > 0, me[k] < counts[k] - 1) for k in range(3)]
    pieces = ys_sem.shape[1]
    each = SX // pieces

    def halo(k, side, piece=0):
        if k == 1:
            part = pl.ds(piece * each, each)
            return neighbour_copy(
                k, side, ysend.at[side, part], yrecv.at[1 - side, part],
                ys_sem.at[side, piece], yr_sem.at[1 - side, piece])
        if k == 0:
            src = s_v.at[pl.ds(2 if side == 0 else SX, 2), pl.ds(8, SY), :]
            dst = s_v.at[pl.ds(SX + 2 if side == 0 else 0, 2), pl.ds(8, SY), :]
        else:
            src, dst = zsend.at[side], zrecv.at[1 - side]
        return neighbour_copy(k, side, src, dst, hs_sem.at[k, side], hr_sem.at[k, 1 - side])

    def neighbour_copy(k, side, src, dst, send, recv):
        other = me[k] - 1 if side == 0 else me[k] + 1
        return pltpu.make_async_remote_copy(
            src_ref=src, dst_ref=dst, send_sem=send, recv_sem=recv,
            device_id={axes[k]: other}, device_id_type=MESH,
        )

    def start_halo(k, side, piece=0):
        @pl.when(has[k][side])
        def _():
            halo(k, side, piece).start()

    lane = iota((SY, SZ), 1)

    def one_slab(x, carry):
        low, high = carry
        s = w_v[x] + f_v[x]
        s_v[x + 2, 8:8 + SY, :] = s
        ysend[0, x] = s[0:2]
        ysend[1, x] = s[SY - 2:SY]
        here = lane // 2 == x
        low = jnp.where(here, pltpu.roll(s, 2 * x, 1), low)
        high = jnp.where(here, pltpu.roll(s, lax.rem(2 * x + 2, SZ), 1), high)
        return low, high

    carry = (jnp.zeros((SY, SZ), f32), jnp.zeros((SY, SZ), f32))
    done = set()
    sent = set()
    for c in order:
        for copy in loads[c]:
            copy.wait()
        carry = lax.fori_loop(c * SPF, (c + 1) * SPF, one_slab, carry)
        done.add(c)
        for piece in range(pieces):
            inside = range(piece * each // SPF, (piece + 1) * each // SPF)
            if piece not in sent and all(n in done for n in inside):
                sent.add(piece)
                start_halo(1, 0, piece)
                start_halo(1, 1, piece)
        if c == 0:
            start_halo(0, 0)
        if c == cells - 1:
            start_halo(0, 1)
    zsend[0] = carry[0]
    zsend[1] = carry[1]
    start_halo(2, 0)
    start_halo(2, 1)

    accf[...] = jnp.zeros(accf.shape, f32)
    accc[...] = jnp.zeros(accc.shape, f32)
    for copy in small:
        copy.wait()
    shape = (EX * QE, PX * PY)
    rows, cols = iota(shape, 0), iota(shape, 1)
    ox, oy = me[0] * PX, me[1] * PY
    outer, inner = rows // (EX * PY), rows % (EX * PY)
    planes = bend_planes(inner // PY - 2 + ox, ext_q(inner % PY + PY * outer) + oy,
                         cols // PY + ox, cols % PY + oy, PX * nx, PY * ny)
    RZ = tz_v.shape[2]

    def ext_point(row):
        return jnp.where(row < PZ, row, jnp.where(row < PZ + 2, row - PZ - 2, row - 2))

    oz = me[2] * PZ
    zr, zc = ext_point(iota((RZ, PZ), 0)) + oz, iota((RZ, PZ), 1) + oz
    along = (same(zr, zc), diff1(zr, zc), diff2(zr, zc, PZ * nz))
    for a in range(3):
        block = fc_ref[a].reshape(PX * PY, PZ)
        factors = [nn(plane, block) for plane in planes]
        for half in range(2):
            part = slice(half * EX * PY, (half + 1) * EX * PY)
            bend_v[half, a] = (nt(along[0], factors[0][part]) + nt(along[1], factors[1][part])
                               + nt(along[2], factors[2][part]))
    shape = (KX * QC, KX * QC)
    rows, cols = iota(shape, 0), iota(shape, 1)
    planes = bend_planes(rows // QC, rows % QC, cols // QC, cols % QC, KX, KY)
    zr, zc = iota((KZ, KZ), 0), iota((KZ, KZ), 1)
    for a in range(3):
        for p in range(KX):
            ccp[a, p * QC:p * QC + KY, :] = cc_ref[a, p]
        block = ccp[a]
        bendc[a] = (nn(planes[0], block) + nn(planes[1], nn(block, diff1(zr, zc)))
                    + BEND * nn(block, diff2(zr, zc, KZ)))

    for k in (0, 1, 2):
        for side in range(2):
            for piece in range(pieces if k == 1 else 1):
                @pl.when(has[k][side])
                def _(k=k, side=side, piece=piece):
                    halo(k, side, piece).wait_send()

                @pl.when(has[k][1 - side])
                def _(k=k, side=side, piece=piece):
                    halo(k, side, piece).wait_recv()

    even = lane % 2 == 0
    dl = zrecv[0] - zsend[1]
    dh = zrecv[1] - zsend[0]
    zcorr[0] = jnp.where(even, dl - 8.0 * pltpu.roll(dl, SZ - 1, 1), dl)
    zcorr[1] = jnp.where(even, -dh, 8.0 * pltpu.roll(dh, 1, 1) - dh)

    def forces(i):
        slot = i % 2
        for xx in range(SPF):
            x = i * SPF + xx
            s_v[x + 2, 6:8, :] = yrecv[0, x]
            s_v[x + 2, 8 + SY:10 + SY, :] = yrecv[1, x]
            d = w_v[x] - f_v[x]
            s = s_v[x + 2, 8:8 + SY, :]
            gx = (s_v[x, 8:8 + SY, :] - s_v[x + 4, 8:8 + SY, :]
                  + 8.0 * (s_v[x + 3, 8:8 + SY, :] - s_v[x + 1, 8:8 + SY, :]))
            gy = (s_v[x + 2, 6:6 + SY, :] - s_v[x + 2, 10:10 + SY, :]
                  + 8.0 * (s_v[x + 2, 9:9 + SY, :] - s_v[x + 2, 7:7 + SY, :]))
            gz = (pltpu.roll(s, 2, 1) - pltpu.roll(s, SZ - 2, 1)
                  + 8.0 * (pltpu.roll(s, SZ - 1, 1) - pltpu.roll(s, 1, 1)))
            corr = jnp.where(lane < 2, pltpu.roll(zcorr[0], (SZ - 2 * x) % SZ, 1), 0.0)
            corr = jnp.where(lane >= SZ - 2,
                             pltpu.roll(zcorr[1], (2 * SZ - 2 - 2 * x) % SZ, 1), corr)
            gz = gz + corr
            for a, g in enumerate((gx, gy, gz)):
                force = g * d
                high = force.astype(bf16)
                fh_v[slot, xx * SY:(xx + 1) * SY, a * SZ:(a + 1) * SZ] = high
                fl_v[slot, xx * SY:(xx + 1) * SY, a * SZ:(a + 1) * SZ] = (
                    force - high.astype(f32)).astype(bf16)

    def gather(i):
        slot = i % 2
        k, ph = divmod(i, SPC // SPF)
        many = 5 * QE + 4 * QC
        weights = jnp.concatenate([wf_v[0], wc_v[ph, 0], wf_v[1], wc_v[ph, 1]], axis=0)
        both = jnp.dot(weights, fh_v[slot], preferred_element_type=f32)
        out = both[:many] + both[many:] + jnp.dot(
            weights[:many], fl_v[slot], preferred_element_type=f32)
        fine = out[:5 * QE].reshape(5, 2, PY, lanes)
        accf[0, i:i + 5] += fine[:, 0]
        accf[1, i:i + 5] += fine[:, 1]
        at = me[0] * (SX // SPC) + k + (1 if ph >= SPC // SPF // 2 else 0)
        accc[pl.ds(at, 4)] += out[5 * QE:].reshape(4, QC, lanes)

    forces(0)
    for i in range(cells):
        if i + 1 < cells:
            forces(i + 1)
        gather(i)

    rows, cols = iota((RZ, SZ), 0), iota((RZ, SZ), 1)
    bz = weight(cols, ext_point(rows), SPF) * (SPF ** -1.5 / 24.0)
    rows, cols = iota((KZ, SZ), 0), iota((KZ, SZ), 1)
    bzc = weight(cols + me[2] * SZ, rows, SPC) * (SPC ** -1.5 / 24.0)
    for a in range(3):
        for half in range(2):
            block = accf[half, :, :, a * SZ:(a + 1) * SZ].reshape(EX * PY, SZ)
            tz_v[half, a] = nt(bz, block) + bend_v[half, a]
            for side in range(2):
                zmsg[side, half, 2 * a:2 * a + 2, :] = tz_v[
                    half, a, PZ + 2 * side:PZ + 2 * side + 2, :]
    blocks = [accc[2:2 + KX, :, a * SZ:(a + 1) * SZ].reshape(KX * QC, SZ) for a in range(3)]
    cslots[2, me[2]] = nt(bzc, jnp.concatenate(blocks, axis=0))

    def coarse_copy(k, d, slot):
        n = counts[k]
        return pltpu.make_async_remote_copy(
            src_ref=cslots.at[k, slot], dst_ref=cslots.at[k, slot],
            send_sem=cs_sem.at[k, d], recv_sem=cr_sem.at[k, d],
            device_id={axes[k]: lax.rem(me[k] + d, n)}, device_id_type=MESH,
        )

    def exchange(k, source, got):
        for side in range(2):
            @pl.when(has[k][side])
            def _(side=side):
                neighbour_copy(k, side, source(side), got.at[1 - side],
                               ms_sem.at[k, side], mr_sem.at[k, 1 - side]).start()
        for d in range(1, counts[k]):
            coarse_copy(k, d, me[k]).start()
        for side in range(2):
            @pl.when(has[k][side])
            def _(side=side):
                neighbour_copy(k, side, source(side), got.at[1 - side],
                               ms_sem.at[k, side], mr_sem.at[k, 1 - side]).wait_send()

            @pl.when(has[k][1 - side])
            def _(side=side):
                neighbour_copy(k, side, source(side), got.at[1 - side],
                               ms_sem.at[k, side], mr_sem.at[k, 1 - side]).wait_recv()
        for d in range(1, counts[k]):
            coarse_copy(k, d, me[k]).wait_send()
            coarse_copy(k, d, lax.rem(me[k] + counts[k] - d, counts[k])).wait_recv()
        whole = cslots[k, 0]
        for n in range(1, counts[k]):
            whole = whole + cslots[k, n]
        return whole

    whole = exchange(2, lambda side: zmsg.at[side], zgot)
    for half in range(2):
        for a in range(3):
            tz_v[half, a, 0:2, :] = tz_v[half, a, 0:2, :] + zgot[0, half, 2 * a:2 * a + 2, :]
            tz_v[half, a, PZ - 2:PZ, :] = (
                tz_v[half, a, PZ - 2:PZ, :] + zgot[1, half, 2 * a:2 * a + 2, :])
            a_v[half, a * PZ:(a + 1) * PZ, :] = tz_v[half, a, 0:PZ, :]

    cslots[1, me[1]] = whole
    whole = exchange(1, lambda side: a_v.at[1], agot)
    shape = (EX * PY, EX * PY)
    rows, cols = iota(shape, 0), iota(shape, 1)
    p_same = rows // PY == cols // PY
    q, r = rows % PY, cols % PY
    low = jnp.where(p_same & (q == r + 2) & (r < 2), 1.0, 0.0)
    high = jnp.where(p_same & (q == r - (PY - 2)) & (r >= PY - 2), 1.0, 0.0)
    b_v[...] = a_v[0] + nn(agot[0], low) + nn(agot[1], high)

    cslots[0, me[0]] = whole
    whole = exchange(0, lambda side: b_v, bgot)
    shape = (PX * PY, EX * PY)
    rows, cols = iota(shape, 0), iota(shape, 1)
    own = jnp.where(cols == rows + 2 * PY, 1.0, 0.0)
    low = jnp.where((cols == rows + (PX + 2) * PY) & (rows < 2 * PY), 1.0, 0.0)
    high = jnp.where((cols == rows - (PX - 2) * PY) & (rows >= (PX - 2) * PY), 1.0, 0.0)
    shape = (3 * KX * QC, 3 * KX * QC)
    turned = nt(same(iota(shape, 0), iota(shape, 1)), whole)
    for a in range(3):
        part = slice(a * PZ, (a + 1) * PZ)
        out = nt(own, b_v[part]) + nt(low, bgot[0, part]) + nt(high, bgot[1, part])
        fo_ref[a] = out.reshape(PX, PY, PZ)
        out = turned[a * KX * QC:(a + 1) * KX * QC] + bendc[a]
        for p in range(KX):
            co_ref[a, p] = out[p * QC:p * QC + KY, :]


def write_out(f_ref, c_ref, fo_ref, co_ref):
    fo_ref[...] = f_ref[...]
    co_ref[...] = c_ref[...]


def solution(mesh):
    sizes = tuple(mesh.shape[a] for a in ("gx", "gy", "gz"))

    def step(warped, fixed, fine, coarse):
        SX, SY, SZ = warped.shape
        PX, PY, PZ = SX // SPF, SY // SPF, SZ // SPF
        KX, KY, KZ = coarse.shape[1:]
        QC = KY
        EX, QE, RZ = PX + 4, 2 * PY, PZ + 8
        KC = SPF * SY
        most = max(sizes)
        vmem = pl.BlockSpec(memory_space=pltpu.VMEM)
        hbm = pl.BlockSpec(memory_space=pltpu.HBM)
        V = pltpu.VMEM
        D = pltpu.SemaphoreType.DMA
        held = pl.pallas_call(
            functools.partial(kernel, sizes),
            out_shape=(pltpu.VMEM(fine.shape, f32), pltpu.VMEM(coarse.shape, f32)),
            in_specs=[hbm] * 4,
            out_specs=(vmem, vmem),
            scratch_shapes=[
                V((SX, SY, SZ), f32), V((SX, SY, SZ), f32),
                V((3, PX, PY, PZ), f32), V(coarse.shape, f32),
                V((SX + 4, SY + 16, SZ), f32),
                V((2, SX, 2, SZ), f32), V((2, SX, 2, SZ), f32),
                V((2, SY, SZ), f32), V((2, SY, SZ), f32), V((2, SY, SZ), f32),
                V((2, 5 * QE, KC), bf16), V((SPC // SPF, 2, 4 * QC, KC), bf16),
                V((2, KC, 3 * SZ), bf16), V((2, KC, 3 * SZ), bf16),
                V((2, EX, PY, 3 * SZ), f32), V((KX + 4, QC, 3 * SZ), f32),
                V((2, 3, RZ, EX * PY), f32), V((2, 3, RZ, EX * PY), f32),
                V((3, KX * QC, KZ), f32), V((3, KX * QC, KZ), f32),
                V((2, 2, 8, EX * PY), f32), V((2, 2, 8, EX * PY), f32),
                V((2, 3 * PZ, EX * PY), f32), V((2, 3 * PZ, EX * PY), f32),
                V((3 * PZ, EX * PY), f32), V((2, 3 * PZ, EX * PY), f32),
                V((3, most, KZ, 3 * KX * QC), f32),
                D((2, SX // SPF)), D((2,)), D((3, 2)), D((3, 2)), D((2, 4)), D((2, 4)),
                D((3, 2)), D((3, 2)), D((3, most)), D((3, most)),
            ],
            compiler_params=pltpu.CompilerParams(
                collective_id=0, has_side_effects=True, vmem_limit_bytes=66000000
            ),
        )(warped, fixed, fine, coarse)
        held = [pltpu.with_memory_space_constraint(h, memory_space=pltpu.VMEM) for h in held]
        return pl.pallas_call(
            write_out,
            out_shape=(jax.ShapeDtypeStruct(fine.shape, f32),
                       jax.ShapeDtypeStruct(coarse.shape, f32)),
            in_specs=[vmem] * 2,
            out_specs=(vmem, vmem),
        )(*held)

    in_specs = (P("gx", "gy", "gz"), P("gx", "gy", "gz"), P(None, "gx", "gy", "gz"), P())
    out_specs = (P(None, "gx", "gy", "gz"), P())
    return jax.shard_map(
        step, mesh=mesh, in_specs=in_specs, out_specs=out_specs, check_vma=False
    )
```

```python
import functools

import jax
import jax.numpy as jnp
from jax import lax
from jax.experimental import pallas as pl
from jax.experimental.pallas import tpu as pltpu
from jax.sharding import PartitionSpec as P

SPF = 8
SPC = 32
BEND = 0.01
MESH = pl.DeviceIdType.MESH
f32 = jnp.float32
bf16 = jnp.bfloat16
AXES = ("gx", "gy", "gz")
SIDES = (0, 1)
AROUND = [(dx, dy) for dx in (-1, 0, 1) for dy in (-1, 0, 1) if dx or dy]


def dot(a, b):
    return jnp.dot(a, b, preferred_element_type=f32)


def spline(t):
    m = jnp.abs(t)
    inner = 2.0 / 3.0 - m * m + 0.5 * m * m * m
    r = jnp.maximum(2.0 - m, 0.0)
    outer = r * r * r * (1.0 / 6.0)
    return jnp.where(m < 1.0, inner, outer)


def weight(voxel, point, spacing):
    scaled = (2 * voxel + 1 - spacing * (2 * point + 1)).astype(f32)
    return spline(scaled * (0.5 / spacing))


def iota(shape, axis):
    return lax.broadcasted_iota(jnp.int32, shape, axis)


def split2(value):
    high = value.astype(bf16)
    return high, (value - high.astype(f32)).astype(bf16)


def split3(value):
    high = value.astype(bf16)
    rest = value - high.astype(f32)
    mid = rest.astype(bf16)
    return high, mid, (rest - mid.astype(f32)).astype(bf16)


def same(out, inp):
    return jnp.where(out == inp, 1.0, 0.0).astype(f32)


def diff1(out, inp):
    d = jnp.abs(out - inp)
    return jnp.where(d == 0, -2.0, jnp.where(d == 1, 1.0, 0.0)).astype(f32)


def diff2(out, inp, count):
    d = jnp.abs(out - inp)
    edge = (inp == 0) | (inp == count - 1)
    centre = jnp.where(edge, 5.0, 6.0)
    return jnp.where(
        d == 0, centre, jnp.where(d == 1, -4.0, jnp.where(d == 2, 1.0, 0.0))
    ).astype(f32)


def cross(ref, x, rows):
    first, count = rows
    here = ref[x, first:first + count]
    return (ref[x - 1, first:first + count] + ref[x + 1, first:first + count]
            + ref[x, first - 1:first - 1 + count] + ref[x, first + 1:first + 1 + count]
            - 4.0 * here), here


def kernel(sizes, w_hbm, f_hbm, fc_hbm, cc_hbm, fo_ref, co_ref,
           w_v, f_v, fc_ref, cc_ref, s_v, ysend, yrecv, zsend, zrecv, dz_v,
           wf_v, wc_v, wy_v, wq_v, wx_v, wz_v, wh_v, fh_v, fl_v,
           accf, accc, pad_v, mid_v, bend_v, padc_v, midc_v, bendc_v,
           part_v, zm_v, zg_v, zt_v, g_v, xm_v, ym_v, xg_v, yg_v, cg_v,
           cz_v, cp_v,
           load_sem, small_sem, hs_sem, hr_sem, ys_sem, yr_sem,
           ms_sem, mr_sem, as_sem, ar_sem, cs_sem, cr_sem, ps_sem, pr_sem):
    nx, ny, nz = sizes
    me = [lax.axis_index(a) for a in AXES]
    SX, SY, SZ = w_v.shape
    PX, PY, PZ = SX // SPF, SY // SPF, SZ // SPF
    KX, KY, KZ = cc_ref.shape[1:]
    EX, QE = PX + 4, PY + 8
    XC, QC = accc.shape[:2]
    cells = SX // SPF
    per = SPC // SPF
    lanes = 3 * SZ
    NF, NC = EX * QE, XC * QC
    LW = 128
    has = [(me[k] > 0, me[k] < sizes[k] - 1) for k in range(3)]

    small = (pltpu.make_async_copy(fc_hbm, fc_ref, small_sem.at[0]),
             pltpu.make_async_copy(cc_hbm, cc_ref, small_sem.at[1]))
    for copy in small:
        copy.start()
    loads = []
    for c in range(cells):
        part = pl.ds(c * SPF, SPF)
        loads.append((
            pltpu.make_async_copy(w_hbm.at[part], w_v.at[part], load_sem.at[0, c]),
            pltpu.make_async_copy(f_hbm.at[part], f_v.at[part], load_sem.at[1, c]),
        ))
    order = [0, cells - 1] + list(range(1, cells - 1))
    for c in order:
        loads[c][0].start()
        loads[c][1].start()

    barrier = pltpu.get_barrier_semaphore()
    total = 0
    plane = [(ox, oy) for ox in range(nx) for oy in range(ny) if ox or oy]

    def in_plane(ox, oy):
        return {"gx": lax.rem(me[0] + ox, nx), "gy": lax.rem(me[1] + oy, ny)}

    for d in range(1, nz):
        pl.semaphore_signal(
            barrier, inc=1, device_id={"gz": lax.rem(me[2] + d, nz)}, device_id_type=MESH)
        total += 1
    for ox, oy in plane:
        pl.semaphore_signal(barrier, inc=1, device_id=in_plane(ox, oy), device_id_type=MESH)
        total += 1

    s_v[2:SX + 2, 0:8, :] = jnp.zeros((SX, 8, SZ), f32)
    s_v[2:SX + 2, 8 + SY:16 + SY, :] = jnp.zeros((SX, 8, SZ), f32)
    accf[...] = jnp.zeros(accf.shape, f32)
    accc[...] = jnp.zeros(accc.shape, f32)
    pad_v[...] = jnp.zeros(pad_v.shape, f32)
    mid_v[...] = jnp.zeros(mid_v.shape, f32)
    padc_v[...] = jnp.zeros(padc_v.shape, f32)
    midc_v[...] = jnp.zeros(midc_v.shape, f32)
    zt_v[...] = jnp.zeros(zt_v.shape, f32)
    dz_v[...] = jnp.zeros(dz_v.shape, f32)
    zsend[...] = jnp.zeros(zsend.shape, f32)
    xpad = (pl.ds(0, 2), pl.ds(SX + 2, 2))

    def zero(ref, index):
        ref[index] = jnp.zeros(ref.at[index].shape, f32)

    for side in SIDES:
        @pl.when(jnp.logical_not(has[0][side]))
        def _(side=side):
            zero(s_v, (xpad[side], slice(8, 8 + SY)))
            zero(xg_v, side)
            for other in SIDES:
                zero(cg_v, (side, other))

        @pl.when(jnp.logical_not(has[1][side]))
        def _(side=side):
            zero(yrecv, side)
            zero(yg_v, side)
            for other in SIDES:
                zero(cg_v, (other, side))

        @pl.when(jnp.logical_not(has[2][side]))
        def _(side=side):
            zero(zrecv, side)
            zero(zg_v, side)

    def edge_row(row):
        return jnp.where(row < PY, row, jnp.where(row < PY + 2, row - PY - 2,
                         jnp.where(row < PY + 4, row - 2, row + 8 * PY)))

    def put(ref, index, value):
        high, low = split2(value)
        ref[(0,) + index] = high
        ref[(1,) + index] = low

    KV = SPF * SY
    cols = iota((QE, KV), 1)
    along_y = weight(cols % SY, edge_row(iota((QE, KV), 0)), SPF)
    along_x = weight(iota((8, KV), 1) // SY, iota((8, KV), 0) - 2, SPF)
    for p in range(5):
        put(wf_v, (slice(p * QE, (p + 1) * QE),), along_y * along_x[p:p + 1])
    rows, cols = iota((4 * QC, KV), 0), iota((4 * QC, KV), 1)
    along_y = weight(cols % SY + me[1] * SY, rows % QC, SPC)
    for ph in range(per):
        first = -2 if ph < per // 2 else -1
        along_x = weight(cols // SY + ph * SPF, rows // QC + first, SPC)
        high, low = split2(along_x * along_y)
        wc_v[ph, 0] = high
        wc_v[ph, 1] = low

    KH = 4 * SX
    place = (iota((16, KH), 1) // SX)
    yat = jnp.where(place < 2, place, SY - 4 + place)
    along_y = weight(yat, edge_row(iota((16, KH), 0)), SPF)
    along_x = weight(iota((16, KH), 1) % SX, iota((16, KH), 0) - 2, SPF)
    for p in range(EX):
        put(wy_v, (slice(p * QE, (p + 1) * QE),), along_y * along_x[p:p + 1])
    rows, cols = iota((NC, KH), 0), iota((NC, KH), 1)
    place = cols // SX
    yat = jnp.where(place < 2, place, SY - 4 + place)
    put(wy_v, (slice(NF, NF + NC),), weight(cols % SX, rows // QC - 2, SPC)
        * weight(yat + me[1] * SY, rows % QC, SPC))

    KP = 2 * SZ
    rows, cols = iota((QE, SY), 0), iota((QE, SY), 1)
    put(wq_v, (slice(0, QE),), weight(cols, edge_row(rows), SPF))
    rows, cols = iota((QC, SY), 0), iota((QC, SY), 1)
    put(wq_v, (slice(QE, QE + QC),), weight(cols + me[1] * SY, rows, SPC))
    col = iota((EX, KP), 1)
    xat = jnp.where(col < SZ, (col + SZ - 2) % SZ, col % SZ) // 2
    wx_v[0:EX] = weight(xat, iota((EX, KP), 0) - 2, SPF)
    wx_v[EX:EX + XC] = weight(xat[0:XC], iota((XC, KP), 0) - 2, SPC)

    def fine_lane(l):
        e = (l - 3 * PZ) % 8
        centre = l < 3 * PZ
        known = centre | ((l < 3 * PZ + 16) & (e < 6))
        comp = jnp.where(centre, l // PZ, jnp.where(known, e // 2, 3))
        point = jnp.where(centre, l % PZ, jnp.where(l < 3 * PZ + 8, e % 2 - 2, PZ + e % 2))
        return comp, point

    def both_levels(z):
        l = iota(z.shape, 1)[:, 0:LW]
        z = z[:, 0:LW]
        comp, point = fine_lane(l)
        fine = weight(z, point, SPF) * (SPF ** -1.5 / 24.0)
        ccomp = l // KZ
        coarse = weight(z + me[2] * SZ, l % KZ, SPC) * (SPC ** -1.5 / 24.0)
        return jnp.concatenate([comp, ccomp], 1), jnp.concatenate([fine, coarse], 1)

    comp, value = both_levels(iota((SZ, 2 * LW), 0))
    high, low = split2(value)
    high, low = high.astype(f32), low.astype(f32)
    for a in range(3):
        part = slice(a * SZ, (a + 1) * SZ)
        wz_v[0, part] = jnp.where(comp == a, high, 0.0).astype(bf16)
        wz_v[1, part] = jnp.where(comp == a, low, 0.0).astype(bf16)
    row = iota((8, 2 * LW), 0)
    comp, value = both_levels(jnp.where(row < 2, row, SZ - 4 + row))
    value = jnp.where(comp == 2, value, 0.0)
    odd = iota((SZ, 2 * LW), 0) % 2 == 1
    for side in SIDES:
        part = slice(side * SZ, (side + 1) * SZ)
        put(wh_v, (part,), jnp.where(odd, value[2 * side + 1:2 * side + 2],
                                     value[2 * side:2 * side + 1]))

    for copy in small:
        copy.wait()

    def spread(ref, a, count, width, matrix):
        block = ref[a].reshape(count, width)
        return sum(dot(part, matrix) for part in split3(block))

    zin, l = iota((PZ, LW), 0), iota((PZ, LW), 1)
    comp, point = fine_lane(l)
    oz = me[2] * PZ
    shares = 0.0
    for a in range(3):
        m = jnp.concatenate([same(point, zin), 2.0 * diff1(point, zin),
                             diff2(point + oz, zin + oz, PZ * nz)], 1)
        ok = jnp.concatenate([comp == a] * 3, 1)
        shares = shares + spread(fc_ref, a, PX * PY, PZ, jnp.where(ok, m, 0.0).astype(bf16))
    shares = shares.reshape(PX, PY, 3 * LW)
    pad_v[3:3 + PX, 8:8 + PY, :] = shares[:, :, 0:LW]
    inside = iota((PY + 8, LW), 0) - 4 + me[1] * PY
    inside = (inside >= 0) & (inside < PY * ny)
    for p in range(-1, PX + 1):
        u, _ = cross(pad_v, 3 + p, (4, PY + 8))
        keep = inside & (me[0] * PX + p >= 0) & (me[0] * PX + p < PX * nx)
        mid_v[3 + p, 4:12 + PY] = jnp.where(keep, u, 0.0)
    mid_v[3:3 + PX, 8:8 + PY, :] = mid_v[3:3 + PX, 8:8 + PY, :] + shares[:, :, LW:2 * LW]
    row = iota((PY, LW), 0)
    for p in range(-2, PX + 2):
        v = [cross(mid_v, 3 + p, (first, PY))[0] for first in (8, 6, 6 + PY)]
        centre = v[0]
        if 0 <= p < PX:
            centre = centre + shares[p, :, 2 * LW:3 * LW]
        bend_v[2 + p, 0:PY] = centre * BEND
        bend_v[2 + p, PY:2 * PY] = jnp.where(
            row < 2, v[1], jnp.where(row < 4, v[2], 0.0)) * BEND

    pieces = ys_sem.shape[1]
    each = SX // pieces

    def neighbour_copy(k, side, src, dst, send, recv):
        other = me[k] - 1 if side == 0 else me[k] + 1
        return pltpu.make_async_remote_copy(
            src_ref=src, dst_ref=dst, send_sem=send, recv_sem=recv,
            device_id={AXES[k]: other}, device_id_type=MESH,
        )

    def halo(k, side, piece=0):
        if k == 1:
            part = pl.ds(piece * each, each)
            return neighbour_copy(
                k, side, ysend.at[side, :, part], yrecv.at[1 - side, :, part],
                ys_sem.at[side, piece], yr_sem.at[1 - side, piece])
        if k == 0:
            src = s_v.at[pl.ds(2 if side == 0 else SX, 2), pl.ds(8, SY), :]
            dst = s_v.at[pl.ds(SX + 2 if side == 0 else 0, 2), pl.ds(8, SY), :]
        else:
            src, dst = zsend.at[side], zrecv.at[1 - side]
        return neighbour_copy(k, side, src, dst, hs_sem.at[k, side], hr_sem.at[k, 1 - side])

    def start_halo(k, side, piece=0):
        @pl.when(has[k][side])
        def _():
            halo(k, side, piece).start()

    def wait_halo(k):
        for side in SIDES:
            for piece in range(pieces if k == 1 else 1):
                @pl.when(has[k][side])
                def _(side=side, piece=piece):
                    halo(k, side, piece).wait_send()

                @pl.when(has[k][1 - side])
                def _(side=side, piece=piece):
                    halo(k, side, piece).wait_recv()

    tile_lane = iota((8, SZ), 1)
    srows = s_v.reshape((SX + 4) * (SY + 16), SZ)
    drows = w_v.reshape(SX * SY, SZ)

    def sums(c):
        for copy in loads[c]:
            copy.wait()
        for y in range(0, SY, 8):
            rows = slice(y, y + 8)
            packs = [zsend[0, rows], zsend[1, rows], dz_v[0, rows], dz_v[1, rows]]
            for x in range(c * SPF, (c + 1) * SPF):
                w, f = w_v[x, rows], f_v[x, rows]
                s, d = w + f, w - f
                s_v[x + 2, 8 + y:16 + y] = s
                w_v[x, rows] = d
                shift = (2 * x + 2) % SZ
                s, d = pltpu.roll(s, shift, 1), pltpu.roll(d, shift, 1)
                low = tile_lane // 2 == (x + 1) % (SZ // 2)
                high = tile_lane // 2 == x
                packs = [jnp.where(low, s, packs[0]), jnp.where(high, s, packs[1]),
                         jnp.where(low, d, packs[2]), jnp.where(high, d, packs[3])]
            zsend[0, rows], zsend[1, rows], dz_v[0, rows], dz_v[1, rows] = packs

    def yfaces(piece):
        for side in SIDES:
            for k in range(2):
                y = k if side == 0 else SY - 2 + k
                ysend[side, k, pl.ds(piece * each, each)] = srows[
                    pl.ds((piece * each + 2) * (SY + 16) + 8 + y, each, stride=SY + 16), :]
            start_halo(1, side, piece)

    def forces(i, slot):
        for xx in range(SPF):
            x = i * SPF + xx
            d = w_v[x]
            s = s_v[x + 2, 8:8 + SY, :]
            gx = (s_v[x, 8:8 + SY, :] - s_v[x + 4, 8:8 + SY, :]
                  + 8.0 * (s_v[x + 3, 8:8 + SY, :] - s_v[x + 1, 8:8 + SY, :]))
            gy = (s_v[x + 2, 6:6 + SY, :] - s_v[x + 2, 10:10 + SY, :]
                  + 8.0 * (s_v[x + 2, 9:9 + SY, :] - s_v[x + 2, 7:7 + SY, :]))
            gz = (pltpu.roll(s, 2, 1) - pltpu.roll(s, SZ - 2, 1)
                  + 8.0 * (pltpu.roll(s, SZ - 1, 1) - pltpu.roll(s, 1, 1)))
            for a, g in enumerate((gx, gy, gz)):
                high, low = split2(g * d)
                fh_v[slot, xx * SY:(xx + 1) * SY, a * SZ:(a + 1) * SZ] = high
                fl_v[slot, xx * SY:(xx + 1) * SY, a * SZ:(a + 1) * SZ] = low

    lane = iota((SY, SZ), 1)

    def gather(i, slot):
        k, ph = divmod(i, per)
        many = 5 * QE + 4 * QC
        weights = jnp.concatenate([wf_v[0], wc_v[ph, 0], wf_v[1], wc_v[ph, 1]], axis=0)
        both = dot(weights, fh_v[slot])
        out = both[:many] + both[many:] + dot(weights[:many], fl_v[slot])
        accf[i:i + 5] += out[:5 * QE].reshape(5, QE, lanes)
        at = k + (1 if ph >= per // 2 else 0)
        accc[at:at + 4] += out[5 * QE:].reshape(4, QC, lanes)

    summed, sent = set(), set()

    def run_sums(c):
        sums(c)
        summed.add(c)

    def run_faces():
        for piece in range(pieces):
            inside = range(piece * each // SPF, (piece + 1) * each // SPF)
            if piece not in sent and all(n in summed for n in inside):
                sent.add(piece)
                yfaces(piece)

    for c in order[:3]:
        run_sums(c)
    pl.semaphore_wait(barrier, total)
    start_halo(0, 0)
    start_halo(0, 1)
    run_faces()
    for c in order[3:]:
        run_sums(c)
        run_faces()
    start_halo(2, 0)
    start_halo(2, 1)

    turn = list(range(1, cells - 1)) + [0, cells - 1]
    forces(turn[0], 0)
    for n, i in enumerate(turn):
        if n + 1 < cells:
            if turn[n + 1] == 0:
                wait_halo(0)
            forces(turn[n + 1], (n + 1) % 2)
        gather(i, n % 2)

    wait_halo(1)
    wait_halo(2)
    adds = []
    for side in SIDES:
        h0, h1 = yrecv[side, 0], yrecv[side, 1]
        g = (h0 - 8.0 * h1, h1) if side == 0 else (-h0, 8.0 * h0 - h1)
        for k in range(2):
            y = k if side == 0 else SY - 2 + k
            adds.append(g[k] * drows[pl.ds(y, SX, stride=SY), :])
    high, low = split2(jnp.concatenate(adds, 0))
    weights = wy_v[0]
    added = dot(weights, high) + dot(wy_v[1], high) + dot(weights, low)

    even = lane % 2 == 0
    hl, hh = zrecv[0] - zsend[1], zrecv[1] - zsend[0]
    cl = jnp.where(even, hl - 8.0 * pltpu.roll(hl, SZ - 1, 1), hl)
    ch = jnp.where(even, -hh, 8.0 * pltpu.roll(hh, 1, 1) - hh)
    fz = jnp.concatenate([pltpu.roll(cl, 2, 1) * dz_v[0],
                          pltpu.roll(ch, SZ - 2, 1) * dz_v[1]], 1)
    high, low = split2(fz)
    g = dot(wq_v[0], high) + dot(wq_v[1], high) + dot(wq_v[0], low)
    blocks = [g[0:QE] * wx_v[p:p + 1] for p in range(EX)]
    blocks += [g[QE:QE + QC] * wx_v[EX + p:EX + p + 1] for p in range(XC)]
    hhigh, hlow = split2(jnp.concatenate(blocks, 0))

    table = jnp.concatenate([accf[...].reshape(NF, lanes), accc[...].reshape(NC, lanes)], 0)
    table = jnp.concatenate(
        [table[:, 0:SZ], table[:, SZ:2 * SZ] + added, table[:, 2 * SZ:]], 1)
    high, low = split2(table)
    whole = (dot(high, wz_v[0]) + dot(high, wz_v[1]) + dot(low, wz_v[0])
             + dot(hhigh, wh_v[0]) + dot(hhigh, wh_v[1]) + dot(hlow, wh_v[0]))

    cz_v[me[2]] = whole[NF:NF + NC, LW:2 * LW].reshape(XC, QC, LW)

    def coarse_z(d, slot):
        return pltpu.make_async_remote_copy(
            src_ref=cz_v.at[slot], dst_ref=cz_v.at[slot],
            send_sem=cs_sem.at[d], recv_sem=cr_sem.at[d],
            device_id={"gz": lax.rem(me[2] + d, nz)}, device_id_type=MESH)

    for d in range(1, nz):
        coarse_z(d, me[2]).start()

    fine = whole[0:NF, 0:LW] + bend_v[...].reshape(NF, LW)
    part_v[...] = fine
    tall = jnp.concatenate([fine, jnp.zeros((2 * LW - NF, LW), f32)], 0).T
    for side in SIDES:
        zm_v[side] = tall[3 * PZ + 8 * side:3 * PZ + 8 * side + 8]

    def fine_z(side):
        return neighbour_copy(2, side, zm_v.at[side], zg_v.at[1 - side],
                              ms_sem.at[side], mr_sem.at[1 - side])

    for side in SIDES:
        @pl.when(has[2][side])
        def _(side=side):
            fine_z(side).start()

    zin, l = iota((KZ, LW), 0), iota((KZ, LW), 1)
    shares = 0.0
    for a in range(3):
        m = jnp.concatenate([same(l % KZ, zin), 2.0 * diff1(l % KZ, zin),
                             diff2(l % KZ, zin, KZ)], 1)
        ok = jnp.concatenate([l // KZ == a] * 3, 1)
        shares = shares + spread(cc_ref, a, KX * KY, KZ, jnp.where(ok, m, 0.0).astype(bf16))
    shares = shares.reshape(KX, KY, 3 * LW)
    padc_v[1:1 + KX, 8:8 + KY, :] = shares[:, :, 0:LW]
    for p in range(KX):
        midc_v[1 + p, 8:8 + KY] = (
            cross(padc_v, 1 + p, (8, KY))[0] + shares[p, :, LW:2 * LW])
    for p in range(KX):
        bendc_v[p] = (cross(midc_v, 1 + p, (8, KY))[0] + shares[p, :, 2 * LW:]) * BEND

    for d in range(1, nz):
        coarse_z(d, me[2]).wait_send()
        coarse_z(d, lax.rem(me[2] + nz - d, nz)).wait_recv()
    block = cz_v[0]
    for n in range(1, nz):
        block = block + cz_v[n]

    cp_v[me[0], me[1]] = block

    def coarse_plane(ox, oy, sx, sy):
        return pltpu.make_async_remote_copy(
            src_ref=cp_v.at[sx, sy], dst_ref=cp_v.at[sx, sy],
            send_sem=ps_sem.at[ox, oy], recv_sem=pr_sem.at[ox, oy],
            device_id=in_plane(ox, oy), device_id_type=MESH)

    for ox, oy in plane:
        coarse_plane(ox, oy, me[0], me[1]).start()

    for side in SIDES:
        @pl.when(has[2][side])
        def _(side=side):
            fine_z(side).wait_send()

        @pl.when(has[2][1 - side])
        def _(side=side):
            fine_z(side).wait_recv()
    for a in range(3):
        zt_v[a * PZ:a * PZ + 2] = zg_v[0, 2 * a:2 * a + 2]
        zt_v[(a + 1) * PZ - 2:(a + 1) * PZ] = zg_v[1, 2 * a:2 * a + 2]
    g_v[...] = (part_v[...] + zt_v[...].T[0:NF]).reshape(EX, QE, LW)
    for side in SIDES:
        at = 0 if side == 0 else PX + 2
        xm_v[side] = g_v[at:at + 2, 0:PY]
    ym_v[...] = g_v[:, PY:PY + 4]

    def fine_plane(dx, dy):
        xs, ys = (0 if dx > 0 else 1), (0 if dy > 0 else 1)
        if dy == 0:
            src, dst = xm_v.at[1 - xs], xg_v.at[xs]
        elif dx == 0:
            src, dst = ym_v.at[pl.ds(2, PX)], yg_v.at[ys]
        else:
            src = ym_v.at[pl.ds(0 if dx < 0 else PX + 2, 2)]
            dst = cg_v.at[xs, ys]
        return pltpu.make_async_remote_copy(
            src_ref=src, dst_ref=dst,
            send_sem=as_sem.at[dx + 1, dy + 1], recv_sem=ar_sem.at[dx + 1, dy + 1],
            device_id={"gx": me[0] + dx, "gy": me[1] + dy}, device_id_type=MESH)

    def there(dx, dy):
        x, y = me[0] + dx, me[1] + dy
        return (x >= 0) & (x < nx) & (y >= 0) & (y < ny)

    for dx, dy in AROUND:
        @pl.when(there(dx, dy))
        def _(dx=dx, dy=dy):
            fine_plane(dx, dy).start()
    for dx, dy in AROUND:
        @pl.when(there(dx, dy))
        def _(dx=dx, dy=dy):
            fine_plane(dx, dy).wait_send()

        @pl.when(there(-dx, -dy))
        def _(dx=dx, dy=dy):
            fine_plane(dx, dy).wait_recv()

    row = iota((PY, LW), 0)
    for p in range(PX):
        out = g_v[2 + p, 0:PY]
        low, high = yg_v[0, p], yg_v[1, p]
        for side in SIDES:
            q = p if side == 0 else p - (PX - 2)
            if 0 <= q < 2:
                out = out + xg_v[side, q]
                low, high = low + cg_v[side, 0, q], high + cg_v[side, 1, q]
        fill = jnp.zeros((PY - 4, LW), f32)
        low = pltpu.roll(jnp.concatenate([low, fill], 0), PY - 2, 0)
        high = pltpu.roll(jnp.concatenate([high, fill], 0), PY - 2, 0)
        out = out + jnp.where(row < 2, low, jnp.where(row >= PY - 2, high, 0.0))
        for a in range(3):
            fo_ref[a, p] = (out if a == 0 else pltpu.roll(out, LW - a * PZ, 1))[:, 0:PZ]

    for ox, oy in plane:
        coarse_plane(ox, oy, me[0], me[1]).wait_send()
        coarse_plane(ox, oy, lax.rem(me[0] + nx - ox, nx),
                     lax.rem(me[1] + ny - oy, ny)).wait_recv()
    for p in range(KX):
        out = bendc_v[p]
        for ix in range(nx):
            q = p + 2 - ix * (SX // SPC)
            if 0 <= q < XC:
                for iy in range(ny):
                    out = out + cp_v[ix, iy, q]
        for a in range(3):
            co_ref[a, p] = (out if a == 0 else pltpu.roll(out, LW - a * KZ, 1))[:, 0:KZ]


def write_out(f_ref, c_ref, fo_ref, co_ref):
    fo_ref[...] = f_ref[...]
    co_ref[...] = c_ref[...]


def solution(mesh):
    sizes = tuple(mesh.shape[a] for a in AXES)

    def step(warped, fixed, fine, coarse):
        SX, SY, SZ = warped.shape
        PX, PY, PZ = SX // SPF, SY // SPF, SZ // SPF
        KX, KY, KZ = coarse.shape[1:]
        nx, ny, nz = sizes
        EX, QE = PX + 4, PY + 8
        XC, QC = SX // SPC + 4, KY
        KV = SPF * SY
        NF, NC, LW = EX * QE, XC * QC, 128
        vmem = pl.BlockSpec(memory_space=pltpu.VMEM)
        hbm = pl.BlockSpec(memory_space=pltpu.HBM)
        V = pltpu.VMEM
        D = pltpu.SemaphoreType.DMA
        held = pl.pallas_call(
            functools.partial(kernel, sizes),
            out_shape=(pltpu.VMEM(fine.shape, f32), pltpu.VMEM(coarse.shape, f32)),
            in_specs=[hbm] * 4,
            out_specs=(vmem, vmem),
            scratch_shapes=[
                V((SX, SY, SZ), f32), V((SX, SY, SZ), f32),
                V((3, PX, PY, PZ), f32), V(coarse.shape, f32),
                V((SX + 4, SY + 16, SZ), f32),
                V((2, 2, SX, SZ), f32), V((2, 2, SX, SZ), f32),
                V((2, SY, SZ), f32), V((2, SY, SZ), f32), V((2, SY, SZ), f32),
                V((2, 5 * QE, KV), bf16), V((SPC // SPF, 2, 4 * QC, KV), bf16),
                V((2, NF + NC, 4 * SX), bf16), V((2, QE + QC, SY), bf16),
                V((EX + XC, 2 * SZ), f32),
                V((2, 3 * SZ, 2 * LW), bf16), V((2, 2 * SZ, 2 * LW), bf16),
                V((2, KV, 3 * SZ), bf16), V((2, KV, 3 * SZ), bf16),
                V((EX, QE, 3 * SZ), f32), V((XC, QC, 3 * SZ), f32),
                V((PX + 6, PY + 16, LW), f32), V((PX + 6, PY + 16, LW), f32),
                V((EX, QE, LW), f32),
                V((KX + 2, KY + 16, LW), f32), V((KX + 2, KY + 16, LW), f32),
                V((KX, KY, LW), f32),
                V((NF, LW), f32), V((2, 8, 2 * LW), f32), V((2, 8, 2 * LW), f32),
                V((LW, 2 * LW), f32), V((EX, QE, LW), f32),
                V((2, 2, PY, LW), f32), V((EX, 4, LW), f32),
                V((2, 2, PY, LW), f32), V((2, PX, 4, LW), f32), V((2, 2, 2, 4, LW), f32),
                V((nz, XC, QC, LW), f32), V((nx, ny, XC, QC, LW), f32),
                D((2, SX // SPF)), D((2,)), D((3, 2)), D((3, 2)), D((2, 4)), D((2, 4)),
                D((2,)), D((2,)), D((3, 3)), D((3, 3)), D((nz,)), D((nz,)),
                D((nx, ny)), D((nx, ny)),
            ],
            compiler_params=pltpu.CompilerParams(
                collective_id=0, has_side_effects=True, vmem_limit_bytes=64000000
            ),
        )(warped, fixed, fine, coarse)
        held = [pltpu.with_memory_space_constraint(h, memory_space=pltpu.VMEM) for h in held]
        return pl.pallas_call(
            write_out,
            out_shape=(jax.ShapeDtypeStruct(fine.shape, f32),
                       jax.ShapeDtypeStruct(coarse.shape, f32)),
            in_specs=[vmem] * 2,
            out_specs=(vmem, vmem),
        )(*held)

    in_specs = (P("gx", "gy", "gz"), P("gx", "gy", "gz"), P(None, "gx", "gy", "gz"), P())
    out_specs = (P(None, "gx", "gy", "gz"), P())
    return jax.shard_map(
        step, mesh=mesh, in_specs=in_specs, out_specs=out_specs, check_vma=False
    )
```

```python
import functools

import jax
import jax.numpy as jnp
from jax import lax
from jax.experimental import pallas as pl
from jax.experimental.pallas import tpu as pltpu
from jax.sharding import PartitionSpec as P

SPF = 8
SPC = 32
BEND = 0.01
MESH = pl.DeviceIdType.MESH
f32 = jnp.float32
bf16 = jnp.bfloat16
AXES = ("gx", "gy", "gz")
SIDES = (0, 1)
BEFORE = 3
STEPS = (-1, 0, 1)
AROUND = sorted(
    ((dx, dy, dz) for dx in STEPS for dy in STEPS for dz in STEPS if dx or dy or dz),
    key=lambda d: -sum(map(abs, d)))


def dot(a, b):
    return jnp.dot(a, b, preferred_element_type=f32)


def spline(t):
    m = jnp.abs(t)
    inner = 2.0 / 3.0 - m * m + 0.5 * m * m * m
    r = jnp.maximum(2.0 - m, 0.0)
    outer = r * r * r * (1.0 / 6.0)
    return jnp.where(m < 1.0, inner, outer)


def weight(voxel, point, spacing):
    scaled = (2 * voxel + 1 - spacing * (2 * point + 1)).astype(f32)
    return spline(scaled * (0.5 / spacing))


def iota(shape, axis):
    return lax.broadcasted_iota(jnp.int32, shape, axis)


def split2(value):
    high = value.astype(bf16)
    return high, (value - high.astype(f32)).astype(bf16)


def split3(value):
    high = value.astype(bf16)
    rest = value - high.astype(f32)
    mid = rest.astype(bf16)
    return high, mid, (rest - mid.astype(f32)).astype(bf16)


def same(out, inp):
    return jnp.where(out == inp, 1.0, 0.0).astype(f32)


def diff1(out, inp):
    d = jnp.abs(out - inp)
    return jnp.where(d == 0, -2.0, jnp.where(d == 1, 1.0, 0.0)).astype(f32)


def diff2(out, inp, count):
    d = jnp.abs(out - inp)
    edge = (inp == 0) | (inp == count - 1)
    centre = jnp.where(edge, 5.0, 6.0)
    return jnp.where(
        d == 0, centre, jnp.where(d == 1, -4.0, jnp.where(d == 2, 1.0, 0.0))
    ).astype(f32)


def cross(ref, x, rows):
    first, count = rows
    here = ref[x, first:first + count]
    return (ref[x - 1, first:first + count] + ref[x + 1, first:first + count]
            + ref[x, first - 1:first - 1 + count] + ref[x, first + 1:first + 1 + count]
            - 4.0 * here), here


def kernel(sizes, w_hbm, f_hbm, fc_hbm, cc_hbm, fo_ref, co_ref,
           w_v, f_v, fc_ref, cc_ref, s_v, ysend, yrecv, zsend, zrecv, dz_v,
           wf_v, wc_v, wy_v, wq_v, wx_v, wz_v, wh_v, fh_v, fl_v,
           accf, accc, pad_v, mid_v, bend_v, padc_v, midc_v,
           zm_v, zg_v, zt_v, xm_v, ym_v, xg_v, yg_v, cg_v, all_v,
           load_sem, small_sem, hs_sem, hr_sem, ys_sem, yr_sem,
           as_sem, ar_sem, cs_sem, cr_sem, in_sem):
    nx, ny, nz = sizes
    me = [lax.axis_index(a) for a in AXES]
    SX, SY, SZ = w_v.shape
    PX, PY, PZ = SX // SPF, SY // SPF, SZ // SPF
    KX, KY, KZ = cc_ref.shape[1:]
    EX, QE = PX + 4, PY + 8
    QC, XR = accc.shape[:2]
    CX, CZ = SX // SPC, SZ // SPC
    XC, ZC = CX + 4, CZ + 4
    GL = 32
    PG = 128 // GL
    cells = SX // SPF
    per = SPC // SPF
    lanes = 3 * SZ
    NF, NC = EX * QE, QC * XR
    LW = 128
    has = [(me[k] > 0, me[k] < sizes[k] - 1) for k in range(3)]

    small = (pltpu.make_async_copy(fc_hbm, fc_ref, small_sem.at[0]),
             pltpu.make_async_copy(cc_hbm, cc_ref, small_sem.at[1]))
    for copy in small:
        copy.start()
    loads = []
    for c in range(cells):
        part = pl.ds(c * SPF, SPF)
        loads.append((
            pltpu.make_async_copy(w_hbm.at[part], w_v.at[part], load_sem.at[0, c]),
            pltpu.make_async_copy(f_hbm.at[part], f_v.at[part], load_sem.at[1, c]),
        ))
    groups = [(0, 1), (cells - 2, cells - 1)]
    groups += [(c, c + 1) for c in range(2, cells - 2, 2)]
    for c in sum(groups, ()):
        loads[c][0].start()
        loads[c][1].start()

    for at in (0, SX + 2):
        s_v[at:at + 2, 8:8 + SY, :] = jnp.zeros((2, SY, SZ), f32)
    for ref in (yrecv, zrecv, xg_v, yg_v, cg_v, zg_v):
        ref[...] = jnp.zeros(ref.shape, f32)

    barrier = pltpu.get_barrier_semaphore()
    total = 0
    plane = [(ox, oy) for ox in range(nx) for oy in range(ny) if ox or oy]

    def in_plane(ox, oy):
        return {"gx": lax.rem(me[0] + ox, nx), "gy": lax.rem(me[1] + oy, ny)}

    for d in range(1, nz):
        pl.semaphore_signal(
            barrier, inc=1, device_id={"gz": lax.rem(me[2] + d, nz)}, device_id_type=MESH)
        total += 1
    for ox, oy in plane:
        pl.semaphore_signal(barrier, inc=1, device_id=in_plane(ox, oy), device_id_type=MESH)
        total += 1

    s_v[2:SX + 2, 0:8, :] = jnp.zeros((SX, 8, SZ), f32)
    s_v[2:SX + 2, 8 + SY:16 + SY, :] = jnp.zeros((SX, 8, SZ), f32)
    for ref in (accf, accc, pad_v, mid_v, padc_v, midc_v, zt_v, dz_v, zsend):
        ref[...] = jnp.zeros(ref.shape, f32)

    def edge_row(row):
        return jnp.where(row < PY, row, jnp.where(row < PY + 2, row - PY - 2,
                         jnp.where(row < PY + 4, row - 2, row + 8 * PY)))

    def put(ref, index, value):
        high, low = split2(value)
        ref[(0,) + index] = high
        ref[(1,) + index] = low

    KV = SPF * SY
    cols = iota((QE, KV), 1)
    along_y = weight(cols % SY, edge_row(iota((QE, KV), 0)), SPF)
    along_x = weight(iota((8, KV), 1) // SY, iota((8, KV), 0) - 2, SPF)
    for p in range(5):
        put(wf_v, (slice(p * QE, (p + 1) * QE),), along_y * along_x[p:p + 1])
    rows, cols = iota((4 * QC, KV), 0), iota((4 * QC, KV), 1)
    along_y = weight(cols % SY + me[1] * SY, rows // 4, SPC)
    for ph in range(per):
        first = -2 if ph < per // 2 else -1
        along_x = weight(cols // SY + ph * SPF, rows % 4 + first, SPC)
        high, low = split2(along_x * along_y)
        wc_v[ph, 0] = high
        wc_v[ph, 1] = low

    KH = 4 * SX
    place = (iota((16, KH), 1) // SX)
    yat = jnp.where(place < 2, place, SY - 4 + place)
    along_y = weight(yat, edge_row(iota((16, KH), 0)), SPF)
    along_x = weight(iota((16, KH), 1) % SX, iota((16, KH), 0) - 2, SPF)
    turned = list(range(2, 2 + PX)) + [0, 1, PX + 2, PX + 3]
    for n, p in enumerate(turned):
        put(wy_v, (slice(n * QE, (n + 1) * QE),), along_y * along_x[p:p + 1])
    rows, cols = iota((NC, KH), 0), iota((NC, KH), 1)
    place = cols // SX
    yat = jnp.where(place < 2, place, SY - 4 + place)
    put(wy_v, (slice(NF, NF + NC),), weight(cols % SX, rows % XR - 2, SPC)
        * weight(yat + me[1] * SY, rows // XR, SPC))

    KP = 2 * SZ
    rows, cols = iota((QE, SY), 0), iota((QE, SY), 1)
    put(wq_v, (slice(0, QE),), weight(cols, edge_row(rows), SPF))
    rows, cols = iota((QC, SY), 0), iota((QC, SY), 1)
    put(wq_v, (slice(QE, QE + QC),), weight(cols + me[1] * SY, rows, SPC))
    col = iota((EX, KP), 1)
    xat = jnp.where(col < SZ, (col + SZ - 2) % SZ, col % SZ) // 2
    wx_v[0:EX] = weight(xat, iota((EX, KP), 0) - 2, SPF)
    wx_v[EX:EX + XR] = weight(xat[0:XR], iota((XR, KP), 0) - 2, SPC)

    def fine_lane(l):
        e = (l - 3 * PZ) % 8
        centre = l < 3 * PZ
        known = centre | ((l < 3 * PZ + 16) & (e < 6))
        comp = jnp.where(centre, l // PZ, jnp.where(known, e // 2, 3))
        point = jnp.where(centre, l % PZ, jnp.where(l < 3 * PZ + 8, e % 2 - 2, PZ + e % 2))
        return comp, point

    def both_levels(z):
        l = iota(z.shape, 1)[:, 0:LW]
        z = z[:, 0:LW]
        comp, point = fine_lane(l)
        fine = weight(z, point, SPF) * (SPF ** -1.5 / 24.0)
        ccomp = l // ZC
        coarse = weight(z, l % ZC - 2, SPC) * (SPC ** -1.5 / 24.0)
        return jnp.concatenate([comp, ccomp], 1), jnp.concatenate([fine, coarse], 1)

    comp, value = both_levels(iota((SZ, 2 * LW), 0))
    high, low = split2(value)
    high, low = high.astype(f32), low.astype(f32)
    for a in range(3):
        part = slice(a * SZ, (a + 1) * SZ)
        wz_v[0, part] = jnp.where(comp == a, high, 0.0).astype(bf16)
        wz_v[1, part] = jnp.where(comp == a, low, 0.0).astype(bf16)
    row = iota((8, 2 * LW), 0)
    comp, value = both_levels(jnp.where(row < 2, row, SZ - 4 + row))
    value = jnp.where(comp == 2, value, 0.0)
    odd = iota((SZ, 2 * LW), 0) % 2 == 1
    for side in SIDES:
        part = slice(side * SZ, (side + 1) * SZ)
        put(wh_v, (part,), jnp.where(odd, value[2 * side + 1:2 * side + 2],
                                     value[2 * side:2 * side + 1]))

    for copy in small:
        copy.wait()

    def spread(ref, a, count, width, matrix):
        block = ref[a].reshape(count, width)
        return sum(dot(part, matrix) for part in split3(block))

    zin, l = iota((PZ, LW), 0), iota((PZ, LW), 1)
    comp, point = fine_lane(l)
    oz = me[2] * PZ
    shares = 0.0
    for a in range(3):
        m = jnp.concatenate([same(point, zin), 2.0 * diff1(point, zin),
                             diff2(point + oz, zin + oz, PZ * nz)], 1)
        ok = jnp.concatenate([comp == a] * 3, 1)
        shares = shares + spread(fc_ref, a, PX * PY, PZ, jnp.where(ok, m, 0.0).astype(bf16))
    shares = shares.reshape(PX, PY, 3 * LW)
    pad_v[3:3 + PX, 8:8 + PY, :] = shares[:, :, 0:LW]
    inside = iota((PY + 8, LW), 0) - 4 + me[1] * PY
    inside = (inside >= 0) & (inside < PY * ny)
    for p in range(-1, PX + 1):
        u, _ = cross(pad_v, 3 + p, (4, PY + 8))
        keep = inside & (me[0] * PX + p >= 0) & (me[0] * PX + p < PX * nx)
        mid_v[3 + p, 4:12 + PY] = jnp.where(keep, u, 0.0)
    mid_v[3:3 + PX, 8:8 + PY, :] = mid_v[3:3 + PX, 8:8 + PY, :] + shares[:, :, LW:2 * LW]
    row = iota((PY, LW), 0)
    for p in range(-2, PX + 2):
        v = [cross(mid_v, 3 + p, (first, PY))[0] for first in (8, 6, 6 + PY)]
        centre = v[0]
        if 0 <= p < PX:
            centre = centre + shares[p, :, 2 * LW:3 * LW]
        at = turned.index(2 + p)
        bend_v[at, 0:PY] = centre * BEND
        bend_v[at, PY:2 * PY] = jnp.where(
            row < 2, v[1], jnp.where(row < 4, v[2], 0.0)) * BEND

    pieces = ys_sem.shape[1]
    each = SX // pieces

    def neighbour_copy(k, side, src, dst, send, recv):
        other = me[k] - 1 if side == 0 else me[k] + 1
        return pltpu.make_async_remote_copy(
            src_ref=src, dst_ref=dst, send_sem=send, recv_sem=recv,
            device_id={AXES[k]: other}, device_id_type=MESH,
        )

    def halo(k, side, piece=0):
        if k == 1:
            part = pl.ds(piece * each, each)
            return neighbour_copy(
                k, side, ysend.at[side, :, part], yrecv.at[1 - side, :, part],
                ys_sem.at[side, piece], yr_sem.at[1 - side, piece])
        if k == 0:
            src = s_v.at[pl.ds(2 if side == 0 else SX, 2), pl.ds(8, SY), :]
            dst = s_v.at[pl.ds(SX + 2 if side == 0 else 0, 2), pl.ds(8, SY), :]
        else:
            src, dst = zsend.at[side], zrecv.at[1 - side]
        return neighbour_copy(k, side, src, dst, hs_sem.at[k, side], hr_sem.at[k, 1 - side])

    def start_halo(k, side, piece=0):
        @pl.when(has[k][side])
        def _():
            halo(k, side, piece).start()

    def wait_halo(k):
        for side in SIDES:
            for piece in range(pieces if k == 1 else 1):
                @pl.when(has[k][side])
                def _(side=side, piece=piece):
                    halo(k, side, piece).wait_send()

                @pl.when(has[k][1 - side])
                def _(side=side, piece=piece):
                    halo(k, side, piece).wait_recv()

    tile_lane = iota((8, SZ), 1)
    srows = s_v.reshape((SX + 4) * (SY + 16), SZ)
    wrows, frows = w_v.reshape(SX * SY, SZ), f_v.reshape(SX * SY, SZ)

    def sums(group):
        for c in group:
            for copy in loads[c]:
                copy.wait()
        for y in range(0, SY, 8):
            rows = slice(y, y + 8)
            packs = [zsend[0, rows], zsend[1, rows], dz_v[0, rows], dz_v[1, rows]]
            for x in range(group[0] * SPF, (group[-1] + 1) * SPF):
                w, f = w_v[x, rows], f_v[x, rows]
                s, d = w + f, w - f
                s_v[x + 2, 8 + y:16 + y] = s
                shift = (2 * x + 2) % SZ
                s, d = pltpu.roll(s, shift, 1), pltpu.roll(d, shift, 1)
                low = tile_lane // 2 == (x + 1) % (SZ // 2)
                high = tile_lane // 2 == x
                packs = [jnp.where(low, s, packs[0]), jnp.where(high, s, packs[1]),
                         jnp.where(low, d, packs[2]), jnp.where(high, d, packs[3])]
            zsend[0, rows], zsend[1, rows], dz_v[0, rows], dz_v[1, rows] = packs

    def yfaces(piece):
        for side in SIDES:
            for k in range(2):
                y = k if side == 0 else SY - 2 + k
                ysend[side, k, pl.ds(piece * each, each)] = srows[
                    pl.ds((piece * each + 2) * (SY + 16) + 8 + y, each, stride=SY + 16), :]
            start_halo(1, side, piece)

    def forces(i, slot):
        for xx in range(SPF):
            x = i * SPF + xx
            d = w_v[x] - f_v[x]
            s = s_v[x + 2, 8:8 + SY, :]
            gx = (s_v[x, 8:8 + SY, :] - s_v[x + 4, 8:8 + SY, :]
                  + 8.0 * (s_v[x + 3, 8:8 + SY, :] - s_v[x + 1, 8:8 + SY, :]))
            gy = (s_v[x + 2, 6:6 + SY, :] - s_v[x + 2, 10:10 + SY, :]
                  + 8.0 * (s_v[x + 2, 9:9 + SY, :] - s_v[x + 2, 7:7 + SY, :]))
            gz = (pltpu.roll(s, 2, 1) - pltpu.roll(s, SZ - 2, 1)
                  + 8.0 * (pltpu.roll(s, SZ - 1, 1) - pltpu.roll(s, 1, 1)))
            for a, g in enumerate((gx, gy, gz)):
                high, low = split2(g * d)
                fh_v[slot, xx * SY:(xx + 1) * SY, a * SZ:(a + 1) * SZ] = high
                fl_v[slot, xx * SY:(xx + 1) * SY, a * SZ:(a + 1) * SZ] = low

    lane = iota((SY, SZ), 1)

    def gather(i, slot):
        k, ph = divmod(i, per)
        many = 5 * QE + 4 * QC
        weights = jnp.concatenate([wf_v[0], wc_v[ph, 0], wf_v[1], wc_v[ph, 1]], axis=0)
        both = dot(weights, fh_v[slot])
        out = both[:many] + both[many:] + dot(weights[:many], fl_v[slot])
        accf[i:i + 5] += out[:5 * QE].reshape(5, QE, lanes)
        at = k + (1 if ph >= per // 2 else 0)
        accc[:, at:at + 4] += out[5 * QE:].reshape(QC, 4, lanes)

    def run_sums(group):
        sums(group)
        summed.append(group)

    def run_faces():
        while summed:
            yfaces(summed.pop(0)[0] * SPF // each)

    summed = []
    for group in groups[:BEFORE]:
        run_sums(group)
    pl.semaphore_wait(barrier, total)
    for d in range(1, nz):
        pl.semaphore_signal(
            in_sem, inc=1, device_id={"gz": lax.rem(me[2] + d, nz)}, device_id_type=MESH)
    start_halo(0, 0)
    start_halo(0, 1)
    run_faces()
    for group in groups[BEFORE:]:
        run_sums(group)
        run_faces()
    start_halo(2, 0)
    start_halo(2, 1)

    turn = list(range(1, cells - 1)) + [0, cells - 1]
    forces(turn[0], 0)
    for n, i in enumerate(turn):
        if n + 1 < cells:
            if turn[n + 1] == 0:
                wait_halo(0)
            forces(turn[n + 1], (n + 1) % 2)
        gather(i, n % 2)

    wait_halo(1)
    wait_halo(2)
    adds = []
    for side in SIDES:
        h0, h1 = yrecv[side, 0], yrecv[side, 1]
        g = (h0 - 8.0 * h1, h1) if side == 0 else (-h0, 8.0 * h0 - h1)
        for k in range(2):
            y = k if side == 0 else SY - 2 + k
            at = pl.ds(y, SX, stride=SY)
            adds.append(g[k] * (wrows[at, :] - frows[at, :]))
    high, low = split2(jnp.concatenate(adds, 0))
    weights = wy_v[0]
    added = dot(weights, high) + dot(wy_v[1], high) + dot(weights, low)

    even = lane % 2 == 0
    hl, hh = zrecv[0] - zsend[1], zrecv[1] - zsend[0]
    cl = jnp.where(even, hl - 8.0 * pltpu.roll(hl, SZ - 1, 1), hl)
    ch = jnp.where(even, -hh, 8.0 * pltpu.roll(hh, 1, 1) - hh)
    fz = jnp.concatenate([pltpu.roll(cl, 2, 1) * dz_v[0],
                          pltpu.roll(ch, SZ - 2, 1) * dz_v[1]], 1)
    high, low = split2(fz)
    g = dot(wq_v[0], high) + dot(wq_v[1], high) + dot(wq_v[0], low)
    blocks = [g[0:QE] * wx_v[p:p + 1] for p in turned]
    blocks += [g[QE + q:QE + q + 1] * wx_v[EX:EX + XR] for q in range(QC)]
    hhigh, hlow = split2(jnp.concatenate(blocks, 0))

    table = jnp.concatenate(
        [accf[2:2 + PX].reshape(PX * QE, lanes), accf[0:2].reshape(2 * QE, lanes),
         accf[2 + PX:].reshape(2 * QE, lanes), accc[...].reshape(NC, lanes)], 0)
    table = jnp.concatenate(
        [table[:, 0:SZ], table[:, SZ:2 * SZ] + added, table[:, 2 * SZ:]], 1)
    high, low = split2(table)
    whole = (dot(high, wz_v[0]) + dot(high, wz_v[1]) + dot(low, wz_v[0])
             + dot(hhigh, wh_v[0]) + dot(hhigh, wh_v[1]) + dot(hlow, wh_v[0]))

    pl.semaphore_wait(in_sem, nz - 1)

    def coarse_copy(o, at):
        return pltpu.make_async_remote_copy(
            src_ref=all_v.at[at], dst_ref=all_v.at[at],
            send_sem=cs_sem.at[o], recv_sem=cr_sem.at[o],
            device_id=tuple(lax.rem(me[k] + o[k], sizes[k]) for k in range(3)),
            device_id_type=MESH)

    everyone = [(ox, oy, oz) for ox in range(nx) for oy in range(ny) for oz in range(nz)][1:]
    far = sorted(everyone, key=lambda o: -sum(min(o[k], sizes[k] - o[k]) for k in range(3)))
    for v in range(0, QC, PG):
        share = 0.0
        for q in range(v, min(v + PG, QC)):
            tile = whole[NF + q * XR:NF + (q + 1) * XR, LW:2 * LW]
            share = share + (tile if q == v else pltpu.roll(tile, (q - v) * GL, 1))
        all_v[me[0], me[1], me[2], v // PG] = share
    for o in far:
        coarse_copy(o, tuple(me)).start()

    fine = whole[0:NF, 0:LW] + bend_v[...].reshape(NF, LW)
    tall = jnp.concatenate([fine, jnp.zeros((2 * LW - NF, LW), f32)], 0).T
    fine = fine.reshape(EX, QE, LW)
    for side in SIDES:
        at = 3 * PZ + 8 * side
        for half in range(2):
            zm_v[side, half] = tall[at:at + 8, half * LW:(half + 1) * LW]
        at = PX + 2 * side
        xm_v[side] = fine[at:at + 2, 0:PY]
    ym_v[...] = fine[:, PY:PY + 4]

    def fine_copy(dx, dy, dz):
        xs, ys, zs = (0 if d > 0 else 1 for d in (dx, dy, dz))
        if dz:
            src = zm_v.at[1 - zs, 1 if dx else 0]
            dst = zg_v.at[zs, 1 - dx, 1 - dy]
        elif dy == 0:
            src, dst = xm_v.at[1 - xs], xg_v.at[xs]
        elif dx == 0:
            src, dst = ym_v.at[pl.ds(0, PX)], yg_v.at[ys]
        else:
            src, dst = ym_v.at[pl.ds(PX if dx < 0 else PX + 2, 2)], cg_v.at[xs, ys]
        at = (dx + 1, dy + 1, dz + 1)
        return pltpu.make_async_remote_copy(
            src_ref=src, dst_ref=dst, send_sem=as_sem.at[at], recv_sem=ar_sem.at[at],
            device_id=(me[0] + dx, me[1] + dy, me[2] + dz), device_id_type=MESH)

    def there(step):
        ok = None
        for k in range(3):
            if step[k]:
                here = has[k][0 if step[k] < 0 else 1]
                ok = here if ok is None else ok & here
        return ok

    for step in AROUND:
        @pl.when(there(step))
        def _(step=step):
            fine_copy(*step).start()

    zin, l = iota((KZ, LW), 0), iota((KZ, LW), 1)
    shares = 0.0
    for a in range(3):
        m = jnp.concatenate([same(l % KZ, zin), 2.0 * diff1(l % KZ, zin),
                             diff2(l % KZ, zin, KZ)], 1)
        ok = jnp.concatenate([l // KZ == a] * 3, 1)
        shares = shares + spread(cc_ref, a, KX * KY, KZ, jnp.where(ok, m, 0.0).astype(bf16))
    shares = shares.reshape(KX, KY, 3 * LW)
    padc_v[1:1 + KX, 8:8 + KY, :] = shares[:, :, 0:LW]
    for p in range(KX):
        midc_v[1 + p, 8:8 + KY] = (
            cross(padc_v, 1 + p, (8, KY))[0] + shares[p, :, LW:2 * LW])
    for p in range(KX):
        out = (cross(midc_v, 1 + p, (8, KY))[0] + shares[p, :, 2 * LW:]) * BEND
        for a in range(3):
            co_ref[a, p * KY:(p + 1) * KY] = (
                out if a == 0 else pltpu.roll(out, LW - a * KZ, 1))

    for step in AROUND:
        back = tuple(-d for d in step)

        @pl.when(there(back))
        def _(step=step):
            fine_copy(*step).wait_recv()
    tile = iota((8, LW), 1)
    x, y = tile // QE, tile % QE
    for side in SIDES:
        got = 0.0
        for sx in STEPS:
            shift = {-1: -2 * QE, 0: 0, 1: (PX - 2) * QE}[sx]
            xin = {-1: x < 2, 0: x < PX, 1: x >= PX - 2}[sx]
            for sy in STEPS:
                yin = {-1: y < 2, 0: y < PY, 1: (y >= PY - 2) & (y < PY)}[sy]
                turn = (shift + {-1: -PY - 2, 0: 0, 1: -2}[sy]) % LW
                value = zg_v[side, 1 + sx, 1 + sy]
                value = pltpu.roll(value, turn, 1) if turn else value
                got = got + jnp.where(xin & yin, value, 0.0)
        for a in range(3):
            at = a * PZ + side * (PZ - 2)
            zt_v[at:at + 2] = got[2 * a:2 * a + 2]
    across = zt_v[...].T.reshape(PX, QE, LW)
    row = iota((PY, LW), 0)
    for p in range(PX):
        out = fine[p, 0:PY] + across[p, 0:PY]
        low, high = yg_v[0, p], yg_v[1, p]
        for side in SIDES:
            q = p if side == 0 else p - (PX - 2)
            if 0 <= q < 2:
                out = out + xg_v[side, q]
                low, high = low + cg_v[side, 0, q], high + cg_v[side, 1, q]
        fill = jnp.zeros((PY - 4, LW), f32)
        low = pltpu.roll(jnp.concatenate([low, fill], 0), PY - 2, 0)
        high = pltpu.roll(jnp.concatenate([high, fill], 0), PY - 2, 0)
        out = out + jnp.where(row < 2, low, jnp.where(row >= PY - 2, high, 0.0))
        for a in range(3):
            fo_ref[a, p] = (out if a == 0 else pltpu.roll(out, LW - a * PZ, 1))[:, 0:PZ]

    for o in far:
        coarse_copy(o, tuple(lax.rem(me[k] + sizes[k] - o[k], sizes[k])
                             for k in range(3))).wait_recv()
    row = iota((XR, LW), 0)
    for v in range(0, QC, PG):
        for b in range(0, KX, XR):
            placed = []
            for iz in range(nz):
                here = 0.0
                for ix in range(nx):
                    first = CX * ix - 2 - b
                    if first <= -XC or first >= XR:
                        continue
                    block = all_v[ix, 0, iz, v // PG]
                    for iy in range(1, ny):
                        block = block + all_v[ix, iy, iz, v // PG]
                    block = pltpu.roll(block, first % XR, 0)
                    here = here + jnp.where((row >= first) & (row < first + XC), block, 0.0)
                placed.append(here)
            for q in range(v, min(v + PG, QC)):
                for a in range(3):
                    out = 0.0
                    for iz in range(nz):
                        first = CZ * iz - 2
                        value = pltpu.roll(placed[iz], (first - (q - v) * GL - a * ZC) % LW, 1)
                        inside = (tile >= first) & (tile < first + ZC)
                        out = out + jnp.where(inside, value, 0.0)
                    at = pl.ds(b * KY + q, XR, stride=KY)
                    co_ref[a, at, :] = co_ref[a, at, :] + out

    for o in far:
        coarse_copy(o, tuple(me)).wait_send()
    for step in AROUND:
        @pl.when(there(step))
        def _(step=step):
            fine_copy(*step).wait_send()


def write_out(f_ref, c_ref, fo_ref, co_ref):
    fo_ref[...] = f_ref[...]
    KX, KY, KZ = co_ref.shape[1:]
    for a in range(3):
        for p in range(KX):
            co_ref[a, p] = c_ref[a, p * KY:(p + 1) * KY, 0:KZ]


def solution(mesh):
    sizes = tuple(mesh.shape[a] for a in AXES)

    def step(warped, fixed, fine, coarse):
        SX, SY, SZ = warped.shape
        PX, PY, PZ = SX // SPF, SY // SPF, SZ // SPF
        KX, KY, KZ = coarse.shape[1:]
        nx, ny, nz = sizes
        EX, QE = PX + 4, PY + 8
        XR, QC = -(-(SX // SPC + 4) // 8) * 8, KY
        KV = SPF * SY
        NF, NC, LW = EX * QE, XR * QC, 128
        vmem = pl.BlockSpec(memory_space=pltpu.VMEM)
        hbm = pl.BlockSpec(memory_space=pltpu.HBM)
        V = pltpu.VMEM
        D = pltpu.SemaphoreType.DMA
        held = pl.pallas_call(
            functools.partial(kernel, sizes),
            out_shape=(pltpu.VMEM(fine.shape, f32), pltpu.VMEM((3, KX * KY, LW), f32)),
            in_specs=[hbm] * 4,
            out_specs=(vmem, vmem),
            scratch_shapes=[
                V((SX, SY, SZ), f32), V((SX, SY, SZ), f32),
                V((3, PX, PY, PZ), f32), V(coarse.shape, f32),
                V((SX + 4, SY + 16, SZ), f32),
                V((2, 2, SX, SZ), f32), V((2, 2, SX, SZ), f32),
                V((2, SY, SZ), f32), V((2, SY, SZ), f32), V((2, SY, SZ), f32),
                V((2, 5 * QE, KV), bf16), V((SPC // SPF, 2, 4 * QC, KV), bf16),
                V((2, NF + NC, 4 * SX), bf16), V((2, QE + QC, SY), bf16),
                V((EX + XR, 2 * SZ), f32),
                V((2, 3 * SZ, 2 * LW), bf16), V((2, 2 * SZ, 2 * LW), bf16),
                V((2, KV, 3 * SZ), bf16), V((2, KV, 3 * SZ), bf16),
                V((EX, QE, 3 * SZ), f32), V((QC, XR, 3 * SZ), f32),
                V((PX + 6, PY + 16, LW), f32), V((PX + 6, PY + 16, LW), f32),
                V((EX, QE, LW), f32),
                V((KX + 2, KY + 16, LW), f32), V((KX + 2, KY + 16, LW), f32),
                V((2, 2, 8, LW), f32), V((2, 3, 3, 8, LW), f32), V((LW, LW), f32),
                V((2, 2, PY, LW), f32), V((EX, 4, LW), f32),
                V((2, 2, PY, LW), f32), V((2, PX, 4, LW), f32), V((2, 2, 2, 4, LW), f32),
                V((nx, ny, nz, -(-QC // 4), XR, LW), f32),
                D((2, SX // SPF)), D((2,)), D((3, 2)), D((3, 2)), D((2, 4)), D((2, 4)),
                D((3, 3, 3)), D((3, 3, 3)), D(sizes), D(sizes), pltpu.SemaphoreType.REGULAR,
            ],
            compiler_params=pltpu.CompilerParams(
                collective_id=0, has_side_effects=True, vmem_limit_bytes=64000000
            ),
        )(warped, fixed, fine, coarse)
        held = [pltpu.with_memory_space_constraint(h, memory_space=pltpu.VMEM) for h in held]
        return pl.pallas_call(
            write_out,
            out_shape=(jax.ShapeDtypeStruct(fine.shape, f32),
                       jax.ShapeDtypeStruct(coarse.shape, f32)),
            in_specs=[vmem] * 2,
            out_specs=(vmem, vmem),
        )(*held)

    in_specs = (P("gx", "gy", "gz"), P("gx", "gy", "gz"), P(None, "gx", "gy", "gz"), P())
    out_specs = (P(None, "gx", "gy", "gz"), P())
    return jax.shard_map(
        step, mesh=mesh, in_specs=in_specs, out_specs=out_specs, check_vma=False
    )
```

```python
import functools

import jax
import jax.numpy as jnp
from jax import lax
from jax.experimental import pallas as pl
from jax.experimental.pallas import tpu as pltpu
from jax.sharding import PartitionSpec as P

SPF = 8
SPC = 32
BEND = 0.01
MESH = pl.DeviceIdType.MESH
f32 = jnp.float32
bf16 = jnp.bfloat16
AXES = ("gx", "gy", "gz")
SIDES = (0, 1)
BEFORE = 3
STEPS = (-1, 0, 1)
AROUND = sorted(
    ((dx, dy, dz) for dx in STEPS for dy in STEPS for dz in STEPS if dx or dy or dz),
    key=lambda d: -sum(map(abs, d)))


def dot(a, b):
    return jnp.dot(a, b, preferred_element_type=f32)


def spline(t):
    m = jnp.abs(t)
    inner = 2.0 / 3.0 - m * m + 0.5 * m * m * m
    r = jnp.maximum(2.0 - m, 0.0)
    outer = r * r * r * (1.0 / 6.0)
    return jnp.where(m < 1.0, inner, outer)


def weight(voxel, point, spacing):
    scaled = (2 * voxel + 1 - spacing * (2 * point + 1)).astype(f32)
    return spline(scaled * (0.5 / spacing))


def iota(shape, axis):
    return lax.broadcasted_iota(jnp.int32, shape, axis)


def split2(value):
    high = value.astype(bf16)
    return high, (value - high.astype(f32)).astype(bf16)


def split3(value):
    high = value.astype(bf16)
    rest = value - high.astype(f32)
    mid = rest.astype(bf16)
    return high, mid, (rest - mid.astype(f32)).astype(bf16)


def same(out, inp):
    return jnp.where(out == inp, 1.0, 0.0).astype(f32)


def diff1(out, inp):
    d = jnp.abs(out - inp)
    return jnp.where(d == 0, -2.0, jnp.where(d == 1, 1.0, 0.0)).astype(f32)


def diff2(out, inp, count):
    d = jnp.abs(out - inp)
    edge = (inp == 0) | (inp == count - 1)
    centre = jnp.where(edge, 5.0, 6.0)
    return jnp.where(
        d == 0, centre, jnp.where(d == 1, -4.0, jnp.where(d == 2, 1.0, 0.0))
    ).astype(f32)


def cross(ref, x, rows):
    first, count = rows
    here = ref[x, first:first + count]
    return (ref[x - 1, first:first + count] + ref[x + 1, first:first + count]
            + ref[x, first - 1:first - 1 + count] + ref[x, first + 1:first + 1 + count]
            - 4.0 * here), here


def kernel(sizes, w_hbm, f_hbm, fc_hbm, cc_hbm, fo_ref, co_ref,
           w_v, f_v, fc_ref, cc_ref, s_v, ysend, yrecv, zsend, zrecv, dz_v,
           wf_v, wc_v, wy_v, wq_v, wx_v, wz_v, wh_v, fh_v, fl_v, parts_v, band_v,
           accf, accc, whole_v, pad_v, mid_v, bend_v, padc_v, midc_v,
           zm_v, zg_v, zt_v, xm_v, ym_v, xg_v, yg_v, cg_v, all_v,
           load_sem, small_sem, hs_sem, hr_sem, ys_sem, yr_sem,
           as_sem, ar_sem, cs_sem, cr_sem, in_sem):
    nx, ny, nz = sizes
    me = [lax.axis_index(a) for a in AXES]
    SX, SY, SZ = w_v.shape
    PX, PY, PZ = SX // SPF, SY // SPF, SZ // SPF
    KX, KY, KZ = cc_ref.shape[1:]
    EX, QE = PX + 4, PY + 8
    QC, XR = accc.shape[:2]
    CX, CZ = SX // SPC, SZ // SPC
    XC, ZC = CX + 4, CZ + 4
    GL = 32
    PG = 128 // GL
    cells = SX // SPF
    per = SPC // SPF
    lanes = 3 * SZ
    NF, NC = EX * QE, QC * XR
    LW = 128
    has = [(me[k] > 0, me[k] < sizes[k] - 1) for k in range(3)]

    small = (pltpu.make_async_copy(fc_hbm, fc_ref, small_sem.at[0]),
             pltpu.make_async_copy(cc_hbm, cc_ref, small_sem.at[1]))
    for copy in small:
        copy.start()
    loads = []
    for c in range(cells):
        part = pl.ds(c * SPF, SPF)
        loads.append((
            pltpu.make_async_copy(w_hbm.at[part], w_v.at[part], load_sem.at[0, c]),
            pltpu.make_async_copy(f_hbm.at[part], f_v.at[part], load_sem.at[1, c]),
        ))
    groups = [(0, 1), (cells - 2, cells - 1)]
    groups += [(c, c + 1) for c in range(2, cells - 2, 2)]
    for c in sum(groups, ()):
        loads[c][0].start()
        loads[c][1].start()

    for at in (0, SX + 2):
        s_v[at:at + 2, 8:8 + SY, :] = jnp.zeros((2, SY, SZ), f32)
    for ref in (yrecv, zrecv, xg_v, yg_v, cg_v, zg_v):
        ref[...] = jnp.zeros(ref.shape, f32)

    barrier = pltpu.get_barrier_semaphore()
    total = 0
    plane = [(ox, oy) for ox in range(nx) for oy in range(ny) if ox or oy]

    def in_plane(ox, oy):
        return {"gx": lax.rem(me[0] + ox, nx), "gy": lax.rem(me[1] + oy, ny)}

    for d in range(1, nz):
        pl.semaphore_signal(
            barrier, inc=1, device_id={"gz": lax.rem(me[2] + d, nz)}, device_id_type=MESH)
        total += 1
    for ox, oy in plane:
        pl.semaphore_signal(barrier, inc=1, device_id=in_plane(ox, oy), device_id_type=MESH)
        total += 1

    s_v[2:SX + 2, 0:8, :] = jnp.zeros((SX, 8, SZ), f32)
    s_v[2:SX + 2, 8 + SY:16 + SY, :] = jnp.zeros((SX, 8, SZ), f32)
    for ref in (accf, accc, pad_v, mid_v, padc_v, midc_v, zt_v, dz_v, zsend):
        ref[...] = jnp.zeros(ref.shape, f32)

    def edge_row(row):
        return jnp.where(row < PY, row, jnp.where(row < PY + 2, row - PY - 2,
                         jnp.where(row < PY + 4, row - 2, row + 8 * PY)))

    def put(ref, index, value):
        high, low = split2(value)
        ref[(0,) + index] = high
        ref[(1,) + index] = low

    KV = SPF * SY
    cols = iota((QE, KV), 1)
    along_y = weight(cols % SY, edge_row(iota((QE, KV), 0)), SPF)
    along_x = weight(iota((8, KV), 1) // SY, iota((8, KV), 0) - 2, SPF)
    for p in range(5):
        put(wf_v, (slice(p * QE, (p + 1) * QE),), along_y * along_x[p:p + 1])
    rows, cols = iota((4 * QC, KV), 0), iota((4 * QC, KV), 1)
    along_y = weight(cols % SY + me[1] * SY, rows // 4, SPC)
    for ph in range(per):
        first = -2 if ph < per // 2 else -1
        along_x = weight(cols // SY + ph * SPF, rows % 4 + first, SPC)
        high, low = split2(along_x * along_y)
        wc_v[ph, 0] = high
        wc_v[ph, 1] = low

    KH = 4 * SX
    place = (iota((16, KH), 1) // SX)
    yat = jnp.where(place < 2, place, SY - 4 + place)
    along_y = weight(yat, edge_row(iota((16, KH), 0)), SPF)
    along_x = weight(iota((16, KH), 1) % SX, iota((16, KH), 0) - 2, SPF)
    turned = list(range(2, 2 + PX)) + [0, 1, PX + 2, PX + 3]
    for n, p in enumerate(turned):
        put(wy_v, (slice(n * QE, (n + 1) * QE),), along_y * along_x[p:p + 1])
    rows, cols = iota((NC, KH), 0), iota((NC, KH), 1)
    place = cols // SX
    yat = jnp.where(place < 2, place, SY - 4 + place)
    put(wy_v, (slice(NF, NF + NC),), weight(cols % SX, rows % XR - 2, SPC)
        * weight(yat + me[1] * SY, rows // XR, SPC))

    KP = 2 * SZ
    rows, cols = iota((QE, SY), 0), iota((QE, SY), 1)
    put(wq_v, (slice(0, QE),), weight(cols, edge_row(rows), SPF))
    rows, cols = iota((QC, SY), 0), iota((QC, SY), 1)
    put(wq_v, (slice(QE, QE + QC),), weight(cols + me[1] * SY, rows, SPC))
    col = iota((EX, KP), 1)
    xat = jnp.where(col < SZ, (col + SZ - 2) % SZ, col % SZ) // 2
    wx_v[0:EX] = weight(xat, iota((EX, KP), 0) - 2, SPF)
    wx_v[EX:EX + XR] = weight(xat[0:XR], iota((XR, KP), 0) - 2, SPC)

    def fine_lane(l):
        e = (l - 3 * PZ) % 8
        centre = l < 3 * PZ
        known = centre | ((l < 3 * PZ + 16) & (e < 6))
        comp = jnp.where(centre, l // PZ, jnp.where(known, e // 2, 3))
        point = jnp.where(centre, l % PZ, jnp.where(l < 3 * PZ + 8, e % 2 - 2, PZ + e % 2))
        return comp, point

    def both_levels(z):
        l = iota(z.shape, 1)[:, 0:LW]
        z = z[:, 0:LW]
        comp, point = fine_lane(l)
        fine = weight(z, point, SPF) * (SPF ** -1.5 / 24.0)
        ccomp = l // ZC
        coarse = weight(z, l % ZC - 2, SPC) * (SPC ** -1.5 / 24.0)
        return jnp.concatenate([comp, ccomp], 1), jnp.concatenate([fine, coarse], 1)

    comp, value = both_levels(iota((SZ, 2 * LW), 0))
    high, low = split2(value)
    high, low = high.astype(f32), low.astype(f32)
    for a in range(3):
        part = slice(a * SZ, (a + 1) * SZ)
        wz_v[0, part] = jnp.where(comp == a, high, 0.0).astype(bf16)
        wz_v[1, part] = jnp.where(comp == a, low, 0.0).astype(bf16)
    row = iota((8, 2 * LW), 0)
    comp, value = both_levels(jnp.where(row < 2, row, SZ - 4 + row))
    value = jnp.where(comp == 2, value, 0.0)
    odd = iota((SZ, 2 * LW), 0) % 2 == 1
    for side in SIDES:
        part = slice(side * SZ, (side + 1) * SZ)
        put(wh_v, (part,), jnp.where(odd, value[2 * side + 1:2 * side + 2],
                                     value[2 * side:2 * side + 1]))

    step = iota((SZ, SZ), 1) - iota((SZ, SZ), 0)
    band = (jnp.where(step == 2, 1.0, 0.0) - jnp.where(step == 1, 8.0, 0.0)
            + jnp.where(step == -1, 8.0, 0.0) - jnp.where(step == -2, 1.0, 0.0)).astype(bf16)
    band_v[0:SZ] = band
    band_v[SZ:2 * SZ] = band

    for copy in small:
        copy.wait()

    def spread(ref, a, count, width, matrix):
        block = ref[a].reshape(count, width)
        return sum(dot(part, matrix) for part in split3(block))

    zin, l = iota((PZ, LW), 0), iota((PZ, LW), 1)
    comp, point = fine_lane(l)
    oz = me[2] * PZ
    shares = 0.0
    for a in range(3):
        m = jnp.concatenate([same(point, zin), 2.0 * diff1(point, zin),
                             diff2(point + oz, zin + oz, PZ * nz)], 1)
        ok = jnp.concatenate([comp == a] * 3, 1)
        shares = shares + spread(fc_ref, a, PX * PY, PZ, jnp.where(ok, m, 0.0).astype(bf16))
    shares = shares.reshape(PX, PY, 3 * LW)
    pad_v[3:3 + PX, 8:8 + PY, :] = shares[:, :, 0:LW]
    inside = iota((PY + 8, LW), 0) - 4 + me[1] * PY
    inside = (inside >= 0) & (inside < PY * ny)
    for p in range(-1, PX + 1):
        u, _ = cross(pad_v, 3 + p, (4, PY + 8))
        keep = inside & (me[0] * PX + p >= 0) & (me[0] * PX + p < PX * nx)
        mid_v[3 + p, 4:12 + PY] = jnp.where(keep, u, 0.0)
    mid_v[3:3 + PX, 8:8 + PY, :] = mid_v[3:3 + PX, 8:8 + PY, :] + shares[:, :, LW:2 * LW]
    row = iota((PY, LW), 0)
    for p in range(-2, PX + 2):
        v = [cross(mid_v, 3 + p, (first, PY))[0] for first in (8, 6, 6 + PY)]
        centre = v[0]
        if 0 <= p < PX:
            centre = centre + shares[p, :, 2 * LW:3 * LW]
        at = turned.index(2 + p)
        bend_v[at, 0:PY] = centre * BEND
        bend_v[at, PY:2 * PY] = jnp.where(
            row < 2, v[1], jnp.where(row < 4, v[2], 0.0)) * BEND

    pieces = ys_sem.shape[1]
    each = SX // pieces

    def neighbour_copy(k, side, src, dst, send, recv):
        other = me[k] - 1 if side == 0 else me[k] + 1
        return pltpu.make_async_remote_copy(
            src_ref=src, dst_ref=dst, send_sem=send, recv_sem=recv,
            device_id={AXES[k]: other}, device_id_type=MESH,
        )

    def halo(k, side, piece=0):
        if k == 1:
            part = pl.ds(piece * each, each)
            return neighbour_copy(
                k, side, ysend.at[side, :, part], yrecv.at[1 - side, :, part],
                ys_sem.at[side, piece], yr_sem.at[1 - side, piece])
        if k == 0:
            src = s_v.at[pl.ds(2 if side == 0 else SX, 2), pl.ds(8, SY), :]
            dst = s_v.at[pl.ds(SX + 2 if side == 0 else 0, 2), pl.ds(8, SY), :]
        else:
            src, dst = zsend.at[side], zrecv.at[1 - side]
        return neighbour_copy(k, side, src, dst, hs_sem.at[k, side], hr_sem.at[k, 1 - side])

    def start_halo(k, side, piece=0):
        @pl.when(has[k][side])
        def _():
            halo(k, side, piece).start()

    def wait_halo(k):
        for side in SIDES:
            for piece in range(pieces if k == 1 else 1):
                @pl.when(has[k][side])
                def _(side=side, piece=piece):
                    halo(k, side, piece).wait_send()

                @pl.when(has[k][1 - side])
                def _(side=side, piece=piece):
                    halo(k, side, piece).wait_recv()

    tile_lane = iota((16, SZ), 1)

    def pack(packs, value, x):
        value = pltpu.roll(value, (2 * x + 2) % SZ, 1)
        low = tile_lane // 2 == (x + 1) % (SZ // 2)
        return [jnp.where(low, value, packs[0]), jnp.where(tile_lane // 2 == x, value, packs[1])]

    srows = s_v.reshape((SX + 4) * (SY + 16), SZ)
    wrows, frows = w_v.reshape(SX * SY, SZ), f_v.reshape(SX * SY, SZ)

    def sums(group):
        for c in group:
            for copy in loads[c]:
                copy.wait()
        for y in range(0, SY, 16):
            rows = slice(y, y + 16)
            packs = [zsend[0, rows], zsend[1, rows]]
            for x in range(group[0] * SPF, (group[-1] + 1) * SPF):
                s = w_v[x, rows] + f_v[x, rows]
                s_v[x + 2, 8 + y:24 + y] = s
                high, low = split2(s)
                parts_v[x * SY + y:x * SY + y + 16, 0:SZ] = high
                parts_v[x * SY + y:x * SY + y + 16, SZ:2 * SZ] = low
                packs = pack(packs, s, x)
            zsend[0, rows], zsend[1, rows] = packs

    def yfaces(piece):
        for side in SIDES:
            for k in range(2):
                y = k if side == 0 else SY - 2 + k
                ysend[side, k, pl.ds(piece * each, each)] = srows[
                    pl.ds((piece * each + 2) * (SY + 16) + 8 + y, each, stride=SY + 16), :]
            start_halo(1, side, piece)

    def forces(i, slot):
        slopes = dot(parts_v[i * KV:(i + 1) * KV], band_v[...])
        for y in range(0, SY, 16):
            rows = slice(8 + y, 24 + y)
            slabs = [s_v[i * SPF + x, rows] for x in range(SPF + 4)]
            packs = [dz_v[0, y:y + 16], dz_v[1, y:y + 16]]
            for xx in range(SPF):
                x = i * SPF + xx
                d = w_v[x, y:y + 16] - f_v[x, y:y + 16]
                packs = pack(packs, d, x)
                gx = slabs[xx] - slabs[xx + 4] + 8.0 * (slabs[xx + 3] - slabs[xx + 1])
                gy = (s_v[x + 2, 6 + y:22 + y] - s_v[x + 2, 10 + y:26 + y]
                      + 8.0 * (s_v[x + 2, 9 + y:25 + y] - s_v[x + 2, 7 + y:23 + y]))
                gz = slopes[xx * SY + y:xx * SY + y + 16]
                for a, g in enumerate((gx, gy, gz)):
                    at = (slot, slice(xx * SY + y, xx * SY + y + 16),
                          slice(a * SZ, (a + 1) * SZ))
                    fh_v[at], fl_v[at] = split2(g * d)
            dz_v[0, y:y + 16], dz_v[1, y:y + 16] = packs

    lane = iota((SY, SZ), 1)

    def gather(i, slot):
        k, ph = divmod(i, per)
        many = 5 * QE + 4 * QC
        weights = jnp.concatenate([wf_v[0], wc_v[ph, 0], wf_v[1], wc_v[ph, 1]], axis=0)
        both = dot(weights, fh_v[slot])
        out = both[:many] + both[many:] + dot(weights[:many], fl_v[slot])
        accf[i:i + 5] += out[:5 * QE].reshape(5, QE, lanes)
        at = k + (1 if ph >= per // 2 else 0)
        accc[:, at:at + 4] += out[5 * QE:].reshape(QC, 4, lanes)

    def run_sums(group):
        sums(group)
        summed.append(group)

    def run_faces():
        while summed:
            yfaces(summed.pop(0)[0] * SPF // each)

    summed = []
    for group in groups[:BEFORE]:
        run_sums(group)
    pl.semaphore_wait(barrier, total)
    for d in range(1, nz):
        pl.semaphore_signal(
            in_sem, inc=1, device_id={"gz": lax.rem(me[2] + d, nz)}, device_id_type=MESH)
    start_halo(0, 0)
    start_halo(0, 1)
    run_faces()
    for group in groups[BEFORE:]:
        run_sums(group)
        run_faces()
    start_halo(2, 0)
    start_halo(2, 1)

    turn = list(range(1, cells - 1)) + [0, cells - 1]
    forces(turn[0], 0)
    for n, i in enumerate(turn):
        if n + 1 < cells:
            if turn[n + 1] == 0:
                wait_halo(0)
            forces(turn[n + 1], (n + 1) % 2)
        gather(i, n % 2)

    table = jnp.concatenate(
        [accf[2:2 + PX].reshape(PX * QE, lanes), accf[0:2].reshape(2 * QE, lanes),
         accf[2 + PX:].reshape(2 * QE, lanes), accc[...].reshape(NC, lanes)], 0)
    high, low = split2(table)
    whole_v[...] = dot(high, wz_v[0]) + dot(high, wz_v[1]) + dot(low, wz_v[0])
    whole_v[0:NF, 0:LW] = whole_v[0:NF, 0:LW] + bend_v[...].reshape(NF, LW)

    wait_halo(1)
    wait_halo(2)
    adds = []
    for side in SIDES:
        h0, h1 = yrecv[side, 0], yrecv[side, 1]
        g = (h0 - 8.0 * h1, h1) if side == 0 else (-h0, 8.0 * h0 - h1)
        for k in range(2):
            y = k if side == 0 else SY - 2 + k
            at = pl.ds(y, SX, stride=SY)
            adds.append(g[k] * (wrows[at, :] - frows[at, :]))
    high, low = split2(jnp.concatenate(adds, 0))
    weights = wy_v[0]
    added = dot(weights, high) + dot(wy_v[1], high) + dot(weights, low)

    even = lane % 2 == 0
    hl, hh = zrecv[0], zrecv[1]
    cl = jnp.where(even, hl - 8.0 * pltpu.roll(hl, SZ - 1, 1), hl)
    ch = jnp.where(even, -hh, 8.0 * pltpu.roll(hh, 1, 1) - hh)
    fz = jnp.concatenate([pltpu.roll(cl, 2, 1) * dz_v[0],
                          pltpu.roll(ch, SZ - 2, 1) * dz_v[1]], 1)
    high, low = split2(fz)
    g = dot(wq_v[0], high) + dot(wq_v[1], high) + dot(wq_v[0], low)
    blocks = [g[0:QE] * wx_v[p:p + 1] for p in turned]
    blocks += [g[QE + q:QE + q + 1] * wx_v[EX:EX + XR] for q in range(QC)]
    hhigh, hlow = split2(jnp.concatenate(blocks, 0))

    high, low = split2(added)
    part = slice(SZ, 2 * SZ)
    whole = whole_v[...] + (
        dot(high, wz_v[0, part]) + dot(high, wz_v[1, part]) + dot(low, wz_v[0, part])
        + dot(hhigh, wh_v[0]) + dot(hhigh, wh_v[1]) + dot(hlow, wh_v[0]))

    pl.semaphore_wait(in_sem, nz - 1)

    mine = (me[0] * ny + me[1]) * nz + me[2]
    count = nx * ny * nz - 1

    def coarse_wait(sem):
        ref = all_v.at[pl.ds(0, count)]
        pltpu.make_async_copy(ref, ref, sem).wait()

    def coarse_copy(o, at):
        return pltpu.make_async_remote_copy(
            src_ref=all_v.at[at], dst_ref=all_v.at[at],
            send_sem=cs_sem, recv_sem=cr_sem,
            device_id=tuple(lax.rem(me[k] + o[k], sizes[k]) for k in range(3)),
            device_id_type=MESH)

    everyone = [(ox, oy, oz) for ox in range(nx) for oy in range(ny) for oz in range(nz)][1:]
    far = sorted(everyone, key=lambda o: -sum(min(o[k], sizes[k] - o[k]) for k in range(3)))
    for v in range(0, QC, PG):
        share = 0.0
        for q in range(v, min(v + PG, QC)):
            tile = whole[NF + q * XR:NF + (q + 1) * XR, LW:2 * LW]
            share = share + (tile if q == v else pltpu.roll(tile, (q - v) * GL, 1))
        all_v[mine, v // PG] = share[0:XC]
    for o in far:
        coarse_copy(o, mine).start()

    fine = whole[0:NF, 0:LW]
    tall = jnp.concatenate([fine, jnp.zeros((2 * LW - NF, LW), f32)], 0).T
    fine = fine.reshape(EX, QE, LW)
    for side in SIDES:
        at = 3 * PZ + 8 * side
        for half in range(2):
            zm_v[side, half] = tall[at:at + 8, half * LW:(half + 1) * LW]
        at = PX + 2 * side
        xm_v[side] = fine[at:at + 2, 0:PY]
    ym_v[...] = fine[:, PY:PY + 4]

    def fine_copy(dx, dy, dz):
        xs, ys, zs = (0 if d > 0 else 1 for d in (dx, dy, dz))
        if dz:
            src = zm_v.at[1 - zs, 1 if dx else 0]
            dst = zg_v.at[zs, 1 - dx, 1 - dy]
        elif dy == 0:
            src, dst = xm_v.at[1 - xs], xg_v.at[xs]
        elif dx == 0:
            src, dst = ym_v.at[pl.ds(0, PX)], yg_v.at[ys]
        else:
            src, dst = ym_v.at[pl.ds(PX if dx < 0 else PX + 2, 2)], cg_v.at[xs, ys]
        at = (dx + 1, dy + 1, dz + 1)
        return pltpu.make_async_remote_copy(
            src_ref=src, dst_ref=dst, send_sem=as_sem.at[at], recv_sem=ar_sem.at[at],
            device_id=(me[0] + dx, me[1] + dy, me[2] + dz), device_id_type=MESH)

    def there(step):
        ok = None
        for k in range(3):
            if step[k]:
                here = has[k][0 if step[k] < 0 else 1]
                ok = here if ok is None else ok & here
        return ok

    for step in AROUND:
        @pl.when(there(step))
        def _(step=step):
            fine_copy(*step).start()

    zin, l = iota((KZ, LW), 0), iota((KZ, LW), 1)
    shares = 0.0
    for a in range(3):
        m = jnp.concatenate([same(l % KZ, zin), 2.0 * diff1(l % KZ, zin),
                             diff2(l % KZ, zin, KZ)], 1)
        ok = jnp.concatenate([l // KZ == a] * 3, 1)
        shares = shares + spread(cc_ref, a, KX * KY, KZ, jnp.where(ok, m, 0.0).astype(bf16))
    shares = shares.reshape(KX, KY, 3 * LW)
    padc_v[1:1 + KX, 8:8 + KY, :] = shares[:, :, 0:LW]
    for p in range(KX):
        midc_v[1 + p, 8:8 + KY] = (
            cross(padc_v, 1 + p, (8, KY))[0] + shares[p, :, LW:2 * LW])
    for p in range(KX):
        out = (cross(midc_v, 1 + p, (8, KY))[0] + shares[p, :, 2 * LW:]) * BEND
        for a in range(3):
            co_ref[a, p * KY:(p + 1) * KY] = (
                out if a == 0 else pltpu.roll(out, LW - a * KZ, 1))

    for step in AROUND:
        back = tuple(-d for d in step)

        @pl.when(there(back))
        def _(step=step):
            fine_copy(*step).wait_recv()
    tile = iota((8, LW), 1)
    x, y = tile // QE, tile % QE
    for side in SIDES:
        got = 0.0
        for sx in STEPS:
            shift = {-1: -2 * QE, 0: 0, 1: (PX - 2) * QE}[sx]
            xin = {-1: x < 2, 0: x < PX, 1: x >= PX - 2}[sx]
            for sy in STEPS:
                yin = {-1: y < 2, 0: y < PY, 1: (y >= PY - 2) & (y < PY)}[sy]
                turn = (shift + {-1: -PY - 2, 0: 0, 1: -2}[sy]) % LW
                value = zg_v[side, 1 + sx, 1 + sy]
                value = pltpu.roll(value, turn, 1) if turn else value
                got = got + jnp.where(xin & yin, value, 0.0)
        for a in range(3):
            at = a * PZ + side * (PZ - 2)
            zt_v[at:at + 2] = got[2 * a:2 * a + 2]
    across = zt_v[...].T.reshape(PX, QE, LW)
    row = iota((PY, LW), 0)
    for p in range(PX):
        out = fine[p, 0:PY] + across[p, 0:PY]
        low, high = yg_v[0, p], yg_v[1, p]
        for side in SIDES:
            q = p if side == 0 else p - (PX - 2)
            if 0 <= q < 2:
                out = out + xg_v[side, q]
                low, high = low + cg_v[side, 0, q], high + cg_v[side, 1, q]
        fill = jnp.zeros((PY - 4, LW), f32)
        low = pltpu.roll(jnp.concatenate([low, fill], 0), PY - 2, 0)
        high = pltpu.roll(jnp.concatenate([high, fill], 0), PY - 2, 0)
        out = out + jnp.where(row < 2, low, jnp.where(row >= PY - 2, high, 0.0))
        for a in range(3):
            fo_ref[a, p] = (out if a == 0 else pltpu.roll(out, LW - a * PZ, 1))[:, 0:PZ]

    for step in AROUND:
        @pl.when(there(step))
        def _(step=step):
            fine_copy(*step).wait_send()
    if count:
        coarse_wait(cs_sem)
        coarse_wait(cr_sem)
    row = iota((XR, LW), 0)
    for v in range(0, QC, PG):
        for b in range(0, KX, XR):
            placed = []
            for iz in range(nz):
                here = 0.0
                for ix in range(nx):
                    first = CX * ix - 2 - b
                    if first <= -XC or first >= XR:
                        continue
                    block = all_v[ix * ny * nz + iz, v // PG]
                    for iy in range(1, ny):
                        block = block + all_v[(ix * ny + iy) * nz + iz, v // PG]
                    block = jnp.concatenate([block, jnp.zeros((XR - XC, LW), f32)], 0)
                    block = pltpu.roll(block, first % XR, 0)
                    here = here + jnp.where((row >= first) & (row < first + XC), block, 0.0)
                placed.append(here)
            for q in range(v, min(v + PG, QC)):
                for a in range(3):
                    out = 0.0
                    for iz in range(nz):
                        first = CZ * iz - 2
                        value = pltpu.roll(placed[iz], (first - (q - v) * GL - a * ZC) % LW, 1)
                        inside = (tile >= first) & (tile < first + ZC)
                        out = out + jnp.where(inside, value, 0.0)
                    at = pl.ds(b * KY + q, XR, stride=KY)
                    co_ref[a, at, :] = co_ref[a, at, :] + out


def write_out(f_ref, c_ref, fo_ref, co_ref):
    fo_ref[...] = f_ref[...]
    KX, KY, KZ = co_ref.shape[1:]
    for a in range(3):
        for p in range(KX):
            co_ref[a, p] = c_ref[a, p * KY:(p + 1) * KY, 0:KZ]


def solution(mesh):
    sizes = tuple(mesh.shape[a] for a in AXES)

    def step(warped, fixed, fine, coarse):
        SX, SY, SZ = warped.shape
        PX, PY, PZ = SX // SPF, SY // SPF, SZ // SPF
        KX, KY, KZ = coarse.shape[1:]
        nx, ny, nz = sizes
        EX, QE = PX + 4, PY + 8
        XR, QC = -(-(SX // SPC + 4) // 8) * 8, KY
        KV = SPF * SY
        NF, NC, LW = EX * QE, XR * QC, 128
        vmem = pl.BlockSpec(memory_space=pltpu.VMEM)
        hbm = pl.BlockSpec(memory_space=pltpu.HBM)
        V = pltpu.VMEM
        D = pltpu.SemaphoreType.DMA
        held = pl.pallas_call(
            functools.partial(kernel, sizes),
            out_shape=(pltpu.VMEM(fine.shape, f32), pltpu.VMEM((3, KX * KY, LW), f32)),
            in_specs=[hbm] * 4,
            out_specs=(vmem, vmem),
            scratch_shapes=[
                V((SX, SY, SZ), f32), V((SX, SY, SZ), f32),
                V((3, PX, PY, PZ), f32), V(coarse.shape, f32),
                V((SX + 4, SY + 16, SZ), f32),
                V((2, 2, SX, SZ), f32), V((2, 2, SX, SZ), f32),
                V((2, SY, SZ), f32), V((2, SY, SZ), f32), V((2, SY, SZ), f32),
                V((2, 5 * QE, KV), bf16), V((SPC // SPF, 2, 4 * QC, KV), bf16),
                V((2, NF + NC, 4 * SX), bf16), V((2, QE + QC, SY), bf16),
                V((EX + XR, 2 * SZ), f32),
                V((2, 3 * SZ, 2 * LW), bf16), V((2, 2 * SZ, 2 * LW), bf16),
                V((2, KV, 3 * SZ), bf16), V((2, KV, 3 * SZ), bf16),
                V((SX * SY, 2 * SZ), bf16), V((2 * SZ, SZ), bf16),
                V((EX, QE, 3 * SZ), f32), V((QC, XR, 3 * SZ), f32),
                V((NF + NC, 2 * LW), f32),
                V((PX + 6, PY + 16, LW), f32), V((PX + 6, PY + 16, LW), f32),
                V((EX, QE, LW), f32),
                V((KX + 2, KY + 16, LW), f32), V((KX + 2, KY + 16, LW), f32),
                V((2, 2, 8, LW), f32), V((2, 3, 3, 8, LW), f32), V((LW, LW), f32),
                V((2, 2, PY, LW), f32), V((EX, 4, LW), f32),
                V((2, 2, PY, LW), f32), V((2, PX, 4, LW), f32), V((2, 2, 2, 4, LW), f32),
                V((nx * ny * nz, -(-QC // 4), SX // SPC + 4, LW), f32),
                D((2, SX // SPF)), D((2,)), D((3, 2)), D((3, 2)), D((2, 4)), D((2, 4)),
                D((3, 3, 3)), D((3, 3, 3)), D(()), D(()), pltpu.SemaphoreType.REGULAR,
            ],
            compiler_params=pltpu.CompilerParams(
                collective_id=0, has_side_effects=True, vmem_limit_bytes=64000000
            ),
        )(warped, fixed, fine, coarse)
        held = [pltpu.with_memory_space_constraint(h, memory_space=pltpu.VMEM) for h in held]
        return pl.pallas_call(
            write_out,
            out_shape=(jax.ShapeDtypeStruct(fine.shape, f32),
                       jax.ShapeDtypeStruct(coarse.shape, f32)),
            in_specs=[vmem] * 2,
            out_specs=(vmem, vmem),
        )(*held)

    in_specs = (P("gx", "gy", "gz"), P("gx", "gy", "gz"), P(None, "gx", "gy", "gz"), P())
    out_specs = (P(None, "gx", "gy", "gz"), P())
    return jax.shard_map(
        step, mesh=mesh, in_specs=in_specs, out_specs=out_specs, check_vma=False
    )
```

```python
import functools

import jax
import jax.numpy as jnp
from jax import lax
from jax.experimental import pallas as pl
from jax.experimental.pallas import tpu as pltpu
from jax.sharding import PartitionSpec as P

SPF = 8
SPC = 32
BEND = 0.01
MESH = pl.DeviceIdType.MESH
f32 = jnp.float32
bf16 = jnp.bfloat16
AXES = ("gx", "gy", "gz")
SIDES = (0, 1)
BEFORE = 2
STEPS = (-1, 0, 1)
AROUND = sorted(
    ((dx, dy, dz) for dx in STEPS for dy in STEPS for dz in STEPS if dx or dy or dz),
    key=lambda d: -sum(map(abs, d)))


def dot(a, b):
    return jnp.dot(a, b, preferred_element_type=f32)


def spline(t):
    m = jnp.abs(t)
    inner = 2.0 / 3.0 - m * m + 0.5 * m * m * m
    r = jnp.maximum(2.0 - m, 0.0)
    outer = r * r * r * (1.0 / 6.0)
    return jnp.where(m < 1.0, inner, outer)


def weight(voxel, point, spacing):
    scaled = (2 * voxel + 1 - spacing * (2 * point + 1)).astype(f32)
    return spline(scaled * (0.5 / spacing))


def iota(shape, axis):
    return lax.broadcasted_iota(jnp.int32, shape, axis)


def split2(value):
    high = value.astype(bf16)
    return high, (value - high.astype(f32)).astype(bf16)


def split3(value):
    high = value.astype(bf16)
    rest = value - high.astype(f32)
    mid = rest.astype(bf16)
    return high, mid, (rest - mid.astype(f32)).astype(bf16)


def same(out, inp):
    return jnp.where(out == inp, 1.0, 0.0).astype(f32)


def diff1(out, inp):
    d = jnp.abs(out - inp)
    return jnp.where(d == 0, -2.0, jnp.where(d == 1, 1.0, 0.0)).astype(f32)


def diff2(out, inp, count):
    d = jnp.abs(out - inp)
    edge = (inp == 0) | (inp == count - 1)
    centre = jnp.where(edge, 5.0, 6.0)
    return jnp.where(
        d == 0, centre, jnp.where(d == 1, -4.0, jnp.where(d == 2, 1.0, 0.0))
    ).astype(f32)


def cross(ref, x, rows):
    first, count = rows
    here = ref[x, first:first + count]
    return (ref[x - 1, first:first + count] + ref[x + 1, first:first + count]
            + ref[x, first - 1:first - 1 + count] + ref[x, first + 1:first + 1 + count]
            - 4.0 * here), here


def kernel(sizes, w_hbm, f_hbm, fc_hbm, cc_hbm, fo_ref, co_ref,
           w_v, f_v, fc_ref, cc_ref, s_v, ysend, yrecv, zsend, zrecv, dz_v,
           wf_v, wc_v, wy_v, wq_v, wx_v, wz_v, wh_v, fh_v, fl_v, parts_v, band_v,
           accf, accc, whole_v, pad_v, mid_v, bend_v, padc_v, midc_v,
           zm_v, zg_v, zt_v, xm_v, ym_v, xg_v, yg_v, cg_v, all_v,
           load_sem, small_sem, hs_sem, hr_sem, ys_sem, yr_sem,
           as_sem, ar_sem, cs_sem, cr_sem, in_sem):
    nx, ny, nz = sizes
    me = [lax.axis_index(a) for a in AXES]
    SX, SY, SZ = w_v.shape
    PX, PY, PZ = SX // SPF, SY // SPF, SZ // SPF
    KX, KY, KZ = cc_ref.shape[1:]
    EX, QE = PX + 4, PY + 8
    QC, XR = accc.shape[:2]
    CX, CZ = SX // SPC, SZ // SPC
    XC, ZC = CX + 4, CZ + 4
    GL = 32
    PG = 128 // GL
    cells = SX // SPF
    per = SPC // SPF
    lanes = 3 * SZ
    NF, NC = EX * QE, QC * XR
    LW = 128
    has = [(me[k] > 0, me[k] < sizes[k] - 1) for k in range(3)]

    small = (pltpu.make_async_copy(fc_hbm, fc_ref, small_sem.at[0]),
             pltpu.make_async_copy(cc_hbm, cc_ref, small_sem.at[1]))
    for copy in small:
        copy.start()
    loads = []
    for c in range(cells):
        part = pl.ds(c * SPF, SPF)
        loads.append((
            pltpu.make_async_copy(w_hbm.at[part], w_v.at[part], load_sem.at[0, c]),
            pltpu.make_async_copy(f_hbm.at[part], f_v.at[part], load_sem.at[1, c]),
        ))
    groups = [(0, 1), (cells - 2, cells - 1)]
    groups += [(c, c + 1) for c in range(2, cells - 2, 2)]
    for c in sum(groups, ()):
        loads[c][0].start()
        loads[c][1].start()

    for at in (0, SX + 2):
        s_v[at:at + 2, 8:8 + SY, :] = jnp.zeros((2, SY, SZ), f32)
    for ref in (yrecv, zrecv, xg_v, yg_v, cg_v, zg_v):
        ref[...] = jnp.zeros(ref.shape, f32)

    barrier = pltpu.get_barrier_semaphore()
    total = 0
    plane = [(ox, oy) for ox in range(nx) for oy in range(ny) if ox or oy]

    def in_plane(ox, oy):
        return {"gx": lax.rem(me[0] + ox, nx), "gy": lax.rem(me[1] + oy, ny)}

    for d in range(1, nz):
        pl.semaphore_signal(
            barrier, inc=1, device_id={"gz": lax.rem(me[2] + d, nz)}, device_id_type=MESH)
        total += 1
    for ox, oy in plane:
        pl.semaphore_signal(barrier, inc=1, device_id=in_plane(ox, oy), device_id_type=MESH)
        total += 1

    s_v[2:SX + 2, 0:8, :] = jnp.zeros((SX, 8, SZ), f32)
    s_v[2:SX + 2, 8 + SY:16 + SY, :] = jnp.zeros((SX, 8, SZ), f32)
    for ref in (accf, accc, pad_v, mid_v, padc_v, midc_v, zt_v, dz_v, zsend):
        ref[...] = jnp.zeros(ref.shape, f32)

    def edge_row(row):
        return jnp.where(row < PY, row, jnp.where(row < PY + 2, row - PY - 2,
                         jnp.where(row < PY + 4, row - 2, row + 8 * PY)))

    def put(ref, index, value):
        high, low = split2(value)
        ref[(0,) + index] = high
        ref[(1,) + index] = low

    KV = SPF * SY
    cols = iota((QE, KV), 1)
    along_y = weight(cols % SY, edge_row(iota((QE, KV), 0)), SPF)
    along_x = weight(iota((8, KV), 1) // SY, iota((8, KV), 0) - 2, SPF)
    for p in range(5):
        put(wf_v, (slice(p * QE, (p + 1) * QE),), along_y * along_x[p:p + 1])
    rows, cols = iota((4 * QC, KV), 0), iota((4 * QC, KV), 1)
    along_y = weight(cols % SY + me[1] * SY, rows // 4, SPC)
    for ph in range(per):
        first = -2 if ph < per // 2 else -1
        along_x = weight(cols // SY + ph * SPF, rows % 4 + first, SPC)
        high, low = split2(along_x * along_y)
        wc_v[ph, 0] = high
        wc_v[ph, 1] = low

    pieces = ys_sem.shape[1]
    each = SX // pieces

    def neighbour_copy(k, side, src, dst, send, recv):
        other = me[k] - 1 if side == 0 else me[k] + 1
        return pltpu.make_async_remote_copy(
            src_ref=src, dst_ref=dst, send_sem=send, recv_sem=recv,
            device_id={AXES[k]: other}, device_id_type=MESH,
        )

    def halo(k, side, piece=0):
        if k == 1:
            part = pl.ds(piece * each, each)
            return neighbour_copy(
                k, side, ysend.at[side, :, part], yrecv.at[1 - side, :, part],
                ys_sem.at[side, piece], yr_sem.at[1 - side, piece])
        if k == 0:
            src = s_v.at[pl.ds(2 if side == 0 else SX, 2), pl.ds(8, SY), :]
            dst = s_v.at[pl.ds(SX + 2 if side == 0 else 0, 2), pl.ds(8, SY), :]
        else:
            src, dst = zsend.at[side], zrecv.at[1 - side]
        return neighbour_copy(k, side, src, dst, hs_sem.at[k, side], hr_sem.at[k, 1 - side])

    def start_halo(k, side, piece=0):
        @pl.when(has[k][side])
        def _():
            halo(k, side, piece).start()

    def wait_halo(k):
        for side in SIDES:
            for piece in range(pieces if k == 1 else 1):
                @pl.when(has[k][side])
                def _(side=side, piece=piece):
                    halo(k, side, piece).wait_send()

                @pl.when(has[k][1 - side])
                def _(side=side, piece=piece):
                    halo(k, side, piece).wait_recv()

    tile_lane = iota((16, SZ), 1)

    def pack(packs, value, x):
        value = pltpu.roll(value, (2 * x + 2) % SZ, 1)
        low = tile_lane // 2 == (x + 1) % (SZ // 2)
        return [jnp.where(low, value, packs[0]), jnp.where(tile_lane // 2 == x, value, packs[1])]

    srows = s_v.reshape((SX + 4) * (SY + 16), SZ)
    drows = w_v.reshape(SX * SY, SZ)

    def sums(group):
        for c in group:
            for copy in loads[c]:
                copy.wait()
        for y in range(0, SY, 16):
            rows = slice(y, y + 16)
            packs = [zsend[0, rows], zsend[1, rows]]
            for x in range(group[0] * SPF, (group[-1] + 1) * SPF):
                w, f = w_v[x, rows], f_v[x, rows]
                s = w + f
                w_v[x, rows] = w - f
                s_v[x + 2, 8 + y:24 + y] = s
                high, low = split2(s)
                parts_v[x * SY + y:x * SY + y + 16, 0:SZ] = high
                parts_v[x * SY + y:x * SY + y + 16, SZ:2 * SZ] = low
                packs = pack(packs, s, x)
            zsend[0, rows], zsend[1, rows] = packs

    def yfaces(piece):
        for side in SIDES:
            for k in range(2):
                y = k if side == 0 else SY - 2 + k
                ysend[side, k, pl.ds(piece * each, each)] = srows[
                    pl.ds((piece * each + 2) * (SY + 16) + 8 + y, each, stride=SY + 16), :]
            start_halo(1, side, piece)

    def forces(i, slot):
        slopes = dot(parts_v[i * KV:(i + 1) * KV], band_v[...])
        for y in range(0, SY, 16):
            rows = slice(8 + y, 24 + y)
            slabs = [s_v[i * SPF + x, rows] for x in range(SPF + 4)]
            packs = [dz_v[0, y:y + 16], dz_v[1, y:y + 16]]
            for xx in range(SPF):
                x = i * SPF + xx
                d = w_v[x, y:y + 16]
                packs = pack(packs, d, x)
                gx = slabs[xx] - slabs[xx + 4] + 8.0 * (slabs[xx + 3] - slabs[xx + 1])
                gy = (s_v[x + 2, 6 + y:22 + y] - s_v[x + 2, 10 + y:26 + y]
                      + 8.0 * (s_v[x + 2, 9 + y:25 + y] - s_v[x + 2, 7 + y:23 + y]))
                gz = slopes[xx * SY + y:xx * SY + y + 16]
                for a, g in enumerate((gx, gy, gz)):
                    at = (slot, slice(xx * SY + y, xx * SY + y + 16),
                          slice(a * SZ, (a + 1) * SZ))
                    fh_v[at], fl_v[at] = split2(g * d)
            dz_v[0, y:y + 16], dz_v[1, y:y + 16] = packs

    lane = iota((SY, SZ), 1)

    def gather(i, slot):
        k, ph = divmod(i, per)
        many = 5 * QE + 4 * QC
        weights = jnp.concatenate([wf_v[0], wc_v[ph, 0], wf_v[1], wc_v[ph, 1]], axis=0)
        both = dot(weights, fh_v[slot])
        out = both[:many] + both[many:] + dot(weights[:many], fl_v[slot])
        accf[i:i + 5] += out[:5 * QE].reshape(5, QE, lanes)
        at = k + (1 if ph >= per // 2 else 0)
        accc[:, at:at + 4] += out[5 * QE:].reshape(QC, 4, lanes)

    def run_sums(group):
        sums(group)
        summed.append(group)

    def run_faces():
        while summed:
            yfaces(summed.pop(0)[0] * SPF // each)

    summed = []
    for group in groups[:BEFORE]:
        run_sums(group)
    pl.semaphore_wait(barrier, total)
    for d in range(1, nz):
        pl.semaphore_signal(
            in_sem, inc=1, device_id={"gz": lax.rem(me[2] + d, nz)}, device_id_type=MESH)
    start_halo(0, 0)
    start_halo(0, 1)
    run_faces()
    for group in groups[BEFORE:]:
        run_sums(group)
        run_faces()
    start_halo(2, 0)
    start_halo(2, 1)

    KH = 4 * SX
    place = (iota((16, KH), 1) // SX)
    yat = jnp.where(place < 2, place, SY - 4 + place)
    along_y = weight(yat, edge_row(iota((16, KH), 0)), SPF)
    along_x = weight(iota((16, KH), 1) % SX, iota((16, KH), 0) - 2, SPF)
    turned = list(range(2, 2 + PX)) + [0, 1, PX + 2, PX + 3]
    for n, p in enumerate(turned):
        put(wy_v, (slice(n * QE, (n + 1) * QE),), along_y * along_x[p:p + 1])
    rows, cols = iota((NC, KH), 0), iota((NC, KH), 1)
    place = cols // SX
    yat = jnp.where(place < 2, place, SY - 4 + place)
    put(wy_v, (slice(NF, NF + NC),), weight(cols % SX, rows % XR - 2, SPC)
        * weight(yat + me[1] * SY, rows // XR, SPC))

    KP = 2 * SZ
    rows, cols = iota((QE, SY), 0), iota((QE, SY), 1)
    put(wq_v, (slice(0, QE),), weight(cols, edge_row(rows), SPF))
    rows, cols = iota((QC, SY), 0), iota((QC, SY), 1)
    put(wq_v, (slice(QE, QE + QC),), weight(cols + me[1] * SY, rows, SPC))
    col = iota((EX, KP), 1)
    xat = jnp.where(col < SZ, (col + SZ - 2) % SZ, col % SZ) // 2
    wx_v[0:EX] = weight(xat, iota((EX, KP), 0) - 2, SPF)
    wx_v[EX:EX + XR] = weight(xat[0:XR], iota((XR, KP), 0) - 2, SPC)

    def fine_lane(l):
        e = (l - 3 * PZ) % 8
        centre = l < 3 * PZ
        known = centre | ((l < 3 * PZ + 16) & (e < 6))
        comp = jnp.where(centre, l // PZ, jnp.where(known, e // 2, 3))
        point = jnp.where(centre, l % PZ, jnp.where(l < 3 * PZ + 8, e % 2 - 2, PZ + e % 2))
        return comp, point

    def both_levels(z):
        l = iota(z.shape, 1)[:, 0:LW]
        z = z[:, 0:LW]
        comp, point = fine_lane(l)
        fine = weight(z, point, SPF) * (SPF ** -1.5 / 24.0)
        ccomp = l // ZC
        coarse = weight(z, l % ZC - 2, SPC) * (SPC ** -1.5 / 24.0)
        return jnp.concatenate([comp, ccomp], 1), jnp.concatenate([fine, coarse], 1)

    comp, value = both_levels(iota((SZ, 2 * LW), 0))
    high, low = split2(value)
    high, low = high.astype(f32), low.astype(f32)
    for a in range(3):
        part = slice(a * SZ, (a + 1) * SZ)
        wz_v[0, part] = jnp.where(comp == a, high, 0.0).astype(bf16)
        wz_v[1, part] = jnp.where(comp == a, low, 0.0).astype(bf16)
    row = iota((8, 2 * LW), 0)
    comp, value = both_levels(jnp.where(row < 2, row, SZ - 4 + row))
    value = jnp.where(comp == 2, value, 0.0)
    odd = iota((SZ, 2 * LW), 0) % 2 == 1
    for side in SIDES:
        part = slice(side * SZ, (side + 1) * SZ)
        put(wh_v, (part,), jnp.where(odd, value[2 * side + 1:2 * side + 2],
                                     value[2 * side:2 * side + 1]))

    step = iota((SZ, SZ), 1) - iota((SZ, SZ), 0)
    band = (jnp.where(step == 2, 1.0, 0.0) - jnp.where(step == 1, 8.0, 0.0)
            + jnp.where(step == -1, 8.0, 0.0) - jnp.where(step == -2, 1.0, 0.0)).astype(bf16)
    band_v[0:SZ] = band
    band_v[SZ:2 * SZ] = band

    for copy in small:
        copy.wait()

    def spread(ref, a, count, width, matrix):
        block = ref[a].reshape(count, width)
        return sum(dot(part, matrix) for part in split3(block))

    zin, l = iota((PZ, LW), 0), iota((PZ, LW), 1)
    comp, point = fine_lane(l)
    oz = me[2] * PZ
    shares = 0.0
    for a in range(3):
        m = jnp.concatenate([same(point, zin), 2.0 * diff1(point, zin),
                             diff2(point + oz, zin + oz, PZ * nz)], 1)
        ok = jnp.concatenate([comp == a] * 3, 1)
        shares = shares + spread(fc_ref, a, PX * PY, PZ, jnp.where(ok, m, 0.0).astype(bf16))
    shares = shares.reshape(PX, PY, 3 * LW)
    pad_v[3:3 + PX, 8:8 + PY, :] = shares[:, :, 0:LW]
    inside = iota((PY + 8, LW), 0) - 4 + me[1] * PY
    inside = (inside >= 0) & (inside < PY * ny)
    for p in range(-1, PX + 1):
        u, _ = cross(pad_v, 3 + p, (4, PY + 8))
        keep = inside & (me[0] * PX + p >= 0) & (me[0] * PX + p < PX * nx)
        mid_v[3 + p, 4:12 + PY] = jnp.where(keep, u, 0.0)
    mid_v[3:3 + PX, 8:8 + PY, :] = mid_v[3:3 + PX, 8:8 + PY, :] + shares[:, :, LW:2 * LW]
    row = iota((PY, LW), 0)
    for p in range(-2, PX + 2):
        v = [cross(mid_v, 3 + p, (first, PY))[0] for first in (8, 6, 6 + PY)]
        centre = v[0]
        if 0 <= p < PX:
            centre = centre + shares[p, :, 2 * LW:3 * LW]
        at = turned.index(2 + p)
        bend_v[at, 0:PY] = centre * BEND
        bend_v[at, PY:2 * PY] = jnp.where(
            row < 2, v[1], jnp.where(row < 4, v[2], 0.0)) * BEND

    turn = list(range(1, cells - 1)) + [0, cells - 1]
    forces(turn[0], 0)
    for n, i in enumerate(turn):
        if n + 1 < cells:
            if turn[n + 1] == 0:
                wait_halo(0)
            forces(turn[n + 1], (n + 1) % 2)
        gather(i, n % 2)

    table = jnp.concatenate(
        [accf[2:2 + PX].reshape(PX * QE, lanes), accf[0:2].reshape(2 * QE, lanes),
         accf[2 + PX:].reshape(2 * QE, lanes), accc[...].reshape(NC, lanes)], 0)
    high, low = split2(table)
    whole_v[...] = dot(high, wz_v[0]) + dot(high, wz_v[1]) + dot(low, wz_v[0])
    whole_v[0:NF, 0:LW] = whole_v[0:NF, 0:LW] + bend_v[...].reshape(NF, LW)

    wait_halo(1)
    wait_halo(2)
    adds = []
    for side in SIDES:
        h0, h1 = yrecv[side, 0], yrecv[side, 1]
        g = (h0 - 8.0 * h1, h1) if side == 0 else (-h0, 8.0 * h0 - h1)
        for k in range(2):
            y = k if side == 0 else SY - 2 + k
            at = pl.ds(y, SX, stride=SY)
            adds.append(g[k] * drows[at, :])
    high, low = split2(jnp.concatenate(adds, 0))
    weights = wy_v[0]
    added = dot(weights, high) + dot(wy_v[1], high) + dot(weights, low)

    even = lane % 2 == 0
    hl, hh = zrecv[0], zrecv[1]
    cl = jnp.where(even, hl - 8.0 * pltpu.roll(hl, SZ - 1, 1), hl)
    ch = jnp.where(even, -hh, 8.0 * pltpu.roll(hh, 1, 1) - hh)
    fz = jnp.concatenate([pltpu.roll(cl, 2, 1) * dz_v[0],
                          pltpu.roll(ch, SZ - 2, 1) * dz_v[1]], 1)
    high, low = split2(fz)
    g = dot(wq_v[0], high) + dot(wq_v[1], high) + dot(wq_v[0], low)
    blocks = [g[0:QE] * wx_v[p:p + 1] for p in turned]
    blocks += [g[QE + q:QE + q + 1] * wx_v[EX:EX + XR] for q in range(QC)]
    hhigh, hlow = split2(jnp.concatenate(blocks, 0))

    high, low = split2(added)
    part = slice(SZ, 2 * SZ)
    whole = whole_v[...] + (
        dot(high, wz_v[0, part]) + dot(high, wz_v[1, part]) + dot(low, wz_v[0, part])
        + dot(hhigh, wh_v[0]) + dot(hhigh, wh_v[1]) + dot(hlow, wh_v[0]))

    pl.semaphore_wait(in_sem, nz - 1)

    mine = (me[0] * ny + me[1]) * nz + me[2]
    count = nx * ny * nz - 1

    def coarse_wait(sem):
        ref = all_v.at[pl.ds(0, count)]
        pltpu.make_async_copy(ref, ref, sem).wait()

    def coarse_copy(o, at):
        return pltpu.make_async_remote_copy(
            src_ref=all_v.at[at], dst_ref=all_v.at[at],
            send_sem=cs_sem, recv_sem=cr_sem,
            device_id=tuple(lax.rem(me[k] + o[k], sizes[k]) for k in range(3)),
            device_id_type=MESH)

    everyone = [(ox, oy, oz) for ox in range(nx) for oy in range(ny) for oz in range(nz)][1:]
    far = sorted(everyone, key=lambda o: -sum(min(o[k], sizes[k] - o[k]) for k in range(3)))
    for v in range(0, QC, PG):
        share = 0.0
        for q in range(v, min(v + PG, QC)):
            tile = whole[NF + q * XR:NF + (q + 1) * XR, LW:2 * LW]
            share = share + (tile if q == v else pltpu.roll(tile, (q - v) * GL, 1))
        all_v[mine, v // PG] = share[0:XC]
    for o in far:
        coarse_copy(o, mine).start()

    fine = whole[0:NF, 0:LW]
    tall = jnp.concatenate([fine, jnp.zeros((2 * LW - NF, LW), f32)], 0).T
    fine = fine.reshape(EX, QE, LW)
    for side in SIDES:
        at = 3 * PZ + 8 * side
        for half in range(2):
            zm_v[side, half] = tall[at:at + 8, half * LW:(half + 1) * LW]
        at = PX + 2 * side
        xm_v[side] = fine[at:at + 2, 0:PY]
    ym_v[...] = fine[:, PY:PY + 4]

    def fine_copy(dx, dy, dz):
        xs, ys, zs = (0 if d > 0 else 1 for d in (dx, dy, dz))
        if dz:
            src = zm_v.at[1 - zs, 1 if dx else 0]
            dst = zg_v.at[zs, 1 - dx, 1 - dy]
        elif dy == 0:
            src, dst = xm_v.at[1 - xs], xg_v.at[xs]
        elif dx == 0:
            src, dst = ym_v.at[pl.ds(0, PX)], yg_v.at[ys]
        else:
            src, dst = ym_v.at[pl.ds(PX if dx < 0 else PX + 2, 2)], cg_v.at[xs, ys]
        at = (dx + 1, dy + 1, dz + 1)
        return pltpu.make_async_remote_copy(
            src_ref=src, dst_ref=dst, send_sem=as_sem.at[at], recv_sem=ar_sem.at[at],
            device_id=(me[0] + dx, me[1] + dy, me[2] + dz), device_id_type=MESH)

    def there(step):
        ok = None
        for k in range(3):
            if step[k]:
                here = has[k][0 if step[k] < 0 else 1]
                ok = here if ok is None else ok & here
        return ok

    for step in AROUND:
        @pl.when(there(step))
        def _(step=step):
            fine_copy(*step).start()

    zin, l = iota((KZ, LW), 0), iota((KZ, LW), 1)
    shares = 0.0
    for a in range(3):
        m = jnp.concatenate([same(l % KZ, zin), 2.0 * diff1(l % KZ, zin),
                             diff2(l % KZ, zin, KZ)], 1)
        ok = jnp.concatenate([l // KZ == a] * 3, 1)
        shares = shares + spread(cc_ref, a, KX * KY, KZ, jnp.where(ok, m, 0.0).astype(bf16))
    shares = shares.reshape(KX, KY, 3 * LW)
    padc_v[1:1 + KX, 8:8 + KY, :] = shares[:, :, 0:LW]
    for p in range(KX):
        midc_v[1 + p, 8:8 + KY] = (
            cross(padc_v, 1 + p, (8, KY))[0] + shares[p, :, LW:2 * LW])
    for p in range(KX):
        out = (cross(midc_v, 1 + p, (8, KY))[0] + shares[p, :, 2 * LW:]) * BEND
        for a in range(3):
            co_ref[a, p * KY:(p + 1) * KY] = (
                out if a == 0 else pltpu.roll(out, LW - a * KZ, 1))

    for step in AROUND:
        back = tuple(-d for d in step)

        @pl.when(there(back))
        def _(step=step):
            fine_copy(*step).wait_recv()
    tile = iota((8, LW), 1)
    x, y = tile // QE, tile % QE
    for side in SIDES:
        got = 0.0
        for sx in STEPS:
            shift = {-1: -2 * QE, 0: 0, 1: (PX - 2) * QE}[sx]
            xin = {-1: x < 2, 0: x < PX, 1: x >= PX - 2}[sx]
            for sy in STEPS:
                yin = {-1: y < 2, 0: y < PY, 1: (y >= PY - 2) & (y < PY)}[sy]
                turn = (shift + {-1: -PY - 2, 0: 0, 1: -2}[sy]) % LW
                value = zg_v[side, 1 + sx, 1 + sy]
                value = pltpu.roll(value, turn, 1) if turn else value
                got = got + jnp.where(xin & yin, value, 0.0)
        for a in range(3):
            at = a * PZ + side * (PZ - 2)
            zt_v[at:at + 2] = got[2 * a:2 * a + 2]
    across = zt_v[...].T.reshape(PX, QE, LW)
    row = iota((PY, LW), 0)
    for p in range(PX):
        out = fine[p, 0:PY] + across[p, 0:PY]
        low, high = yg_v[0, p], yg_v[1, p]
        for side in SIDES:
            q = p if side == 0 else p - (PX - 2)
            if 0 <= q < 2:
                out = out + xg_v[side, q]
                low, high = low + cg_v[side, 0, q], high + cg_v[side, 1, q]
        fill = jnp.zeros((PY - 4, LW), f32)
        low = pltpu.roll(jnp.concatenate([low, fill], 0), PY - 2, 0)
        high = pltpu.roll(jnp.concatenate([high, fill], 0), PY - 2, 0)
        out = out + jnp.where(row < 2, low, jnp.where(row >= PY - 2, high, 0.0))
        for a in range(3):
            fo_ref[a, p] = (out if a == 0 else pltpu.roll(out, LW - a * PZ, 1))[:, 0:PZ]

    for step in AROUND:
        @pl.when(there(step))
        def _(step=step):
            fine_copy(*step).wait_send()
    if count:
        coarse_wait(cs_sem)
        coarse_wait(cr_sem)
    row = iota((XR, LW), 0)
    for v in range(0, QC, PG):
        for b in range(0, KX, XR):
            placed = []
            for iz in range(nz):
                here = 0.0
                for ix in range(nx):
                    first = CX * ix - 2 - b
                    if first <= -XC or first >= XR:
                        continue
                    block = all_v[ix * ny * nz + iz, v // PG]
                    for iy in range(1, ny):
                        block = block + all_v[(ix * ny + iy) * nz + iz, v // PG]
                    block = jnp.concatenate([block, jnp.zeros((XR - XC, LW), f32)], 0)
                    block = pltpu.roll(block, first % XR, 0)
                    here = here + jnp.where((row >= first) & (row < first + XC), block, 0.0)
                placed.append(here)
            for q in range(v, min(v + PG, QC)):
                for a in range(3):
                    out = 0.0
                    for iz in range(nz):
                        first = CZ * iz - 2
                        value = pltpu.roll(placed[iz], (first - (q - v) * GL - a * ZC) % LW, 1)
                        inside = (tile >= first) & (tile < first + ZC)
                        out = out + jnp.where(inside, value, 0.0)
                    at = pl.ds(b * KY + q, XR, stride=KY)
                    co_ref[a, at, :] = co_ref[a, at, :] + out


def write_out(f_ref, c_ref, fo_ref, co_ref):
    fo_ref[...] = f_ref[...]
    KX, KY, KZ = co_ref.shape[1:]
    for a in range(3):
        for p in range(KX):
            co_ref[a, p] = c_ref[a, p * KY:(p + 1) * KY, 0:KZ]


def solution(mesh):
    sizes = tuple(mesh.shape[a] for a in AXES)

    def step(warped, fixed, fine, coarse):
        SX, SY, SZ = warped.shape
        PX, PY, PZ = SX // SPF, SY // SPF, SZ // SPF
        KX, KY, KZ = coarse.shape[1:]
        nx, ny, nz = sizes
        EX, QE = PX + 4, PY + 8
        XR, QC = -(-(SX // SPC + 4) // 8) * 8, KY
        KV = SPF * SY
        NF, NC, LW = EX * QE, XR * QC, 128
        vmem = pl.BlockSpec(memory_space=pltpu.VMEM)
        hbm = pl.BlockSpec(memory_space=pltpu.HBM)
        V = pltpu.VMEM
        D = pltpu.SemaphoreType.DMA
        held = pl.pallas_call(
            functools.partial(kernel, sizes),
            out_shape=(pltpu.VMEM(fine.shape, f32), pltpu.VMEM((3, KX * KY, LW), f32)),
            in_specs=[hbm] * 4,
            out_specs=(vmem, vmem),
            scratch_shapes=[
                V((SX, SY, SZ), f32), V((SX, SY, SZ), f32),
                V((3, PX, PY, PZ), f32), V(coarse.shape, f32),
                V((SX + 4, SY + 16, SZ), f32),
                V((2, 2, SX, SZ), f32), V((2, 2, SX, SZ), f32),
                V((2, SY, SZ), f32), V((2, SY, SZ), f32), V((2, SY, SZ), f32),
                V((2, 5 * QE, KV), bf16), V((SPC // SPF, 2, 4 * QC, KV), bf16),
                V((2, NF + NC, 4 * SX), bf16), V((2, QE + QC, SY), bf16),
                V((EX + XR, 2 * SZ), f32),
                V((2, 3 * SZ, 2 * LW), bf16), V((2, 2 * SZ, 2 * LW), bf16),
                V((2, KV, 3 * SZ), bf16), V((2, KV, 3 * SZ), bf16),
                V((SX * SY, 2 * SZ), bf16), V((2 * SZ, SZ), bf16),
                V((EX, QE, 3 * SZ), f32), V((QC, XR, 3 * SZ), f32),
                V((NF + NC, 2 * LW), f32),
                V((PX + 6, PY + 16, LW), f32), V((PX + 6, PY + 16, LW), f32),
                V((EX, QE, LW), f32),
                V((KX + 2, KY + 16, LW), f32), V((KX + 2, KY + 16, LW), f32),
                V((2, 2, 8, LW), f32), V((2, 3, 3, 8, LW), f32), V((LW, LW), f32),
                V((2, 2, PY, LW), f32), V((EX, 4, LW), f32),
                V((2, 2, PY, LW), f32), V((2, PX, 4, LW), f32), V((2, 2, 2, 4, LW), f32),
                V((nx * ny * nz, -(-QC // 4), SX // SPC + 4, LW), f32),
                D((2, SX // SPF)), D((2,)), D((3, 2)), D((3, 2)), D((2, 4)), D((2, 4)),
                D((3, 3, 3)), D((3, 3, 3)), D(()), D(()), pltpu.SemaphoreType.REGULAR,
            ],
            compiler_params=pltpu.CompilerParams(
                collective_id=0, has_side_effects=True, vmem_limit_bytes=64000000
            ),
        )(warped, fixed, fine, coarse)
        held = [pltpu.with_memory_space_constraint(h, memory_space=pltpu.VMEM) for h in held]
        return pl.pallas_call(
            write_out,
            out_shape=(jax.ShapeDtypeStruct(fine.shape, f32),
                       jax.ShapeDtypeStruct(coarse.shape, f32)),
            in_specs=[vmem] * 2,
            out_specs=(vmem, vmem),
        )(*held)

    in_specs = (P("gx", "gy", "gz"), P("gx", "gy", "gz"), P(None, "gx", "gy", "gz"), P())
    out_specs = (P(None, "gx", "gy", "gz"), P())
    return jax.shard_map(
        step, mesh=mesh, in_specs=in_specs, out_specs=out_specs, check_vma=False
    )
```

```python
import functools

import jax
import jax.numpy as jnp
from jax import lax
from jax.experimental import pallas as pl
from jax.experimental.pallas import tpu as pltpu
from jax.sharding import PartitionSpec as P

SPF = 8
SPC = 32
BEND = 0.01
MESH = pl.DeviceIdType.MESH
f32 = jnp.float32
bf16 = jnp.bfloat16
AXES = ("gx", "gy", "gz")
SIDES = (0, 1)
BEFORE = 2
STEPS = (-1, 0, 1)
AROUND = sorted(
    ((dx, dy, dz) for dx in STEPS for dy in STEPS for dz in STEPS if dx or dy or dz),
    key=lambda d: -sum(map(abs, d)))


def dot(a, b):
    return jnp.dot(a, b, preferred_element_type=f32)


def spline(t):
    m = jnp.abs(t)
    inner = 2.0 / 3.0 - m * m + 0.5 * m * m * m
    r = jnp.maximum(2.0 - m, 0.0)
    outer = r * r * r * (1.0 / 6.0)
    return jnp.where(m < 1.0, inner, outer)


def weight(voxel, point, spacing):
    scaled = (2 * voxel + 1 - spacing * (2 * point + 1)).astype(f32)
    return spline(scaled * (0.5 / spacing))


def iota(shape, axis):
    return lax.broadcasted_iota(jnp.int32, shape, axis)


def split2(value):
    high = value.astype(bf16)
    return high, (value - high.astype(f32)).astype(bf16)


def thrice(a, b):
    return dot(a[0], b[0]) + dot(a[1], b[0]) + dot(a[0], b[1])


def split3(value):
    high = value.astype(bf16)
    rest = value - high.astype(f32)
    mid = rest.astype(bf16)
    return high, mid, (rest - mid.astype(f32)).astype(bf16)


def same(out, inp):
    return jnp.where(out == inp, 1.0, 0.0).astype(f32)


def diff1(out, inp):
    d = jnp.abs(out - inp)
    return jnp.where(d == 0, -2.0, jnp.where(d == 1, 1.0, 0.0)).astype(f32)


def diff2(out, inp, count):
    d = jnp.abs(out - inp)
    edge = (inp == 0) | (inp == count - 1)
    centre = jnp.where(edge, 5.0, 6.0)
    return jnp.where(
        d == 0, centre, jnp.where(d == 1, -4.0, jnp.where(d == 2, 1.0, 0.0))
    ).astype(f32)


def cross(ref, x, rows):
    first, count = rows
    here = ref[x, first:first + count]
    return (ref[x - 1, first:first + count] + ref[x + 1, first:first + count]
            + ref[x, first - 1:first - 1 + count] + ref[x, first + 1:first + 1 + count]
            - 4.0 * here), here


def kernel(sizes, w_hbm, f_hbm, fc_hbm, cc_hbm, fo_ref, co_ref,
           w_v, f_v, fc_ref, cc_ref, s_v, ysend, yrecv, zsend, zrecv, dz_v,
           wf_v, wc_v, wy_v, wq_v, wx_v, wz_v, wh_v, fh_v, fl_v, parts_v, band_v,
           accf, accc, whole_v, pad_v, mid_v, bend_v, padc_v, midc_v,
           zm_v, zg_v, zt_v, xm_v, ym_v, xg_v, yg_v, cg_v, all_v,
           load_sem, small_sem, hs_sem, hr_sem, ys_sem, yr_sem,
           as_sem, ar_sem, cs_sem, cr_sem, in_sem):
    nx, ny, nz = sizes
    me = [lax.axis_index(a) for a in AXES]
    SX, SY, SZ = w_v.shape
    PX, PY, PZ = SX // SPF, SY // SPF, SZ // SPF
    KX, KY, KZ = cc_ref.shape[1:]
    EX, QE = PX + 4, PY + 8
    QC, XR = accc.shape[:2]
    CX, CZ = SX // SPC, SZ // SPC
    XC, ZC = CX + 4, CZ + 4
    GL = 32
    PG = 128 // GL
    cells = SX // SPF
    per = SPC // SPF
    lanes = 3 * SZ
    NF, NC = EX * QE, QC * XR
    LW = 128
    has = [(me[k] > 0, me[k] < sizes[k] - 1) for k in range(3)]

    small = (pltpu.make_async_copy(fc_hbm, fc_ref, small_sem.at[0]),
             pltpu.make_async_copy(cc_hbm, cc_ref, small_sem.at[1]))
    for copy in small:
        copy.start()
    loads = []
    for c in range(cells):
        part = pl.ds(c * SPF, SPF)
        loads.append((
            pltpu.make_async_copy(w_hbm.at[part], w_v.at[part], load_sem.at[0, c]),
            pltpu.make_async_copy(f_hbm.at[part], f_v.at[part], load_sem.at[1, c]),
        ))
    groups = [(0, 1), (cells - 2, cells - 1)]
    groups += [(c, c + 1) for c in range(2, cells - 2, 2)]
    for c in sum(groups, ()):
        loads[c][0].start()
        loads[c][1].start()

    for at in (0, SX + 2):
        s_v[at:at + 2, 8:8 + SY, :] = jnp.zeros((2, SY, SZ), f32)
    for ref in (yrecv, zrecv, xg_v, yg_v, cg_v, zg_v):
        ref[...] = jnp.zeros(ref.shape, f32)

    barrier = pltpu.get_barrier_semaphore()
    total = 0
    plane = [(ox, oy) for ox in range(nx) for oy in range(ny) if ox or oy]

    def in_plane(ox, oy):
        return {"gx": lax.rem(me[0] + ox, nx), "gy": lax.rem(me[1] + oy, ny)}

    for d in range(1, nz):
        pl.semaphore_signal(
            barrier, inc=1, device_id={"gz": lax.rem(me[2] + d, nz)}, device_id_type=MESH)
        total += 1
    for ox, oy in plane:
        pl.semaphore_signal(barrier, inc=1, device_id=in_plane(ox, oy), device_id_type=MESH)
        total += 1

    s_v[2:SX + 2, 0:8, :] = jnp.zeros((SX, 8, SZ), f32)
    s_v[2:SX + 2, 8 + SY:16 + SY, :] = jnp.zeros((SX, 8, SZ), f32)
    for ref in (accf, accc, pad_v, mid_v, padc_v, midc_v, zt_v, dz_v, zsend):
        ref[...] = jnp.zeros(ref.shape, f32)

    def edge_row(row):
        return jnp.where(row < PY, row, jnp.where(row < PY + 2, row - PY - 2,
                         jnp.where(row < PY + 4, row - 2, row + 8 * PY)))

    def put(ref, index, value):
        high, low = split2(value)
        ref[(0,) + index] = high
        ref[(1,) + index] = low

    KV = SPF * SY
    cols = iota((QE, KV), 1)
    along_y = weight(cols % SY, edge_row(iota((QE, KV), 0)), SPF)
    along_x = weight(iota((8, KV), 1) // SY, iota((8, KV), 0) - 2, SPF)
    for p in range(5):
        put(wf_v, (slice(p * QE, (p + 1) * QE),), along_y * along_x[p:p + 1])
    rows, cols = iota((4 * QC, KV), 0), iota((4 * QC, KV), 1)
    along_y = weight(cols % SY + me[1] * SY, rows // 4, SPC)
    for ph in range(per):
        first = -2 if ph < per // 2 else -1
        along_x = weight(cols // SY + ph * SPF, rows % 4 + first, SPC)
        high, low = split2(along_x * along_y)
        wc_v[ph, 0] = high
        wc_v[ph, 1] = low

    pieces = ys_sem.shape[1]
    each = SX // pieces

    def neighbour_copy(k, side, src, dst, send, recv):
        other = me[k] - 1 if side == 0 else me[k] + 1
        return pltpu.make_async_remote_copy(
            src_ref=src, dst_ref=dst, send_sem=send, recv_sem=recv,
            device_id={AXES[k]: other}, device_id_type=MESH,
        )

    def halo(k, side, piece=0):
        if k == 1:
            part = pl.ds(piece * each, each)
            return neighbour_copy(
                k, side, ysend.at[side, :, part], yrecv.at[1 - side, :, part],
                ys_sem.at[side, piece], yr_sem.at[1 - side, piece])
        if k == 0:
            src = s_v.at[pl.ds(2 if side == 0 else SX, 2), pl.ds(8, SY), :]
            dst = s_v.at[pl.ds(SX + 2 if side == 0 else 0, 2), pl.ds(8, SY), :]
        else:
            src, dst = zsend.at[side], zrecv.at[1 - side]
        return neighbour_copy(k, side, src, dst, hs_sem.at[k, side], hr_sem.at[k, 1 - side])

    def start_halo(k, side, piece=0):
        @pl.when(has[k][side])
        def _():
            halo(k, side, piece).start()

    def wait_halo(k):
        for side in SIDES:
            for piece in range(pieces if k == 1 else 1):
                @pl.when(has[k][side])
                def _(side=side, piece=piece):
                    halo(k, side, piece).wait_send()

                @pl.when(has[k][1 - side])
                def _(side=side, piece=piece):
                    halo(k, side, piece).wait_recv()

    tile_lane = iota((16, SZ), 1)

    def pack(packs, value, x):
        value = pltpu.roll(value, (2 * x + 2) % SZ, 1)
        low = tile_lane // 2 == (x + 1) % (SZ // 2)
        return [jnp.where(low, value, packs[0]), jnp.where(tile_lane // 2 == x, value, packs[1])]

    srows = s_v.reshape((SX + 4) * (SY + 16), SZ)
    drows = w_v.reshape(SX * SY, SZ)

    def sums(group):
        for c in group:
            for copy in loads[c]:
                copy.wait()
        for y in range(0, SY, 16):
            rows = slice(y, y + 16)
            packs = [zsend[0, rows], zsend[1, rows]]
            for x in range(group[0] * SPF, (group[-1] + 1) * SPF):
                w, f = w_v[x, rows], f_v[x, rows]
                s = w + f
                w_v[x, rows] = w - f
                s_v[x + 2, 8 + y:24 + y] = s
                high, low = split2(s)
                parts_v[x * SY + y:x * SY + y + 16, 0:SZ] = high
                parts_v[x * SY + y:x * SY + y + 16, SZ:2 * SZ] = low
                packs = pack(packs, s, x)
            zsend[0, rows], zsend[1, rows] = packs

    def yfaces(piece):
        for side in SIDES:
            for k in range(2):
                y = k if side == 0 else SY - 2 + k
                ysend[side, k, pl.ds(piece * each, each)] = srows[
                    pl.ds((piece * each + 2) * (SY + 16) + 8 + y, each, stride=SY + 16), :]
            start_halo(1, side, piece)

    def forces(i, slot):
        slopes = dot(parts_v[i * KV:(i + 1) * KV], band_v[...])
        for y in range(0, SY, 16):
            rows = slice(8 + y, 24 + y)
            slabs = [s_v[i * SPF + x, rows] for x in range(SPF + 4)]
            packs = [dz_v[0, y:y + 16], dz_v[1, y:y + 16]]
            for xx in range(SPF):
                x = i * SPF + xx
                d = w_v[x, y:y + 16]
                packs = pack(packs, d, x)
                gx = slabs[xx] - slabs[xx + 4] + 8.0 * (slabs[xx + 3] - slabs[xx + 1])
                gy = (s_v[x + 2, 6 + y:22 + y] - s_v[x + 2, 10 + y:26 + y]
                      + 8.0 * (s_v[x + 2, 9 + y:25 + y] - s_v[x + 2, 7 + y:23 + y]))
                gz = slopes[xx * SY + y:xx * SY + y + 16]
                for a, g in enumerate((gx, gy, gz)):
                    at = (slot, slice(xx * SY + y, xx * SY + y + 16),
                          slice(a * SZ, (a + 1) * SZ))
                    fh_v[at], fl_v[at] = split2(g * d)
            dz_v[0, y:y + 16], dz_v[1, y:y + 16] = packs

    lane = iota((SY, SZ), 1)

    def gather(i, slot):
        k, ph = divmod(i, per)
        many = 5 * QE + 4 * QC
        weights = jnp.concatenate([wf_v[0], wc_v[ph, 0], wf_v[1], wc_v[ph, 1]], axis=0)
        both = dot(weights, fh_v[slot])
        out = both[:many] + both[many:] + dot(weights[:many], fl_v[slot])
        accf[i:i + 5] += out[:5 * QE].reshape(5, QE, lanes)
        at = k + (1 if ph >= per // 2 else 0)
        accc[:, at:at + 4] += out[5 * QE:].reshape(QC, 4, lanes)

    def run_sums(group):
        sums(group)
        summed.append(group)

    def run_faces():
        while summed:
            yfaces(summed.pop(0)[0] * SPF // each)

    summed = []
    for group in groups[:BEFORE]:
        run_sums(group)
    pl.semaphore_wait(barrier, total)
    for d in range(1, nz):
        pl.semaphore_signal(
            in_sem, inc=1, device_id={"gz": lax.rem(me[2] + d, nz)}, device_id_type=MESH)
    start_halo(0, 0)
    start_halo(0, 1)
    run_faces()
    for group in groups[BEFORE:]:
        run_sums(group)
        run_faces()
    start_halo(2, 0)
    start_halo(2, 1)

    KH = 4 * SX
    place = (iota((16, KH), 1) // SX)
    yat = jnp.where(place < 2, place, SY - 4 + place)
    along_y = weight(yat, edge_row(iota((16, KH), 0)), SPF)
    along_x = weight(iota((16, KH), 1) % SX, iota((16, KH), 0) - 2, SPF)
    turned = list(range(2, 2 + PX)) + [0, 1, PX + 2, PX + 3]
    for n, p in enumerate(turned):
        put(wy_v, (slice(n * QE, (n + 1) * QE),), along_y * along_x[p:p + 1])
    rows, cols = iota((NC, KH), 0), iota((NC, KH), 1)
    place = cols // SX
    yat = jnp.where(place < 2, place, SY - 4 + place)
    put(wy_v, (slice(NF, NF + NC),), weight(cols % SX, rows % XR - 2, SPC)
        * weight(yat + me[1] * SY, rows // XR, SPC))

    KP = 2 * SZ
    rows, cols = iota((QE, SY), 0), iota((QE, SY), 1)
    put(wq_v, (slice(0, QE),), weight(cols, edge_row(rows), SPF))
    rows, cols = iota((QC, SY), 0), iota((QC, SY), 1)
    put(wq_v, (slice(QE, QE + QC),), weight(cols + me[1] * SY, rows, SPC))
    col = iota((EX, KP), 1)
    xat = jnp.where(col < SZ, col, (col - 2) % SZ) // 2
    wx_v[0:EX] = weight(xat, iota((EX, KP), 0) - 2, SPF)
    wx_v[EX:EX + XR] = weight(xat[0:XR], iota((XR, KP), 0) - 2, SPC)

    def fine_lane(l):
        e = (l - 3 * PZ) % 8
        centre = l < 3 * PZ
        known = centre | ((l < 3 * PZ + 16) & (e < 6))
        comp = jnp.where(centre, l // PZ, jnp.where(known, e // 2, 3))
        point = jnp.where(centre, l % PZ, jnp.where(l < 3 * PZ + 8, e % 2 - 2, PZ + e % 2))
        return comp, point

    def both_levels(z):
        l = iota(z.shape, 1)[:, 0:LW]
        z = z[:, 0:LW]
        comp, point = fine_lane(l)
        fine = weight(z, point, SPF) * (SPF ** -1.5 / 24.0)
        ccomp = l // ZC
        coarse = weight(z, l % ZC - 2, SPC) * (SPC ** -1.5 / 24.0)
        return jnp.concatenate([comp, ccomp], 1), jnp.concatenate([fine, coarse], 1)

    comp, value = both_levels(iota((SZ, 2 * LW), 0))
    high, low = split2(value)
    high, low = high.astype(f32), low.astype(f32)
    for a in range(3):
        part = slice(a * SZ, (a + 1) * SZ)
        wz_v[0, part] = jnp.where(comp == a, high, 0.0).astype(bf16)
        wz_v[1, part] = jnp.where(comp == a, low, 0.0).astype(bf16)
    row = iota((8, 2 * LW), 0)
    comp, value = both_levels(jnp.where(row < 2, row, SZ - 4 + row))
    value = jnp.where(comp == 2, value, 0.0)
    odd = iota((SZ, 2 * LW), 0) % 2 == 1
    for side in SIDES:
        part = slice(side * SZ, (side + 1) * SZ)
        put(wh_v, (part,), jnp.where(odd, value[2 * side + 1:2 * side + 2],
                                     value[2 * side:2 * side + 1]))

    step = iota((SZ, SZ), 1) - iota((SZ, SZ), 0)
    band = (jnp.where(step == 2, 1.0, 0.0) - jnp.where(step == 1, 8.0, 0.0)
            + jnp.where(step == -1, 8.0, 0.0) - jnp.where(step == -2, 1.0, 0.0)).astype(bf16)
    band_v[0:SZ] = band
    band_v[SZ:2 * SZ] = band

    for copy in small:
        copy.wait()

    def spread(ref, a, count, width, matrix):
        block = ref[a].reshape(count, width)
        return sum(dot(part, matrix) for part in split3(block))

    zin, l = iota((PZ, LW), 0), iota((PZ, LW), 1)
    comp, point = fine_lane(l)
    oz = me[2] * PZ
    shares = 0.0
    for a in range(3):
        m = jnp.concatenate([same(point, zin), 2.0 * diff1(point, zin),
                             diff2(point + oz, zin + oz, PZ * nz)], 1)
        ok = jnp.concatenate([comp == a] * 3, 1)
        shares = shares + spread(fc_ref, a, PX * PY, PZ, jnp.where(ok, m, 0.0).astype(bf16))
    shares = shares.reshape(PX, PY, 3 * LW)
    pad_v[3:3 + PX, 8:8 + PY, :] = shares[:, :, 0:LW]
    inside = iota((PY + 8, LW), 0) - 4 + me[1] * PY
    inside = (inside >= 0) & (inside < PY * ny)
    for p in range(-1, PX + 1):
        u, _ = cross(pad_v, 3 + p, (4, PY + 8))
        keep = inside & (me[0] * PX + p >= 0) & (me[0] * PX + p < PX * nx)
        mid_v[3 + p, 4:12 + PY] = jnp.where(keep, u, 0.0)
    mid_v[3:3 + PX, 8:8 + PY, :] = mid_v[3:3 + PX, 8:8 + PY, :] + shares[:, :, LW:2 * LW]
    row = iota((PY, LW), 0)
    for p in range(-2, PX + 2):
        v = [cross(mid_v, 3 + p, (first, PY))[0] for first in (8, 6, 6 + PY)]
        centre = v[0]
        if 0 <= p < PX:
            centre = centre + shares[p, :, 2 * LW:3 * LW]
        at = turned.index(2 + p)
        bend_v[at, 0:PY] = centre * BEND
        bend_v[at, PY:2 * PY] = jnp.where(
            row < 2, v[1], jnp.where(row < 4, v[2], 0.0)) * BEND

    turn = list(range(1, cells - 1)) + [0, cells - 1]
    forces(turn[0], 0)
    for n, i in enumerate(turn):
        if n + 1 < cells:
            if turn[n + 1] == 0:
                wait_halo(0)
            forces(turn[n + 1], (n + 1) % 2)
        gather(i, n % 2)

    table = jnp.concatenate(
        [accf[2:2 + PX].reshape(PX * QE, lanes), accf[0:2].reshape(2 * QE, lanes),
         accf[2 + PX:].reshape(2 * QE, lanes), accc[...].reshape(NC, lanes)], 0)
    parts = split2(table)
    both = ((slice(0, NF), slice(0, LW)), (slice(NF, NF + NC), slice(LW, 2 * LW)))
    for rows, cols in both:
        whole_v[rows] = thrice((parts[0][rows], parts[1][rows]),
                               (wz_v[0, :, cols], wz_v[1, :, cols]))
    whole_v[0:NF] = whole_v[0:NF] + bend_v[...].reshape(NF, LW)
    dlow, dhigh = pltpu.roll(dz_v[0], SZ - 2, 1), pltpu.roll(dz_v[1], 2, 1)

    wait_halo(1)
    wait_halo(2)
    adds = []
    for side in SIDES:
        h0, h1 = yrecv[side, 0], yrecv[side, 1]
        g = (h0 - 8.0 * h1, h1) if side == 0 else (-h0, 8.0 * h0 - h1)
        for k in range(2):
            y = k if side == 0 else SY - 2 + k
            at = pl.ds(y, SX, stride=SY)
            adds.append(g[k] * drows[at, :])
    faces = split2(jnp.concatenate(adds, 0))
    even = lane % 2 == 0
    hl, hh = zrecv[0], zrecv[1]
    cl = jnp.where(even, hl - 8.0 * pltpu.roll(hl, SZ - 1, 1), hl)
    ch = jnp.where(even, -hh, 8.0 * pltpu.roll(hh, 1, 1) - hh)
    g = thrice(wq_v, split2(jnp.concatenate([cl * dlow, ch * dhigh], 1)))

    def with_halos(rows, cols, blocks):
        added = thrice((wy_v[0, rows], wy_v[1, rows]), faces)
        part = slice(SZ, 2 * SZ)
        return whole_v[rows] + (
            thrice(split2(added), (wz_v[0, part, cols], wz_v[1, part, cols]))
            + thrice(split2(jnp.concatenate(blocks, 0)), (wh_v[0, :, cols], wh_v[1, :, cols])))

    coarse = with_halos(
        *both[1], [g[QE + q:QE + q + 1] * wx_v[EX:EX + XR] for q in range(QC)])

    pl.semaphore_wait(in_sem, nz - 1)

    mine = (me[0] * ny + me[1]) * nz + me[2]
    count = nx * ny * nz - 1

    def coarse_wait(sem):
        ref = all_v.at[pl.ds(0, count)]
        pltpu.make_async_copy(ref, ref, sem).wait()

    def coarse_copy(o, at):
        return pltpu.make_async_remote_copy(
            src_ref=all_v.at[at], dst_ref=all_v.at[at],
            send_sem=cs_sem, recv_sem=cr_sem,
            device_id=tuple(lax.rem(me[k] + o[k], sizes[k]) for k in range(3)),
            device_id_type=MESH)

    everyone = [(ox, oy, oz) for ox in range(nx) for oy in range(ny) for oz in range(nz)][1:]
    far = sorted(everyone, key=lambda o: -sum(min(o[k], sizes[k] - o[k]) for k in range(3)))
    for v in range(0, QC, PG):
        share = 0.0
        for q in range(v, min(v + PG, QC)):
            tile = coarse[q * XR:(q + 1) * XR]
            share = share + (tile if q == v else pltpu.roll(tile, (q - v) * GL, 1))
        all_v[mine, v // PG] = share[0:XC]

    @pl.when(me[0] >= 0)
    def _():
        for o in far:
            coarse_copy(o, mine).start()

    fine = with_halos(*both[0], [g[0:QE] * wx_v[p:p + 1] for p in turned])
    tall = jnp.concatenate([fine, jnp.zeros((2 * LW - NF, LW), f32)], 0).T
    fine = fine.reshape(EX, QE, LW)
    for side in SIDES:
        at = 3 * PZ + 8 * side
        for half in range(2):
            zm_v[side, half] = tall[at:at + 8, half * LW:(half + 1) * LW]
        at = PX + 2 * side
        xm_v[side] = fine[at:at + 2, 0:PY]
    ym_v[...] = fine[:, PY:PY + 4]

    def fine_copy(dx, dy, dz):
        xs, ys, zs = (0 if d > 0 else 1 for d in (dx, dy, dz))
        if dz:
            src = zm_v.at[1 - zs, 1 if dx else 0]
            dst = zg_v.at[zs, 1 - dx, 1 - dy]
        elif dy == 0:
            src, dst = xm_v.at[1 - xs], xg_v.at[xs]
        elif dx == 0:
            src, dst = ym_v.at[pl.ds(0, PX)], yg_v.at[ys]
        else:
            src, dst = ym_v.at[pl.ds(PX if dx < 0 else PX + 2, 2)], cg_v.at[xs, ys]
        at = (dx + 1, dy + 1, dz + 1)
        return pltpu.make_async_remote_copy(
            src_ref=src, dst_ref=dst, send_sem=as_sem.at[at], recv_sem=ar_sem.at[at],
            device_id=(me[0] + dx, me[1] + dy, me[2] + dz), device_id_type=MESH)

    def there(step):
        ok = None
        for k in range(3):
            if step[k]:
                here = has[k][0 if step[k] < 0 else 1]
                ok = here if ok is None else ok & here
        return ok

    for step in AROUND:
        @pl.when(there(step))
        def _(step=step):
            fine_copy(*step).start()

    zin, l = iota((KZ, LW), 0), iota((KZ, LW), 1)
    shares = 0.0
    for a in range(3):
        m = jnp.concatenate([same(l % KZ, zin), 2.0 * diff1(l % KZ, zin),
                             diff2(l % KZ, zin, KZ)], 1)
        ok = jnp.concatenate([l // KZ == a] * 3, 1)
        shares = shares + spread(cc_ref, a, KX * KY, KZ, jnp.where(ok, m, 0.0).astype(bf16))
    shares = shares.reshape(KX, KY, 3 * LW)
    padc_v[1:1 + KX, 8:8 + KY, :] = shares[:, :, 0:LW]
    for p in range(KX):
        midc_v[1 + p, 8:8 + KY] = (
            cross(padc_v, 1 + p, (8, KY))[0] + shares[p, :, LW:2 * LW])
    for p in range(KX):
        out = (cross(midc_v, 1 + p, (8, KY))[0] + shares[p, :, 2 * LW:]) * BEND
        for a in range(3):
            co_ref[a, p * KY:(p + 1) * KY] = (
                out if a == 0 else pltpu.roll(out, LW - a * KZ, 1))

    for step in AROUND:
        back = tuple(-d for d in step)

        @pl.when(there(back))
        def _(step=step):
            fine_copy(*step).wait_recv()
    tile = iota((8, LW), 1)
    x, y = tile // QE, tile % QE
    for side in SIDES:
        got = 0.0
        for sx in STEPS:
            shift = {-1: -2 * QE, 0: 0, 1: (PX - 2) * QE}[sx]
            xin = {-1: x < 2, 0: x < PX, 1: x >= PX - 2}[sx]
            for sy in STEPS:
                yin = {-1: y < 2, 0: y < PY, 1: (y >= PY - 2) & (y < PY)}[sy]
                turn = (shift + {-1: -PY - 2, 0: 0, 1: -2}[sy]) % LW
                value = zg_v[side, 1 + sx, 1 + sy]
                value = pltpu.roll(value, turn, 1) if turn else value
                got = got + jnp.where(xin & yin, value, 0.0)
        for a in range(3):
            at = a * PZ + side * (PZ - 2)
            zt_v[at:at + 2] = got[2 * a:2 * a + 2]
    across = zt_v[...].T.reshape(PX, QE, LW)
    row = iota((PY, LW), 0)
    for p in range(PX):
        out = fine[p, 0:PY] + across[p, 0:PY]
        low, high = yg_v[0, p], yg_v[1, p]
        for side in SIDES:
            q = p if side == 0 else p - (PX - 2)
            if 0 <= q < 2:
                out = out + xg_v[side, q]
                low, high = low + cg_v[side, 0, q], high + cg_v[side, 1, q]
        fill = jnp.zeros((PY - 4, LW), f32)
        low = pltpu.roll(jnp.concatenate([low, fill], 0), PY - 2, 0)
        high = pltpu.roll(jnp.concatenate([high, fill], 0), PY - 2, 0)
        out = out + jnp.where(row < 2, low, jnp.where(row >= PY - 2, high, 0.0))
        for a in range(3):
            fo_ref[a, p] = (out if a == 0 else pltpu.roll(out, LW - a * PZ, 1))[:, 0:PZ]

    for step in AROUND:
        @pl.when(there(step))
        def _(step=step):
            fine_copy(*step).wait_send()
    if count:
        coarse_wait(cs_sem)
        coarse_wait(cr_sem)
    row = iota((XR, LW), 0)
    for v in range(0, QC, PG):
        for b in range(0, KX, XR):
            placed = []
            for iz in range(nz):
                here = 0.0
                for ix in range(nx):
                    first = CX * ix - 2 - b
                    if first <= -XC or first >= XR:
                        continue
                    block = all_v[ix * ny * nz + iz, v // PG]
                    for iy in range(1, ny):
                        block = block + all_v[(ix * ny + iy) * nz + iz, v // PG]
                    block = jnp.concatenate([block, jnp.zeros((XR - XC, LW), f32)], 0)
                    block = pltpu.roll(block, first % XR, 0)
                    here = here + jnp.where((row >= first) & (row < first + XC), block, 0.0)
                placed.append(here)
            for q in range(v, min(v + PG, QC)):
                for a in range(3):
                    out = 0.0
                    for iz in range(nz):
                        first = CZ * iz - 2
                        value = pltpu.roll(placed[iz], (first - (q - v) * GL - a * ZC) % LW, 1)
                        inside = (tile >= first) & (tile < first + ZC)
                        out = out + jnp.where(inside, value, 0.0)
                    at = pl.ds(b * KY + q, XR, stride=KY)
                    co_ref[a, at, :] = co_ref[a, at, :] + out


def write_out(f_ref, c_ref, fo_ref, co_ref):
    fo_ref[...] = f_ref[...]
    KX, KY, KZ = co_ref.shape[1:]
    for a in range(3):
        for p in range(KX):
            co_ref[a, p] = c_ref[a, p * KY:(p + 1) * KY, 0:KZ]


def solution(mesh):
    sizes = tuple(mesh.shape[a] for a in AXES)

    def step(warped, fixed, fine, coarse):
        SX, SY, SZ = warped.shape
        PX, PY, PZ = SX // SPF, SY // SPF, SZ // SPF
        KX, KY, KZ = coarse.shape[1:]
        nx, ny, nz = sizes
        EX, QE = PX + 4, PY + 8
        XR, QC = -(-(SX // SPC + 4) // 8) * 8, KY
        KV = SPF * SY
        NF, NC, LW = EX * QE, XR * QC, 128
        vmem = pl.BlockSpec(memory_space=pltpu.VMEM)
        hbm = pl.BlockSpec(memory_space=pltpu.HBM)
        V = pltpu.VMEM
        D = pltpu.SemaphoreType.DMA
        held = pl.pallas_call(
            functools.partial(kernel, sizes),
            out_shape=(pltpu.VMEM(fine.shape, f32), pltpu.VMEM((3, KX * KY, LW), f32)),
            in_specs=[hbm] * 4,
            out_specs=(vmem, vmem),
            scratch_shapes=[
                V((SX, SY, SZ), f32), V((SX, SY, SZ), f32),
                V((3, PX, PY, PZ), f32), V(coarse.shape, f32),
                V((SX + 4, SY + 16, SZ), f32),
                V((2, 2, SX, SZ), f32), V((2, 2, SX, SZ), f32),
                V((2, SY, SZ), f32), V((2, SY, SZ), f32), V((2, SY, SZ), f32),
                V((2, 5 * QE, KV), bf16), V((SPC // SPF, 2, 4 * QC, KV), bf16),
                V((2, NF + NC, 4 * SX), bf16), V((2, QE + QC, SY), bf16),
                V((EX + XR, 2 * SZ), f32),
                V((2, 3 * SZ, 2 * LW), bf16), V((2, 2 * SZ, 2 * LW), bf16),
                V((2, KV, 3 * SZ), bf16), V((2, KV, 3 * SZ), bf16),
                V((SX * SY, 2 * SZ), bf16), V((2 * SZ, SZ), bf16),
                V((EX, QE, 3 * SZ), f32), V((QC, XR, 3 * SZ), f32),
                V((NF + NC, LW), f32),
                V((PX + 6, PY + 16, LW), f32), V((PX + 6, PY + 16, LW), f32),
                V((EX, QE, LW), f32),
                V((KX + 2, KY + 16, LW), f32), V((KX + 2, KY + 16, LW), f32),
                V((2, 2, 8, LW), f32), V((2, 3, 3, 8, LW), f32), V((LW, LW), f32),
                V((2, 2, PY, LW), f32), V((EX, 4, LW), f32),
                V((2, 2, PY, LW), f32), V((2, PX, 4, LW), f32), V((2, 2, 2, 4, LW), f32),
                V((nx * ny * nz, -(-QC // 4), SX // SPC + 4, LW), f32),
                D((2, SX // SPF)), D((2,)), D((3, 2)), D((3, 2)), D((2, 4)), D((2, 4)),
                D((3, 3, 3)), D((3, 3, 3)), D(()), D(()), pltpu.SemaphoreType.REGULAR,
            ],
            compiler_params=pltpu.CompilerParams(
                collective_id=0, has_side_effects=True, vmem_limit_bytes=64000000
            ),
        )(warped, fixed, fine, coarse)
        held = [pltpu.with_memory_space_constraint(h, memory_space=pltpu.VMEM) for h in held]
        return pl.pallas_call(
            write_out,
            out_shape=(jax.ShapeDtypeStruct(fine.shape, f32),
                       jax.ShapeDtypeStruct(coarse.shape, f32)),
            in_specs=[vmem] * 2,
            out_specs=(vmem, vmem),
        )(*held)

    in_specs = (P("gx", "gy", "gz"), P("gx", "gy", "gz"), P(None, "gx", "gy", "gz"), P())
    out_specs = (P(None, "gx", "gy", "gz"), P())
    return jax.shard_map(
        step, mesh=mesh, in_specs=in_specs, out_specs=out_specs, check_vma=False
    )
```

```python
import functools

import jax
import jax.numpy as jnp
from jax import lax
from jax.experimental import pallas as pl
from jax.experimental.pallas import tpu as pltpu
from jax.sharding import PartitionSpec as P

SPF = 8
SPC = 32
BEND = 0.01
MESH = pl.DeviceIdType.MESH
f32 = jnp.float32
bf16 = jnp.bfloat16
AXES = ("gx", "gy", "gz")
SIDES = (0, 1)
BEFORE = 2
STEPS = (-1, 0, 1)
AROUND = sorted(
    ((dx, dy, dz) for dx in STEPS for dy in STEPS for dz in STEPS if dx or dy or dz),
    key=lambda d: -sum(map(abs, d)))


def dot(a, b):
    return jnp.dot(a, b, preferred_element_type=f32)


def spline(t):
    m = jnp.abs(t)
    inner = 2.0 / 3.0 - m * m + 0.5 * m * m * m
    r = jnp.maximum(2.0 - m, 0.0)
    outer = r * r * r * (1.0 / 6.0)
    return jnp.where(m < 1.0, inner, outer)


def weight(voxel, point, spacing):
    scaled = (2 * voxel + 1 - spacing * (2 * point + 1)).astype(f32)
    return spline(scaled * (0.5 / spacing))


def iota(shape, axis):
    return lax.broadcasted_iota(jnp.int32, shape, axis)


def split2(value):
    high = value.astype(bf16)
    return high, (value - high.astype(f32)).astype(bf16)


def thrice(a, b):
    return dot(a[0], b[0]) + dot(a[1], b[0]) + dot(a[0], b[1])


def split3(value):
    high = value.astype(bf16)
    rest = value - high.astype(f32)
    mid = rest.astype(bf16)
    return high, mid, (rest - mid.astype(f32)).astype(bf16)


def same(out, inp):
    return jnp.where(out == inp, 1.0, 0.0).astype(f32)


def diff1(out, inp):
    d = jnp.abs(out - inp)
    return jnp.where(d == 0, -2.0, jnp.where(d == 1, 1.0, 0.0)).astype(f32)


def diff2(out, inp, count):
    d = jnp.abs(out - inp)
    edge = (inp == 0) | (inp == count - 1)
    centre = jnp.where(edge, 5.0, 6.0)
    return jnp.where(
        d == 0, centre, jnp.where(d == 1, -4.0, jnp.where(d == 2, 1.0, 0.0))
    ).astype(f32)


def cross(ref, x, rows):
    first, count = rows
    here = ref[x, first:first + count]
    return (ref[x - 1, first:first + count] + ref[x + 1, first:first + count]
            + ref[x, first - 1:first - 1 + count] + ref[x, first + 1:first + 1 + count]
            - 4.0 * here), here


def kernel(sizes, w_hbm, f_hbm, fc_hbm, cc_hbm, fo_ref, co_ref,
           w_v, f_v, fc_ref, cc_ref, s_v, ysend, yrecv, zsend, zrecv, dz_v,
           wf_v, wc_v, wy_v, wq_v, wx_v, wz_v, wh_v, fh_v, fl_v, parts_v, band_v,
           accf, accc, whole_v, pad_v, mid_v, bend_v, padc_v, midc_v,
           zm_v, zg_v, zt_v, xm_v, ym_v, xg_v, yg_v, cg_v, all_v,
           load_sem, small_sem, hs_sem, hr_sem, ys_sem, yr_sem,
           as_sem, ar_sem, cs_sem, cr_sem, in_sem):
    nx, ny, nz = sizes
    me = [lax.axis_index(a) for a in AXES]
    SX, SY, SZ = w_v.shape
    PX, PY, PZ = SX // SPF, SY // SPF, SZ // SPF
    KX, KY, KZ = cc_ref.shape[1:]
    EX, QE = PX + 4, PY + 8
    QC, XR = accc.shape[:2]
    CX, CZ = SX // SPC, SZ // SPC
    XC, ZC = CX + 4, CZ + 4
    GL = 32
    PG = 128 // GL
    cells = SX // SPF
    per = SPC // SPF
    lanes = 3 * SZ
    NF, NC = EX * QE, QC * XR
    LW = 128
    has = [(me[k] > 0, me[k] < sizes[k] - 1) for k in range(3)]

    small = (pltpu.make_async_copy(fc_hbm, fc_ref, small_sem.at[0]),
             pltpu.make_async_copy(cc_hbm, cc_ref, small_sem.at[1]))
    for copy in small:
        copy.start()
    loads = []
    groups = [(0, 1), (cells - 2, cells - 1)]
    groups += [(c, c + 1) for c in range(2, cells - 2, 2)]
    for n, group in enumerate(groups):
        part = pl.ds(group[0] * SPF, len(group) * SPF)
        loads.append((
            pltpu.make_async_copy(w_hbm.at[part], w_v.at[part], load_sem.at[0, n]),
            pltpu.make_async_copy(f_hbm.at[part], f_v.at[part], load_sem.at[1, n]),
        ))
        for copy in loads[n]:
            copy.start()

    for at in (0, SX + 2):
        s_v[at:at + 2, 8:8 + SY, :] = jnp.zeros((2, SY, SZ), f32)
    for ref in (yrecv, zrecv, xg_v, yg_v, cg_v, zg_v):
        ref[...] = jnp.zeros(ref.shape, f32)

    barrier = pltpu.get_barrier_semaphore()
    total = 0
    plane = [(ox, oy) for ox in range(nx) for oy in range(ny) if ox or oy]

    def in_plane(ox, oy):
        return {"gx": lax.rem(me[0] + ox, nx), "gy": lax.rem(me[1] + oy, ny)}

    for d in range(1, nz):
        pl.semaphore_signal(
            barrier, inc=1, device_id={"gz": lax.rem(me[2] + d, nz)}, device_id_type=MESH)
        total += 1
    for ox, oy in plane:
        pl.semaphore_signal(barrier, inc=1, device_id=in_plane(ox, oy), device_id_type=MESH)
        total += 1

    s_v[2:SX + 2, 0:8, :] = jnp.zeros((SX, 8, SZ), f32)
    s_v[2:SX + 2, 8 + SY:16 + SY, :] = jnp.zeros((SX, 8, SZ), f32)
    for ref in (accf, accc, pad_v, mid_v, padc_v, midc_v, zt_v, dz_v, zsend):
        ref[...] = jnp.zeros(ref.shape, f32)

    def edge_row(row):
        return jnp.where(row < PY, row, jnp.where(row < PY + 2, row - PY - 2,
                         jnp.where(row < PY + 4, row - 2, row + 8 * PY)))

    def put(ref, index, value):
        high, low = split2(value)
        ref[(0,) + index] = high
        ref[(1,) + index] = low

    KV = SPF * SY
    cols = iota((QE, KV), 1)
    along_y = weight(cols % SY, edge_row(iota((QE, KV), 0)), SPF)
    along_x = weight(iota((8, KV), 1) // SY, iota((8, KV), 0) - 2, SPF)
    for p in range(5):
        put(wf_v, (slice(p * QE, (p + 1) * QE),), along_y * along_x[p:p + 1])
    rows, cols = iota((4 * QC, KV), 0), iota((4 * QC, KV), 1)
    along_y = weight(cols % SY + me[1] * SY, rows // 4, SPC)
    for ph in range(per):
        first = -2 if ph < per // 2 else -1
        along_x = weight(cols // SY + ph * SPF, rows % 4 + first, SPC)
        high, low = split2(along_x * along_y)
        wc_v[ph, 0] = high
        wc_v[ph, 1] = low

    pieces = ys_sem.shape[1]
    each = SX // pieces

    def neighbour_copy(k, side, src, dst, send, recv):
        other = me[k] - 1 if side == 0 else me[k] + 1
        return pltpu.make_async_remote_copy(
            src_ref=src, dst_ref=dst, send_sem=send, recv_sem=recv,
            device_id={AXES[k]: other}, device_id_type=MESH,
        )

    def halo(k, side, piece=0):
        if k == 1:
            part = pl.ds(piece * each, each)
            return neighbour_copy(
                k, side, ysend.at[side, :, part], yrecv.at[1 - side, :, part],
                ys_sem.at[side, piece], yr_sem.at[1 - side, piece])
        if k == 0:
            src = s_v.at[pl.ds(2 if side == 0 else SX, 2), pl.ds(8, SY), :]
            dst = s_v.at[pl.ds(SX + 2 if side == 0 else 0, 2), pl.ds(8, SY), :]
        else:
            src, dst = zsend.at[side], zrecv.at[1 - side]
        return neighbour_copy(k, side, src, dst, hs_sem.at[k, side], hr_sem.at[k, 1 - side])

    def start_halo(k, side, piece=0):
        @pl.when(has[k][side])
        def _():
            halo(k, side, piece).start()

    def wait_halo(k):
        for side in SIDES:
            for piece in range(pieces if k == 1 else 1):
                @pl.when(has[k][side])
                def _(side=side, piece=piece):
                    halo(k, side, piece).wait_send()

                @pl.when(has[k][1 - side])
                def _(side=side, piece=piece):
                    halo(k, side, piece).wait_recv()

    tile_lane = iota((16, SZ), 1)

    def pack(packs, value, x):
        value = pltpu.roll(value, (2 * x + 2) % SZ, 1)
        low = tile_lane // 2 == (x + 1) % (SZ // 2)
        return [jnp.where(low, value, packs[0]), jnp.where(tile_lane // 2 == x, value, packs[1])]

    srows = s_v.reshape((SX + 4) * (SY + 16), SZ)
    drows = w_v.reshape(SX * SY, SZ)

    def sums(group):
        for copy in loads[groups.index(group)]:
            copy.wait()
        for y in range(0, SY, 16):
            rows = slice(y, y + 16)
            packs = [zsend[0, rows], zsend[1, rows]]
            for x in range(group[0] * SPF, (group[-1] + 1) * SPF):
                w, f = w_v[x, rows], f_v[x, rows]
                s = w + f
                w_v[x, rows] = w - f
                s_v[x + 2, 8 + y:24 + y] = s
                high, low = split2(s)
                parts_v[x * SY + y:x * SY + y + 16, 0:SZ] = high
                parts_v[x * SY + y:x * SY + y + 16, SZ:2 * SZ] = low
                packs = pack(packs, s, x)
            zsend[0, rows], zsend[1, rows] = packs

    def yfaces(piece):
        for side in SIDES:
            for k in range(2):
                y = k if side == 0 else SY - 2 + k
                ysend[side, k, pl.ds(piece * each, each)] = srows[
                    pl.ds((piece * each + 2) * (SY + 16) + 8 + y, each, stride=SY + 16), :]
            start_halo(1, side, piece)

    def forces(i, slot):
        slopes = dot(parts_v[i * KV:(i + 1) * KV], band_v[...])
        for y in range(0, SY, 16):
            rows = slice(8 + y, 24 + y)
            slabs = [s_v[i * SPF + x, rows] for x in range(SPF + 4)]
            packs = [dz_v[0, y:y + 16], dz_v[1, y:y + 16]]
            for xx in range(SPF):
                x = i * SPF + xx
                d = w_v[x, y:y + 16]
                packs = pack(packs, d, x)
                gx = slabs[xx] - slabs[xx + 4] + 8.0 * (slabs[xx + 3] - slabs[xx + 1])
                gy = (s_v[x + 2, 6 + y:22 + y] - s_v[x + 2, 10 + y:26 + y]
                      + 8.0 * (s_v[x + 2, 9 + y:25 + y] - s_v[x + 2, 7 + y:23 + y]))
                gz = slopes[xx * SY + y:xx * SY + y + 16]
                for a, g in enumerate((gx, gy, gz)):
                    at = (slot, slice(xx * SY + y, xx * SY + y + 16),
                          slice(a * SZ, (a + 1) * SZ))
                    fh_v[at], fl_v[at] = split2(g * d)
            dz_v[0, y:y + 16], dz_v[1, y:y + 16] = packs

    lane = iota((SY, SZ), 1)

    def gather(i, slot):
        k, ph = divmod(i, per)
        many = 5 * QE + 4 * QC
        weights = jnp.concatenate([wf_v[0], wc_v[ph, 0], wf_v[1], wc_v[ph, 1]], axis=0)
        both = dot(weights, fh_v[slot])
        out = both[:many] + both[many:] + dot(weights[:many], fl_v[slot])
        accf[i:i + 5] += out[:5 * QE].reshape(5, QE, lanes)
        at = k + (1 if ph >= per // 2 else 0)
        accc[:, at:at + 4] += out[5 * QE:].reshape(QC, 4, lanes)

    def run_sums(group):
        sums(group)
        summed.append(group)

    def run_faces():
        while summed:
            yfaces(summed.pop(0)[0] * SPF // each)

    summed = []
    for group in groups[:BEFORE]:
        run_sums(group)
    pl.semaphore_wait(barrier, total)
    for d in range(1, nz):
        pl.semaphore_signal(
            in_sem, inc=1, device_id={"gz": lax.rem(me[2] + d, nz)}, device_id_type=MESH)
    start_halo(0, 0)
    start_halo(0, 1)
    run_faces()
    for group in groups[BEFORE:]:
        run_sums(group)
        run_faces()
    start_halo(2, 0)
    start_halo(2, 1)

    KH = 4 * SX
    place = (iota((16, KH), 1) // SX)
    yat = jnp.where(place < 2, place, SY - 4 + place)
    along_y = weight(yat, edge_row(iota((16, KH), 0)), SPF)
    along_x = weight(iota((16, KH), 1) % SX, iota((16, KH), 0) - 2, SPF)
    turned = list(range(2, 2 + PX)) + [0, 1, PX + 2, PX + 3]
    for n, p in enumerate(turned):
        put(wy_v, (slice(n * QE, (n + 1) * QE),), along_y * along_x[p:p + 1])
    rows, cols = iota((NC, KH), 0), iota((NC, KH), 1)
    place = cols // SX
    yat = jnp.where(place < 2, place, SY - 4 + place)
    put(wy_v, (slice(NF, NF + NC),), weight(cols % SX, rows % XR - 2, SPC)
        * weight(yat + me[1] * SY, rows // XR, SPC))

    KP = 2 * SZ
    rows, cols = iota((QE, SY), 0), iota((QE, SY), 1)
    put(wq_v, (slice(0, QE),), weight(cols, edge_row(rows), SPF))
    rows, cols = iota((QC, SY), 0), iota((QC, SY), 1)
    put(wq_v, (slice(QE, QE + QC),), weight(cols + me[1] * SY, rows, SPC))
    col = iota((EX, KP), 1)
    xat = jnp.where(col < SZ, col, (col - 2) % SZ) // 2
    wx_v[0:EX] = weight(xat, iota((EX, KP), 0) - 2, SPF)
    wx_v[EX:EX + XR] = weight(xat[0:XR], iota((XR, KP), 0) - 2, SPC)

    def fine_lane(l):
        e = (l - 3 * PZ) % 8
        centre = l < 3 * PZ
        known = centre | ((l < 3 * PZ + 16) & (e < 6))
        comp = jnp.where(centre, l // PZ, jnp.where(known, e // 2, 3))
        point = jnp.where(centre, l % PZ, jnp.where(l < 3 * PZ + 8, e % 2 - 2, PZ + e % 2))
        return comp, point

    def both_levels(z):
        l = iota(z.shape, 1)[:, 0:LW]
        z = z[:, 0:LW]
        comp, point = fine_lane(l)
        fine = weight(z, point, SPF) * (SPF ** -1.5 / 24.0)
        ccomp = l // ZC
        coarse = weight(z, l % ZC - 2, SPC) * (SPC ** -1.5 / 24.0)
        return jnp.concatenate([comp, ccomp], 1), jnp.concatenate([fine, coarse], 1)

    comp, value = both_levels(iota((SZ, 2 * LW), 0))
    high, low = split2(value)
    high, low = high.astype(f32), low.astype(f32)
    for a in range(3):
        part = slice(a * SZ, (a + 1) * SZ)
        wz_v[0, part] = jnp.where(comp == a, high, 0.0).astype(bf16)
        wz_v[1, part] = jnp.where(comp == a, low, 0.0).astype(bf16)
    row = iota((8, 2 * LW), 0)
    comp, value = both_levels(jnp.where(row < 2, row, SZ - 4 + row))
    value = jnp.where(comp == 2, value, 0.0)
    odd = iota((SZ, 2 * LW), 0) % 2 == 1
    for side in SIDES:
        part = slice(side * SZ, (side + 1) * SZ)
        put(wh_v, (part,), jnp.where(odd, value[2 * side + 1:2 * side + 2],
                                     value[2 * side:2 * side + 1]))

    step = iota((SZ, SZ), 1) - iota((SZ, SZ), 0)
    band = (jnp.where(step == 2, 1.0, 0.0) - jnp.where(step == 1, 8.0, 0.0)
            + jnp.where(step == -1, 8.0, 0.0) - jnp.where(step == -2, 1.0, 0.0)).astype(bf16)
    band_v[0:SZ] = band
    band_v[SZ:2 * SZ] = band

    for copy in small:
        copy.wait()

    def spread(ref, a, count, width, matrix):
        block = ref[a].reshape(count, width)
        return sum(dot(part, matrix) for part in split3(block))

    zin, l = iota((PZ, LW), 0), iota((PZ, LW), 1)
    comp, point = fine_lane(l)
    oz = me[2] * PZ
    shares = 0.0
    for a in range(3):
        m = jnp.concatenate([same(point, zin), 2.0 * diff1(point, zin),
                             diff2(point + oz, zin + oz, PZ * nz)], 1)
        ok = jnp.concatenate([comp == a] * 3, 1)
        shares = shares + spread(fc_ref, a, PX * PY, PZ, jnp.where(ok, m, 0.0).astype(bf16))
    shares = shares.reshape(PX, PY, 3 * LW)
    pad_v[3:3 + PX, 8:8 + PY, :] = shares[:, :, 0:LW]
    inside = iota((PY + 8, LW), 0) - 4 + me[1] * PY
    inside = (inside >= 0) & (inside < PY * ny)
    for p in range(-1, PX + 1):
        u, _ = cross(pad_v, 3 + p, (4, PY + 8))
        keep = inside & (me[0] * PX + p >= 0) & (me[0] * PX + p < PX * nx)
        mid_v[3 + p, 4:12 + PY] = jnp.where(keep, u, 0.0)
    mid_v[3:3 + PX, 8:8 + PY, :] = mid_v[3:3 + PX, 8:8 + PY, :] + shares[:, :, LW:2 * LW]
    row = iota((PY, LW), 0)
    for p in range(-2, PX + 2):
        v = [cross(mid_v, 3 + p, (first, PY))[0] for first in (8, 6, 6 + PY)]
        centre = v[0]
        if 0 <= p < PX:
            centre = centre + shares[p, :, 2 * LW:3 * LW]
        at = turned.index(2 + p)
        bend_v[at, 0:PY] = centre * BEND
        bend_v[at, PY:2 * PY] = jnp.where(
            row < 2, v[1], jnp.where(row < 4, v[2], 0.0)) * BEND

    turn = list(range(1, cells - 1)) + [0, cells - 1]
    forces(turn[0], 0)
    for n, i in enumerate(turn):
        if n + 1 < cells:
            if turn[n + 1] == 0:
                wait_halo(0)
            forces(turn[n + 1], (n + 1) % 2)
        gather(i, n % 2)

    table = jnp.concatenate(
        [accf[2:2 + PX].reshape(PX * QE, lanes), accf[0:2].reshape(2 * QE, lanes),
         accf[2 + PX:].reshape(2 * QE, lanes), accc[...].reshape(NC, lanes)], 0)
    parts = split2(table)
    both = ((slice(0, NF), slice(0, LW)), (slice(NF, NF + NC), slice(LW, 2 * LW)))
    for rows, cols in both:
        whole_v[rows] = thrice((parts[0][rows], parts[1][rows]),
                               (wz_v[0, :, cols], wz_v[1, :, cols]))
    whole_v[0:NF] = whole_v[0:NF] + bend_v[...].reshape(NF, LW)
    dlow, dhigh = pltpu.roll(dz_v[0], SZ - 2, 1), pltpu.roll(dz_v[1], 2, 1)

    wait_halo(1)
    wait_halo(2)
    adds = []
    for side in SIDES:
        h0, h1 = yrecv[side, 0], yrecv[side, 1]
        g = (h0 - 8.0 * h1, h1) if side == 0 else (-h0, 8.0 * h0 - h1)
        for k in range(2):
            y = k if side == 0 else SY - 2 + k
            at = pl.ds(y, SX, stride=SY)
            adds.append(g[k] * drows[at, :])
    faces = split2(jnp.concatenate(adds, 0))
    even = lane % 2 == 0
    hl, hh = zrecv[0], zrecv[1]
    cl = jnp.where(even, hl - 8.0 * pltpu.roll(hl, SZ - 1, 1), hl)
    ch = jnp.where(even, -hh, 8.0 * pltpu.roll(hh, 1, 1) - hh)
    g = thrice(wq_v, split2(jnp.concatenate([cl * dlow, ch * dhigh], 1)))

    def with_halos(rows, cols, blocks):
        added = thrice((wy_v[0, rows], wy_v[1, rows]), faces)
        part = slice(SZ, 2 * SZ)
        return whole_v[rows] + (
            thrice(split2(added), (wz_v[0, part, cols], wz_v[1, part, cols]))
            + thrice(split2(jnp.concatenate(blocks, 0)), (wh_v[0, :, cols], wh_v[1, :, cols])))

    coarse = with_halos(
        *both[1], [g[QE + q:QE + q + 1] * wx_v[EX:EX + XR] for q in range(QC)])

    pl.semaphore_wait(in_sem, nz - 1)

    mine = (me[0] * ny + me[1]) * nz + me[2]
    count = nx * ny * nz - 1

    def coarse_wait(sem):
        ref = all_v.at[pl.ds(0, count)]
        pltpu.make_async_copy(ref, ref, sem).wait()

    def coarse_copy(o, at):
        return pltpu.make_async_remote_copy(
            src_ref=all_v.at[at], dst_ref=all_v.at[at],
            send_sem=cs_sem, recv_sem=cr_sem,
            device_id=tuple(lax.rem(me[k] + o[k], sizes[k]) for k in range(3)),
            device_id_type=MESH)

    everyone = [(ox, oy, oz) for ox in range(nx) for oy in range(ny) for oz in range(nz)][1:]
    far = sorted(everyone, key=lambda o: -sum(min(o[k], sizes[k] - o[k]) for k in range(3)))
    for v in range(0, QC, PG):
        share = 0.0
        for q in range(v, min(v + PG, QC)):
            tile = coarse[q * XR:(q + 1) * XR]
            share = share + (tile if q == v else pltpu.roll(tile, (q - v) * GL, 1))
        all_v[mine, v // PG] = share[0:XC]

    @pl.when(me[0] >= 0)
    def _():
        for o in far:
            coarse_copy(o, mine).start()

    fine = with_halos(*both[0], [g[0:QE] * wx_v[p:p + 1] for p in turned])
    tall = jnp.concatenate([fine, jnp.zeros((2 * LW - NF, LW), f32)], 0).T
    fine = fine.reshape(EX, QE, LW)
    for side in SIDES:
        at = 3 * PZ + 8 * side
        for half in range(2):
            zm_v[side, half] = tall[at:at + 8, half * LW:(half + 1) * LW]
        at = PX + 2 * side
        xm_v[side] = fine[at:at + 2, 0:PY]
    ym_v[...] = fine[:, PY:PY + 4]

    def fine_copy(dx, dy, dz):
        xs, ys, zs = (0 if d > 0 else 1 for d in (dx, dy, dz))
        if dz:
            src = zm_v.at[1 - zs, 1 if dx else 0]
            dst = zg_v.at[zs, 1 - dx, 1 - dy]
        elif dy == 0:
            src, dst = xm_v.at[1 - xs], xg_v.at[xs]
        elif dx == 0:
            src, dst = ym_v.at[pl.ds(0, PX)], yg_v.at[ys]
        else:
            src, dst = ym_v.at[pl.ds(PX if dx < 0 else PX + 2, 2)], cg_v.at[xs, ys]
        at = (dx + 1, dy + 1 if ny > 2 else abs(dy), dz + 1)
        return pltpu.make_async_remote_copy(
            src_ref=src, dst_ref=dst, send_sem=as_sem.at[at], recv_sem=ar_sem.at[at],
            device_id=(me[0] + dx, me[1] + dy, me[2] + dz), device_id_type=MESH)

    def there(step):
        ok = None
        for k in range(3):
            if step[k]:
                here = has[k][0 if step[k] < 0 else 1]
                ok = here if ok is None else ok & here
        return ok

    for step in AROUND:
        @pl.when(there(step))
        def _(step=step):
            fine_copy(*step).start()

    zin, l = iota((KZ, LW), 0), iota((KZ, LW), 1)
    shares = 0.0
    for a in range(3):
        m = jnp.concatenate([same(l % KZ, zin), 2.0 * diff1(l % KZ, zin),
                             diff2(l % KZ, zin, KZ)], 1)
        ok = jnp.concatenate([l // KZ == a] * 3, 1)
        shares = shares + spread(cc_ref, a, KX * KY, KZ, jnp.where(ok, m, 0.0).astype(bf16))
    shares = shares.reshape(KX, KY, 3 * LW)
    padc_v[1:1 + KX, 8:8 + KY, :] = shares[:, :, 0:LW]
    for p in range(KX):
        midc_v[1 + p, 8:8 + KY] = (
            cross(padc_v, 1 + p, (8, KY))[0] + shares[p, :, LW:2 * LW])
    for p in range(KX):
        out = (cross(midc_v, 1 + p, (8, KY))[0] + shares[p, :, 2 * LW:]) * BEND
        for a in range(3):
            co_ref[a, p * KY:(p + 1) * KY] = (
                out if a == 0 else pltpu.roll(out, LW - a * KZ, 1))

    for step in AROUND:
        back = tuple(-d for d in step)

        @pl.when(there(back))
        def _(step=step):
            fine_copy(*step).wait_recv()
    tile = iota((8, LW), 1)
    x, y = tile // QE, tile % QE
    for side in SIDES:
        got = 0.0
        for sx in STEPS:
            shift = {-1: -2 * QE, 0: 0, 1: (PX - 2) * QE}[sx]
            xin = {-1: x < 2, 0: x < PX, 1: x >= PX - 2}[sx]
            for sy in STEPS:
                yin = {-1: y < 2, 0: y < PY, 1: (y >= PY - 2) & (y < PY)}[sy]
                turn = (shift + {-1: -PY - 2, 0: 0, 1: -2}[sy]) % LW
                value = zg_v[side, 1 + sx, 1 + sy]
                value = pltpu.roll(value, turn, 1) if turn else value
                got = got + jnp.where(xin & yin, value, 0.0)
        for a in range(3):
            at = a * PZ + side * (PZ - 2)
            zt_v[at:at + 2] = got[2 * a:2 * a + 2]
    across = zt_v[...].T.reshape(PX, QE, LW)
    row = iota((PY, LW), 0)
    for p in range(PX):
        out = fine[p, 0:PY] + across[p, 0:PY]
        low, high = yg_v[0, p], yg_v[1, p]
        for side in SIDES:
            q = p if side == 0 else p - (PX - 2)
            if 0 <= q < 2:
                out = out + xg_v[side, q]
                low, high = low + cg_v[side, 0, q], high + cg_v[side, 1, q]
        fill = jnp.zeros((PY - 4, LW), f32)
        low = pltpu.roll(jnp.concatenate([low, fill], 0), PY - 2, 0)
        high = pltpu.roll(jnp.concatenate([high, fill], 0), PY - 2, 0)
        out = out + jnp.where(row < 2, low, jnp.where(row >= PY - 2, high, 0.0))
        for a in range(3):
            fo_ref[a, p] = (out if a == 0 else pltpu.roll(out, LW - a * PZ, 1))[:, 0:PZ]

    for step in AROUND:
        @pl.when(there(step))
        def _(step=step):
            fine_copy(*step).wait_send()
    if count:
        coarse_wait(cs_sem)
        coarse_wait(cr_sem)
    row = iota((XR, LW), 0)
    for v in range(0, QC, PG):
        for b in range(0, KX, XR):
            placed = []
            for iz in range(nz):
                here = 0.0
                for ix in range(nx):
                    first = CX * ix - 2 - b
                    if first <= -XC or first >= XR:
                        continue
                    block = all_v[ix * ny * nz + iz, v // PG]
                    for iy in range(1, ny):
                        block = block + all_v[(ix * ny + iy) * nz + iz, v // PG]
                    block = jnp.concatenate([block, jnp.zeros((XR - XC, LW), f32)], 0)
                    block = pltpu.roll(block, first % XR, 0)
                    here = here + jnp.where((row >= first) & (row < first + XC), block, 0.0)
                placed.append(here)
            for q in range(v, min(v + PG, QC)):
                for a in range(3):
                    out = 0.0
                    for iz in range(nz):
                        first = CZ * iz - 2
                        value = pltpu.roll(placed[iz], (first - (q - v) * GL - a * ZC) % LW, 1)
                        inside = (tile >= first) & (tile < first + ZC)
                        out = out + jnp.where(inside, value, 0.0)
                    at = pl.ds(b * KY + q, XR, stride=KY)
                    co_ref[a, at, :] = co_ref[a, at, :] + out


def write_out(f_ref, c_ref, fo_ref, co_ref):
    fo_ref[...] = f_ref[...]
    KX, KY, KZ = co_ref.shape[1:]
    for a in range(3):
        for p in range(KX):
            co_ref[a, p] = c_ref[a, p * KY:(p + 1) * KY, 0:KZ]


def solution(mesh):
    sizes = tuple(mesh.shape[a] for a in AXES)

    def step(warped, fixed, fine, coarse):
        SX, SY, SZ = warped.shape
        PX, PY, PZ = SX // SPF, SY // SPF, SZ // SPF
        KX, KY, KZ = coarse.shape[1:]
        nx, ny, nz = sizes
        EX, QE = PX + 4, PY + 8
        XR, QC = -(-(SX // SPC + 4) // 8) * 8, KY
        KV = SPF * SY
        NF, NC, LW = EX * QE, XR * QC, 128
        vmem = pl.BlockSpec(memory_space=pltpu.VMEM)
        hbm = pl.BlockSpec(memory_space=pltpu.HBM)
        V = pltpu.VMEM
        D = pltpu.SemaphoreType.DMA
        held = pl.pallas_call(
            functools.partial(kernel, sizes),
            out_shape=(pltpu.VMEM(fine.shape, f32), pltpu.VMEM((3, KX * KY, LW), f32)),
            in_specs=[hbm] * 4,
            out_specs=(vmem, vmem),
            scratch_shapes=[
                V((SX, SY, SZ), f32), V((SX, SY, SZ), f32),
                V((3, PX, PY, PZ), f32), V(coarse.shape, f32),
                V((SX + 4, SY + 16, SZ), f32),
                V((2, 2, SX, SZ), f32), V((2, 2, SX, SZ), f32),
                V((2, SY, SZ), f32), V((2, SY, SZ), f32), V((2, SY, SZ), f32),
                V((2, 5 * QE, KV), bf16), V((SPC // SPF, 2, 4 * QC, KV), bf16),
                V((2, NF + NC, 4 * SX), bf16), V((2, QE + QC, SY), bf16),
                V((EX + XR, 2 * SZ), f32),
                V((2, 3 * SZ, 2 * LW), bf16), V((2, 2 * SZ, 2 * LW), bf16),
                V((2, KV, 3 * SZ), bf16), V((2, KV, 3 * SZ), bf16),
                V((SX * SY, 2 * SZ), bf16), V((2 * SZ, SZ), bf16),
                V((EX, QE, 3 * SZ), f32), V((QC, XR, 3 * SZ), f32),
                V((NF + NC, LW), f32),
                V((PX + 6, PY + 16, LW), f32), V((PX + 6, PY + 16, LW), f32),
                V((EX, QE, LW), f32),
                V((KX + 2, KY + 16, LW), f32), V((KX + 2, KY + 16, LW), f32),
                V((2, 2, 8, LW), f32), V((2, 3, 3, 8, LW), f32), V((LW, LW), f32),
                V((2, 2, PY, LW), f32), V((EX, 4, LW), f32),
                V((2, 2, PY, LW), f32), V((2, PX, 4, LW), f32), V((2, 2, 2, 4, LW), f32),
                V((nx * ny * nz, -(-QC // 4), SX // SPC + 4, LW), f32),
                D((2, SX // SPF // 2)), D((2,)), D((3, 2)), D((3, 2)), D((2, 4)), D((2, 4)),
                D((3, 3 if ny > 2 else 2, 3)), D((3, 3 if ny > 2 else 2, 3)), D(()), D(()), pltpu.SemaphoreType.REGULAR,
            ],
            compiler_params=pltpu.CompilerParams(
                collective_id=0, has_side_effects=True, vmem_limit_bytes=64000000
            ),
        )(warped, fixed, fine, coarse)
        held = [pltpu.with_memory_space_constraint(h, memory_space=pltpu.VMEM) for h in held]
        return pl.pallas_call(
            write_out,
            out_shape=(jax.ShapeDtypeStruct(fine.shape, f32),
                       jax.ShapeDtypeStruct(coarse.shape, f32)),
            in_specs=[vmem] * 2,
            out_specs=(vmem, vmem),
        )(*held)

    in_specs = (P("gx", "gy", "gz"), P("gx", "gy", "gz"), P(None, "gx", "gy", "gz"), P())
    out_specs = (P(None, "gx", "gy", "gz"), P())
    return jax.shard_map(
        step, mesh=mesh, in_specs=in_specs, out_specs=out_specs, check_vma=False
    )
```
